32 devices in a mesh: seq: 8 (over z, x), head: 4 (over y, core).
Axes of the slice: x: 2, y: 2, z: 4, core: 2. Of those that a mesh axis runs over, the one named last changes fastest.
Arguments:
- tokens: bfloat16 [8192, 2048], P('seq'), may hold values from -6 to 6
- owner_slot: int32 [8192], P('seq'), may hold values from 0 to 2047, as said below
- w_in: bfloat16 [8, 2048, 4096], P('seq', None, 'head'), as said below
- w_bc: bfloat16 [2048, 256], replicated, may hold values from -0.125 to 0.125
- w_dt: bfloat16 [2048, 32], P(None, 'head'), may hold values from -0.125 to 0.125
- conv_x: float32 [4, 2048], P(None, 'head'), may hold values from -3 to 3
- conv_bc: float32 [4, 256], replicated, may hold values from -3 to 3
- dt_bias: float32 [32], P('head'), may hold values from -1 to 1
- decay_rate: float32 [32], P('head'), may hold values from 2e-06 to 0.1
- d_skip: float32 [32], P('head'), may hold values from 0.5 to 2
- norm_gain: float32 [2048], P('head'), may hold values from 0.5 to 1.5
Outputs:
- normed: bfloat16 [8192, 2048], P('seq', 'head')
The draws below stay inside these ranges and needn't reach their ends.
Inputs may be any that keep to these rules, and one draw needn't show every extreme that they name: Within each block of 1024 tokens the values are distinct; the owner owner_slot // 256 gets at most 256 tokens of one block, and in every draw one owner gets exactly 256 tokens of every block. The token's modality is the owner's index modulo 3. Owner o holds the projection of modality o % 3: w_in[o] equals w_in[o % 3].
All inputs are finite; a program needn't handle non-finite values.
Results may differ from the reference program's by a relative error of at most 0.0054.
Values may be sent and summed in bfloat16 or wider, within the bound.
A program may use at most 128 MiB of HBM per device.

```python
import math
import jax
import jax.numpy as jnp
from jax import lax

D = 2048
HDIM = 64
NSTATE = 128
MODS = 3
KCONV = 4
QB = 256
TOK_DEV = 1024
TOKENS = 8192
HEADS = 32
INNER = 2048
CAP = 256
N_SEQ = 8


def owner_plan(key):
    slot_total = N_SEQ * CAP
    slot_ids = jnp.arange(slot_total, dtype=jnp.int32)
    owners = slot_ids // CAP
    full_owner = jax.random.randint(jax.random.fold_in(key, 1), (), 0, N_SEQ)
    busy_modality = jax.random.randint(jax.random.fold_in(key, 2), (), 0, MODS)

    def one_block(block_key):
        random_part = jax.random.randint(jax.random.fold_in(block_key, 3), (slot_total,), 0, 4096)
        scores = random_part + jnp.where(owners == full_owner, 16384, 0) + jnp.where(owners % MODS == busy_modality, 2048, 0)
        ranked = scores * slot_total + slot_ids
        picked = jnp.argsort(-ranked)[:TOK_DEV].astype(jnp.int32)
        modality = picked // CAP % MODS
        order_rank = jax.random.permutation(jax.random.fold_in(block_key, 4), MODS)
        jitter = jax.random.randint(jax.random.fold_in(block_key, 5), (TOK_DEV,), 0, 1024)
        sort_keys = (order_rank[modality] * 1024 + jitter) * slot_total + picked
        return picked[jnp.argsort(sort_keys)].astype(jnp.int32)
    blocks = jax.vmap(one_block)(jax.random.split(jax.random.fold_in(key, 9), N_SEQ))
    return blocks.reshape(N_SEQ * TOK_DEV)


def draw_owner_slot(key, part):
    return owner_plan(key)


def draw_w_in(key, part):
    modal_base = (jax.random.normal(jax.random.fold_in(key, 7), (MODS, D, 2 * INNER), jnp.float32) * D ** (-0.5)).astype(jnp.bfloat16)
    return modal_base[jnp.arange(N_SEQ) % MODS]


def block_scale(own_key, extent, shards, least, largest):
    def one(dim, parts):
        heights = jax.random.uniform(jax.random.fold_in(jax.random.fold_in(own_key, 6), dim), (parts,), jnp.float32, least / len(shards), largest / len(shards))
        return jnp.repeat(jnp.exp(heights), extent[dim] // parts).reshape((-1,) + (1,) * (len(extent) - dim - 1))

    loudness = one(*shards[0])
    for cut in shards[1:]:
        loudness = loudness * one(*cut)
    return loudness


def gaussian(key, shape, spread, bound, cuts=(), held_as=jnp.bfloat16):
    entries = jax.random.normal(key, shape, jnp.float32) * spread
    if len(cuts) > 0:
        entries = block_scale(key, shape, cuts, -0.22, 0.18) * entries
    return jnp.clip(entries, min=-bound, max=bound).astype(held_as)


def setup_inputs(seed: int = 0) -> dict:
    streams_of = jax.random.split(jax.random.key(seed), 12)
    tokens = gaussian(streams_of[0], (TOKENS, D), 1.0, 6.0, ((0, 8),))
    owner_slot = draw_owner_slot(jax.random.fold_in(streams_of[11], 71), 0)
    w_in = draw_w_in(jax.random.fold_in(streams_of[11], 71), 0)
    w_bc = gaussian(streams_of[3], (D, 2 * NSTATE), D ** -0.5, 0.125)
    w_dt = gaussian(streams_of[4], (D, HEADS), D ** -0.5, 0.125, ((1, 4),))
    conv_x = gaussian(streams_of[5], (KCONV, INNER), KCONV ** -0.5, 3.0, ((1, 4),), jnp.float32)
    conv_bc = gaussian(streams_of[6], (KCONV, 2 * NSTATE), KCONV ** -0.5, 3.0, (), jnp.float32)
    dt_bias = jnp.clip(jax.random.uniform(streams_of[7], (HEADS,), jnp.float32, -1.0, 1.0) * block_scale(streams_of[7], (HEADS,), ((0, 4),), -0.4, 0.0), -1.0, 1.0)
    decay_rate = jnp.clip(jnp.exp(math.log(0.1) - 10.819778 * jax.random.uniform(streams_of[8], (HEADS,), jnp.float32) ** block_scale(streams_of[8], (HEADS,), ((0, 4),), -0.2, 0.2)), 1.9999999949504854e-06, 0.1)
    d_skip = jnp.clip(0.5 + 1.5 * jax.random.uniform(streams_of[9], (HEADS,), jnp.float32) ** block_scale(streams_of[9], (HEADS,), ((0, 4),), -0.2, 0.2), 0.5, 2.0)
    norm_gain = jnp.clip(1.0 + 0.1 * jax.random.normal(streams_of[10], (INNER,), jnp.float32), 0.5, 1.5)
    return {"tokens": tokens, "owner_slot": owner_slot, "w_in": w_in, "w_bc": w_bc, "w_dt": w_dt, "conv_x": conv_x, "conv_bc": conv_bc, "dt_bias": dt_bias, "decay_rate": decay_rate, "d_skip": d_skip, "norm_gain": norm_gain}


EPSILON = 1e-05

def causal_conv(values, rim, weights):
    kernel_width = weights.shape[0]
    joined = jnp.concatenate([rim, values]).astype(jnp.float32)
    length = values.shape[0]
    summed = jnp.zeros(values.shape, jnp.float32)
    for offset in range(kernel_width):
        summed = summed + weights[offset] * joined[offset:offset + length]
    return summed

def block_terms(x_blk, b_blk, c_blk, dt_blk, log_blk):
    length = x_blk.shape[0]
    cumulative = jnp.cumsum(log_blk, axis=0)
    scores = jnp.dot(c_blk, b_blk.T, preferred_element_type=jnp.float32)
    log_gaps = cumulative[:, None, :] - cumulative[None, :, :]
    row_index = lax.broadcasted_iota(jnp.int32, (length, length), 0)
    col_index = lax.broadcasted_iota(jnp.int32, (length, length), 1)
    causal = (row_index >= col_index)[:, :, None]
    mixing = (scores[:, :, None] * jnp.exp(jnp.where(causal, log_gaps, -jnp.inf)) * dt_blk[None, :, :]).astype(jnp.bfloat16)
    inside = jnp.einsum('ijh,jhp->ihp', mixing.astype(jnp.float32), x_blk.astype(jnp.float32))
    to_end = jnp.exp(cumulative[-1:, :] - cumulative) * dt_blk
    weighted = (x_blk.astype(jnp.float32) * to_end[:, :, None]).astype(jnp.bfloat16)
    block_state = jnp.einsum('jhp,jn->hpn', weighted.astype(jnp.float32), b_blk.astype(jnp.float32))
    return (inside, block_state, cumulative)

def reference(tokens, owner_slot, w_in, w_bc, w_dt, conv_x, conv_bc, dt_bias, decay_rate, d_skip, norm_gain):
    modality = owner_slot // CAP % MODS
    projected = jnp.zeros((TOKENS, 2 * INNER), jnp.float32)
    for which in range(MODS):
        product = jnp.dot(tokens, w_in[which], preferred_element_type=jnp.float32)
        projected = jnp.where((modality == which)[:, None], product, projected)
    projected = projected.astype(jnp.bfloat16).reshape(TOKENS, HEADS, 2, HDIM)
    x_raw = projected[:, :, 0, :].reshape(TOKENS, INNER)
    z_gate = projected[:, :, 1, :].reshape(TOKENS, INNER)
    bc_raw = jnp.dot(tokens, w_bc, preferred_element_type=jnp.float32).astype(jnp.bfloat16)
    dt_raw = jnp.dot(tokens, w_dt, preferred_element_type=jnp.float32)
    x_conv = jax.nn.silu(causal_conv(x_raw, jnp.zeros((KCONV - 1, INNER), jnp.bfloat16), conv_x)).astype(jnp.bfloat16)
    bc_conv = jax.nn.silu(causal_conv(bc_raw, jnp.zeros((KCONV - 1, 2 * NSTATE), jnp.bfloat16), conv_bc)).astype(jnp.bfloat16)
    steps_dt = jax.nn.softplus(dt_raw + dt_bias)
    log_decay = -steps_dt * decay_rate
    block_total = TOKENS // QB
    pieces = (x_conv.reshape(block_total, QB, HEADS, HDIM), bc_conv[:, :NSTATE].reshape(block_total, QB, NSTATE), bc_conv[:, NSTATE:].reshape(block_total, QB, NSTATE), steps_dt.reshape(block_total, QB, HEADS), log_decay.reshape(block_total, QB, HEADS))

    def advance(states, block):
        x_blk, b_blk, c_blk, dt_blk, log_blk = block
        inside, block_state, cumulative = block_terms(x_blk, b_blk, c_blk, dt_blk, log_blk)
        outside = jnp.exp(cumulative)[:, :, None] * jnp.einsum('in,hpn->ihp', c_blk.astype(jnp.float32), states, precision=lax.Precision.HIGHEST)
        result = inside + outside + d_skip[None, :, None] * x_blk.astype(jnp.float32)
        states = states * jnp.exp(cumulative[-1])[:, None, None] + block_state
        return (states, result)
    start_state = jnp.zeros((HEADS, HDIM, NSTATE), jnp.float32)
    final_state, outputs = lax.scan(advance, start_state, pieces)
    outputs = outputs.reshape(TOKENS, INNER)
    gated = outputs * jax.nn.silu(z_gate.astype(jnp.float32))
    mean_square = lax.optimization_barrier(jnp.mean(gated * gated, axis=1, keepdims=True))
    return (gated * lax.rsqrt(mean_square + EPSILON) * norm_gain).astype(jnp.bfloat16)
```

```python
import functools
import types

import jax
import jax.numpy as jnp
from jax import lax
from jax.experimental import pallas as pl
from jax.experimental.pallas import tpu as pltpu
from jax.sharding import PartitionSpec as P

KCONV = 4
QB = 256
MODS = 3


EPSILON = 1e-05
LANES = 128
MESH = pl.DeviceIdType.MESH


def swapped(value, bit):
    count = lax.axis_size("seq")
    return lax.ppermute(value, "seq", [(source, source ^ bit) for source in range(count)])


def picked(weight, part, head_size, kind):
    columns = weight.shape[1] // 2
    source = lax.broadcasted_iota(jnp.int32, (columns, columns // 2), 0)
    target = lax.broadcasted_iota(jnp.int32, (columns, columns // 2), 1)
    wanted = (target // head_size) * 2 * head_size + kind * head_size + target % head_size
    chooser = (source == wanted).astype(jnp.bfloat16)
    chunk = weight[:, part * columns : (part + 1) * columns]
    return jnp.dot(chunk, chooser, preferred_element_type=jnp.float32).astype(jnp.bfloat16)


def exchange_pair(halves):
    index = lax.axis_index("seq")
    orders = ((1, 2), (2, 1))
    firsts = [swapped(half, bits[0]) for half, bits in zip(halves, orders)]
    slots = []
    for half, got, bits in zip(halves, firsts, orders):
        partner = index ^ bits[1]
        wanted = MODS - partner % MODS - (partner ^ bits[0]) % MODS
        sent = jnp.where(index % MODS == wanted, half, got)
        slots.append((half, got, swapped(sent, bits[1])))
    return slots


def dot(a, b):
    return jnp.dot(a, b, preferred_element_type=jnp.float32)


def dot_nt(a, b):
    return lax.dot_general(a, b, (((1,), (1,)), ((), ())), preferred_element_type=jnp.float32)


def dot_tn(a, b):
    return lax.dot_general(a, b, (((0,), (0,)), ((), ())), preferred_element_type=jnp.float32)


def rounded(value):
    return value.astype(jnp.bfloat16).astype(jnp.float32)


def three_parts(value):
    high = rounded(value)
    middle = rounded(value - high)
    return high, middle, value - high - middle


def side_by_side(value, count):
    high, middle, low = three_parts(value)
    packed = high + pltpu.roll(middle, count, 1) + pltpu.roll(low, 2 * count, 1)
    return packed.astype(jnp.bfloat16)


def silu(value):
    return value * jax.nn.sigmoid(value)


def distances(seq_count):
    steps = []
    while sum(steps) < seq_count - 1:
        steps.append(1 << len(steps))
    return steps


def start_states(sizes, refs, sends, step, own_state, own_decay):
    reach = distances(sizes.seq_count)[step]
    index = lax.axis_index("seq")
    target = (index + reach, lax.axis_index("head"))
    refs.state_out[step] = own_state.astype(jnp.bfloat16)
    refs.decay_out[step] = jnp.broadcast_to(own_decay, refs.decay_out.shape[1:])

    def copies():
        return [
            pltpu.make_async_remote_copy(
                source.at[step],
                landing.at[step],
                refs.scan_send.at[step, place],
                refs.scan_recv.at[step, place],
                device_id=target,
                device_id_type=MESH,
            )
            for place, (source, landing) in enumerate(
                ((refs.state_out, refs.state_in), (refs.decay_out, refs.decay_in))
            )
        ]

    @pl.when(index + reach < sizes.seq_count)
    def _():
        for copy in copies():
            copy.start()

    return copies, reach


def finish_kernel(
    sizes,
    names,
    *all_refs,
):
    refs = types.SimpleNamespace(**dict(zip(names, all_refs)))
    index, column = lax.axis_index("seq"), lax.axis_index("head")
    seq_count, head_count = sizes.seq_count, sizes.head_count
    reaches = distances(seq_count)

    barrier = pltpu.get_barrier_semaphore()
    expected = head_count - 1
    for reach in reaches:
        @pl.when(index + reach < seq_count)
        def _(reach=reach):
            pl.semaphore_signal(barrier, inc=1, device_id=(index + reach, column), device_id_type=MESH)

        @pl.when(index >= reach)
        def _(reach=reach):
            pl.semaphore_signal(barrier, inc=1, device_id=(index - reach, column), device_id_type=MESH)

        expected = expected + jnp.where(index + reach < seq_count, 1, 0) + jnp.where(index >= reach, 1, 0)
    for step in range(1, head_count):
        peer = lax.rem(column + step, head_count)
        pl.semaphore_signal(barrier, inc=1, device_id=(index, peer), device_id_type=MESH)
    pl.semaphore_wait(barrier, expected)
    finish_body(sizes, refs)


def finish_body(sizes, refs):
    index, column = lax.axis_index("seq"), lax.axis_index("head")
    seq_count, head_count = sizes.seq_count, sizes.head_count
    heads, head_size, nstate = sizes.heads, sizes.head_size, sizes.nstate
    rows, channels = refs.x.shape
    blocks = rows // QB
    taps = refs.conv_x.shape[0]
    edge = 16
    reaches = distances(seq_count)

    def rims():
        return [
            pltpu.make_async_remote_copy(
                source.at[pl.ds(rows - edge, edge)],
                landing,
                refs.rim_send.at[place],
                refs.rim_recv.at[place],
                device_id=(index + 1, column),
                device_id_type=MESH,
            )
            for place, (source, landing) in enumerate(((refs.bc, refs.bc_rim), (refs.x, refs.x_rim)))
        ]

    @pl.when(index + 1 < seq_count)
    def _():
        for copy in rims():
            copy.start()

    lane = lax.broadcasted_iota(jnp.int32, (1, LANES), 1)
    params = refs.params
    params[...] = jnp.zeros_like(params)
    params[0:1, 0:heads] = refs.dt_bias[...]
    params[1:2, 0:heads] = refs.decay_rate[...]
    params[2:3, 0:heads] = refs.d_skip[...]
    dt = refs.dt
    dt[...] = jnp.zeros_like(dt)
    dt[:, 0:heads] = refs.dt_raw[...]
    tri_row = lax.broadcasted_iota(jnp.int32, (QB, QB), 0)
    tri_col = lax.broadcasted_iota(jnp.int32, (QB, QB), 1)
    lower = jnp.where(tri_row >= tri_col, 1.0, 0.0).astype(jnp.bfloat16)
    spread_row = lax.broadcasted_iota(jnp.int32, (LANES, channels), 0)
    spread_col = lax.broadcasted_iota(jnp.int32, (LANES, channels), 1)
    wanted = (spread_row % heads == spread_col // head_size) & (spread_row < 3 * heads)
    spread = jnp.where(wanted, 1.0, 0.0).astype(jnp.bfloat16)
    skip_row = dot(side_by_side(params[...], heads), spread)[2:3, :]

    @pl.when(index == 0)
    def _():
        refs.x_rim[...] = jnp.zeros_like(refs.x_rim)
        refs.bc_rim[...] = jnp.zeros_like(refs.bc_rim)

    @pl.when(index > 0)
    def _():
        for copy in rims():
            copy.wait_recv()

    wide = 8
    for source, rim, target in ((refs.bc, refs.bc_rim, refs.bc_wide), (refs.x, refs.x_rim, refs.x_wide)):
        target[0:wide, :] = rim[...].astype(jnp.float32)[edge - wide :, :]
        target[wide:, :] = source[...].astype(jnp.float32)

    carried = jnp.zeros((nstate, channels), jnp.float32)
    carried_decay = jnp.ones((1, channels), jnp.float32)
    for block in range(blocks):
        span = pl.ds(block * QB, QB)
        step_dt = jax.nn.softplus(dt[span, :] + params[0:1, :])
        log_decay = jnp.where(lane < heads, -step_dt * params[1:2, :], 0.0)
        sums = dot(lower, side_by_side(log_decay, heads))
        cum = sums + pltpu.roll(sums, LANES - heads, 1) + pltpu.roll(sums, LANES - 2 * heads, 1)
        cum = jnp.where(lane < heads, cum, 0.0)
        refs.cum[span, :] = cum
        refs.cum_t[:, span] = cum.T[0:heads, :]
        refs.dt_t[:, span] = step_dt.T[0:heads, :]
        last = cum[QB - 1 : QB, :]
        to_end = jnp.where(lane < heads, jnp.exp(last - cum) * step_dt, 0.0)
        from_start = jnp.where(lane < heads, jnp.exp(cum), 0.0)
        to_end = dot(side_by_side(to_end, heads), spread)
        from_start = dot(side_by_side(from_start, heads), spread)
        refs.from_start[span, :] = from_start
        for source, weights, target in (
            (refs.bc_wide, refs.conv_bc, refs.bc_conv),
            (refs.x_wide, refs.conv_x, refs.x_conv),
        ):
            total = jnp.zeros((QB, source.shape[1]), jnp.float32)
            for tap in range(taps):
                shifted = source[pl.ds(block * QB + wide - taps + 1 + tap, QB), :]
                total = total + weights[tap : tap + 1, :] * shifted
            target[span, :] = silu(total).astype(jnp.bfloat16)
        x_blk = refs.x_conv[span, :]
        weighted = (x_blk.astype(jnp.float32) * to_end).astype(jnp.bfloat16)
        added = dot_tn(refs.bc_conv[span, 0:nstate], weighted)
        refs.entering[block] = carried
        refs.prior[block] = jnp.broadcast_to(carried_decay, refs.prior.shape[1:])
        decay = from_start[QB - 1 : QB, :]
        carried = carried * decay + added
        carried_decay = carried_decay * decay
    refs.own_state[...] = carried
    refs.own_decay[...] = jnp.broadcast_to(carried_decay, refs.own_decay.shape)
    copies, reach = start_states(sizes, refs, None, 0, carried, carried_decay)

    half = 2 * head_size
    pair_lane = lax.broadcasted_iota(jnp.int32, (QB, half), 1)
    causal = tri_row >= tri_col

    @pl.loop(0, blocks)
    def _(block):
        begin = pl.multiple_of(block * QB, QB)
        span = pl.ds(begin, QB)
        scores = dot_nt(refs.bc_conv[span, nstate:], refs.bc_conv[span, 0:nstate])
        for pair in range(heads // 2):
            lanes = pl.ds(pair * half, half)
            x_pair = refs.x_conv[span, lanes]
            total = jnp.zeros((QB, half), jnp.float32)
            for which in range(2):
                head = 2 * pair + which
                gap = refs.cum[span, head : head + 1] - refs.cum_t[head : head + 1, span]
                factor = jnp.exp(jnp.where(causal, gap, -jnp.inf))
                mixing = (scores * factor * refs.dt_t[head : head + 1, span]).astype(jnp.bfloat16)
                mine = (pair_lane >= head_size) if which else (pair_lane < head_size)
                total = total + dot(mixing, jnp.where(mine, x_pair, jnp.zeros_like(x_pair)))
            refs.y[span, lanes] = total + skip_row[:, pair * half : (pair + 1) * half] * x_pair.astype(
                jnp.float32
            )

    incoming = refs.incoming
    incoming[...] = jnp.zeros_like(incoming)
    refs.incoming_decay[...] = jnp.ones_like(refs.incoming_decay)
    for step, reach in enumerate(reaches):
        if step > 0:
            copies, reach = start_states(
                sizes, refs, None, step, refs.own_state[...], refs.own_decay[0:1, :]
            )

        @pl.when(index >= reach)
        def _(step=step, copies=copies):
            for copy in copies():
                copy.wait_recv()
            state = refs.state_in[step].astype(jnp.float32)
            decay = refs.decay_in[step]
            incoming[...] = incoming[...] + refs.incoming_decay[0:1, :] * state
            refs.incoming_decay[...] = refs.incoming_decay[...] * decay
            if step + 1 < len(reaches):
                refs.own_state[...] = refs.own_state[...] + refs.own_decay[0:1, :] * state
                refs.own_decay[...] = refs.own_decay[...] * decay

        @pl.when(index + reach < seq_count)
        def _(copies=copies):
            for copy in copies():
                copy.wait_send()

    @pl.when(index + 1 < seq_count)
    def _():
        for copy in rims():
            copy.wait_send()

    ones = jnp.ones((8, LANES), jnp.bfloat16)

    @pl.loop(0, blocks)
    def _(block):
        begin = pl.multiple_of(block * QB, QB)
        span = pl.ds(begin, QB)
        state = refs.entering[block] + incoming[...] * refs.prior[block][0:1, :]
        high, middle, low = three_parts(state)
        c_blk = refs.bc_conv[span, nstate:]
        outside = dot(c_blk, high.astype(jnp.bfloat16)) + dot(c_blk, middle.astype(jnp.bfloat16))
        outside = outside + dot(c_blk, low.astype(jnp.bfloat16))
        value = refs.y[span, :] + refs.from_start[span, :] * outside
        value = value * silu(refs.z[span, :].astype(jnp.float32))
        refs.y[span, :] = value
        squares = value * value
        folded = squares[:, 0:LANES]
        for part in range(1, channels // LANES):
            folded = folded + squares[:, part * LANES : (part + 1) * LANES]
        first, second, third = three_parts(folded)
        total = dot_nt(ones, first.astype(jnp.bfloat16)) + dot_nt(ones, second.astype(jnp.bfloat16))
        refs.square[:, span] = total + dot_nt(ones, third.astype(jnp.bfloat16))

    def shares():
        return [
            pltpu.make_async_remote_copy(
                refs.square,
                refs.square_in.at[step - 1],
                refs.norm_send.at[step - 1],
                refs.norm_recv.at[step - 1],
                device_id=(index, lax.rem(column + step, head_count)),
                device_id_type=MESH,
            )
            for step in range(1, head_count)
        ]

    for copy in shares():
        copy.start()
    for copy in shares():
        copy.wait_recv()
    total = refs.square[...]
    for step in range(1, head_count):
        total = total + refs.square_in[step - 1]
    scale = lax.rsqrt(total / (head_count * channels) + EPSILON)
    first_row = lax.broadcasted_iota(jnp.int32, (8, channels), 0) == 0
    gains = jnp.where(first_row, 1.0, 0.0).astype(jnp.bfloat16)
    for block in range(blocks):
        span = pl.ds(block * QB, QB)
        wide_scale = jnp.zeros((QB, channels), jnp.float32)
        for part in three_parts(scale[:, block * QB : (block + 1) * QB]):
            wide_scale = wide_scale + dot_tn(part.astype(jnp.bfloat16), gains)
        refs.out[span, :] = (refs.y[span, :] * wide_scale * refs.norm_gain[...]).astype(jnp.bfloat16)
    for copy in shares():
        copy.wait_send()


def finish(x_raw, z_gate, bc_raw, dt_raw, conv_x, conv_bc, dt_bias, decay_rate, d_skip, norm_gain):
    rows, channels = x_raw.shape
    both = bc_raw.shape[1]
    heads = dt_bias.shape[0]
    nstate = both // 2
    blocks = rows // QB
    head_count = lax.axis_size("head")
    seq_count = lax.axis_size("seq")
    sizes = types.SimpleNamespace(
        seq_count=seq_count,
        head_count=head_count,
        heads=heads,
        head_size=channels // heads,
        nstate=nstate,
    )
    steps = len(distances(seq_count))
    inputs = dict(
        x=x_raw,
        z=z_gate,
        bc=bc_raw,
        dt_raw=dt_raw,
        conv_x=conv_x,
        conv_bc=conv_bc,
        dt_bias=dt_bias[None],
        decay_rate=decay_rate[None],
        d_skip=d_skip[None],
        norm_gain=norm_gain[None],
    )
    f32, bf16 = jnp.float32, jnp.bfloat16
    dma = pltpu.SemaphoreType.DMA
    scratch = dict(
        x_rim=pltpu.VMEM((16, channels), bf16),
        bc_rim=pltpu.VMEM((16, both), bf16),
        x_wide=pltpu.VMEM((rows + 8, channels), f32),
        bc_wide=pltpu.VMEM((rows + 8, both), f32),
        x_conv=pltpu.VMEM((rows, channels), bf16),
        bc_conv=pltpu.VMEM((rows, both), bf16),
        params=pltpu.VMEM((8, LANES), f32),
        dt=pltpu.VMEM((rows, LANES), f32),
        cum=pltpu.VMEM((rows, LANES), f32),
        cum_t=pltpu.VMEM((heads, rows), f32),
        dt_t=pltpu.VMEM((heads, rows), f32),
        from_start=pltpu.VMEM((rows, channels), f32),
        y=pltpu.VMEM((rows, channels), f32),
        entering=pltpu.VMEM((blocks, nstate, channels), f32),
        prior=pltpu.VMEM((blocks, 8, channels), f32),
        own_state=pltpu.VMEM((nstate, channels), f32),
        own_decay=pltpu.VMEM((8, channels), f32),
        incoming=pltpu.VMEM((nstate, channels), f32),
        incoming_decay=pltpu.VMEM((8, channels), f32),
        state_out=pltpu.VMEM((steps, nstate, channels), bf16),
        state_in=pltpu.VMEM((steps, nstate, channels), bf16),
        decay_out=pltpu.VMEM((steps, 8, channels), f32),
        decay_in=pltpu.VMEM((steps, 8, channels), f32),
        square=pltpu.VMEM((8, rows), f32),
        square_in=pltpu.VMEM((head_count - 1, 8, rows), f32),
        rim_send=dma((2,)),
        rim_recv=dma((2,)),
        scan_send=dma((steps, 2)),
        scan_recv=dma((steps, 2)),
        norm_send=dma((head_count - 1,)),
        norm_recv=dma((head_count - 1,)),
    )
    names = tuple(inputs) + ("out",) + tuple(scratch)
    return pl.pallas_call(
        functools.partial(finish_kernel, sizes, names),
        out_shape=jax.ShapeDtypeStruct((rows, channels), bf16),
        in_specs=[pl.BlockSpec(memory_space=pltpu.VMEM)] * len(inputs),
        out_specs=pl.BlockSpec(memory_space=pltpu.VMEM),
        scratch_shapes=list(scratch.values()),
        compiler_params=pltpu.CompilerParams(
            collective_id=0, has_side_effects=True, vmem_limit_bytes=48 << 20
        ),
    )(*inputs.values())


def per_device(
    tokens, owner_slot, w_in, w_bc, w_dt, conv_x, conv_bc, dt_bias, decay_rate, d_skip, norm_gain
):
    seq_count = lax.axis_size("seq")
    head_count = lax.axis_size("head")
    tok_rows = tokens.shape[0]
    width = tokens.shape[1]
    capacity = 2 * tok_rows // seq_count
    heads_here = dt_bias.shape[0]
    columns = w_in.shape[2]
    head_size = columns // (2 * heads_here)
    nstate = w_bc.shape[1] // 2
    own_index = lax.axis_index("seq")
    own_weight = w_in[0]
    x_halves = (picked(own_weight, 0, head_size, 0), picked(own_weight, 1, head_size, 0))
    z_halves = (picked(own_weight, 0, head_size, 1), picked(own_weight, 1, head_size, 1))
    x_a, x_b = exchange_pair(x_halves)
    z_first, z_second, a_got, b_got = lax.optimization_barrier((*z_halves, x_a[1], x_b[1]))
    x_a, x_b = (x_a[0], a_got, x_a[2]), (x_b[0], b_got, x_b[2])
    z_a, z_b = exchange_pair((z_first, z_second))
    modality = (owner_slot // capacity) % MODS

    def project(slots, bits):
        first = bits[0]
        own_mod = own_index % MODS
        next_mod = (own_index ^ first) % MODS
        products = [
            jnp.dot(tokens, slot, preferred_element_type=jnp.float32).astype(jnp.bfloat16)
            for slot in slots
        ]
        return jnp.where(
            (modality == own_mod)[:, None],
            products[0],
            jnp.where((modality == next_mod)[:, None], products[1], products[2]),
        )

    x_raw = jnp.concatenate([project(x_a, (1, 2)), project(x_b, (2, 1))], axis=1)
    z_gate = jnp.concatenate([project(z_a, (1, 2)), project(z_b, (2, 1))], axis=1)
    bc_raw = jnp.dot(tokens, w_bc, preferred_element_type=jnp.float32).astype(jnp.bfloat16)
    dt_raw = jnp.dot(tokens, w_dt, preferred_element_type=jnp.float32)
    return finish(
        x_raw, z_gate, bc_raw, dt_raw, conv_x, conv_bc, dt_bias, decay_rate, d_skip, norm_gain
    )


def solution(mesh):
    return jax.shard_map(
        per_device,
        mesh=mesh,
        in_specs=(
            P("seq", None),
            P("seq"),
            P("seq", None, "head"),
            P(),
            P(None, "head"),
            P(None, "head"),
            P(),
            P("head"),
            P("head"),
            P("head"),
            P("head"),
        ),
        out_specs=P("seq", "head"),
        check_vma=False,
    )
```

```python
import functools
import types

import jax
import jax.numpy as jnp
from jax import lax
from jax.experimental import pallas as pl
from jax.experimental.pallas import tpu as pltpu
from jax.sharding import PartitionSpec as P

KCONV = 4
QB = 256
MODS = 3
EPSILON = 1e-05
LANES = 128
MESH = pl.DeviceIdType.MESH


def route(start, end, width):
    found = {}
    for first in (0, 1):
        here, there = list(divmod(start, width)), divmod(end, width)
        for axis in (first, 1 - first):
            while here[axis] != there[axis]:
                before = tuple(here)
                here[axis] += 1 if there[axis] > here[axis] else -1
                link = (before, tuple(here))
                found[link] = found.get(link, 0.0) + 0.5
    return found


def serving_plan(count):
    width = max(side for side in range(1, count) if count % side == 0 and side * side <= count)
    foreign = [[owner for owner in range(count) if (owner - home) % MODS] for home in range(count)]
    groups = [(home, place) for home in range(count) for place in range(len(foreign[home]))]
    loads, busy, chosen = {}, [0] * count, {}

    def add(home, server, sign):
        busy[server] += sign
        for weight, ends in ((0.6, (home, server)), (1.0, (server, home))):
            for link, share in route(*ends, width).items():
                loads[link] = loads.get(link, 0.0) + sign * weight * share

    def price(home, server):
        total = 4.0 * busy[server]
        for weight, ends in ((0.6, (home, server)), (1.0, (server, home))):
            for link, share in route(*ends, width).items():
                total += weight * share * (2.0 * loads.get(link, 0.0) + weight * share)
        return total

    for _ in range(6):
        for home, place in groups:
            if (home, place) in chosen:
                add(home, chosen[home, place], -1)
            owner = foreign[home][place]
            options = [server for server in range(count) if (server - owner) % MODS == 0]
            best = min(options, key=lambda server: (round(price(home, server), 6), server))
            chosen[home, place] = best
            add(home, best, 1)
    order = [[] for _ in range(count)]
    for home, place in groups:
        earlier = sum(chosen[home, other] == chosen[home, place] for other in range(place))
        order[chosen[home, place]].append((earlier, place, home))
    served = [[(home, place) for _, place, home in sorted(line)] for line in order]
    slots = {group: slot for line in served for slot, group in enumerate(line)}
    return foreign, chosen, slots, served, loads


def dot(a, b):
    return jnp.dot(a, b, preferred_element_type=jnp.float32)


def dot_nt(a, b):
    return lax.dot_general(a, b, (((1,), (1,)), ((), ())), preferred_element_type=jnp.float32)


def dot_tn(a, b):
    return lax.dot_general(a, b, (((0,), (0,)), ((), ())), preferred_element_type=jnp.float32)


def rounded(value):
    return value.astype(jnp.bfloat16).astype(jnp.float32)


def three_parts(value):
    high = rounded(value)
    middle = rounded(value - high)
    return high, middle, value - high - middle


def side_by_side(value, count):
    high, middle, low = three_parts(value)
    packed = high + pltpu.roll(middle, count, 1) + pltpu.roll(low, 2 * count, 1)
    return packed.astype(jnp.bfloat16)


def silu(value):
    return value * jax.nn.sigmoid(value)


def distances(seq_count):
    steps = []
    while sum(steps) < seq_count - 1:
        steps.append(1 << len(steps))
    return steps


def start_states(sizes, refs, sends, step, own_state, own_decay):
    reach = distances(sizes.seq_count)[step]
    index = lax.axis_index("seq")
    target = (index + reach, lax.axis_index("head"))
    refs.state_out[step] = own_state.astype(jnp.bfloat16)
    refs.decay_out[step] = jnp.broadcast_to(own_decay, refs.decay_out.shape[1:])

    def copies():
        return [
            pltpu.make_async_remote_copy(
                source.at[step],
                landing.at[step],
                refs.scan_send.at[step, place],
                refs.scan_recv.at[step, place],
                device_id=target,
                device_id_type=MESH,
            )
            for place, (source, landing) in enumerate(
                ((refs.state_out, refs.state_in), (refs.decay_out, refs.decay_in))
            )
        ]

    @pl.when(index + reach < sizes.seq_count)
    def _():
        for copy in copies():
            copy.start()

    return copies, reach


def finish_body(sizes, refs):
    index, column = lax.axis_index("seq"), lax.axis_index("head")
    seq_count, head_count = sizes.seq_count, sizes.head_count
    heads, head_size, nstate = sizes.heads, sizes.head_size, sizes.nstate
    rows, channels = refs.x.shape
    blocks = rows // QB
    taps = refs.conv_x.shape[0]
    edge = 16
    reaches = distances(seq_count)

    def rims():
        return [
            pltpu.make_async_remote_copy(
                source.at[pl.ds(rows - edge, edge)],
                landing,
                refs.rim_send.at[place],
                refs.rim_recv.at[place],
                device_id=(index + 1, column),
                device_id_type=MESH,
            )
            for place, (source, landing) in enumerate(((refs.bc, refs.bc_rim), (refs.x, refs.x_rim)))
        ]

    @pl.when(index + 1 < seq_count)
    def _():
        for copy in rims():
            copy.start()

    lane = lax.broadcasted_iota(jnp.int32, (1, LANES), 1)
    params = refs.params
    params[...] = jnp.zeros_like(params)
    params[0:1, 0:heads] = refs.dt_bias[...]
    params[1:2, 0:heads] = refs.decay_rate[...]
    params[2:3, 0:heads] = refs.d_skip[...]
    dt = refs.dt_raw
    tri_row = lax.broadcasted_iota(jnp.int32, (QB, QB), 0)
    tri_col = lax.broadcasted_iota(jnp.int32, (QB, QB), 1)
    lower = jnp.where(tri_row >= tri_col, 1.0, 0.0).astype(jnp.bfloat16)
    spread_row = lax.broadcasted_iota(jnp.int32, (LANES, channels), 0)
    spread_col = lax.broadcasted_iota(jnp.int32, (LANES, channels), 1)
    wanted = (spread_row % heads == spread_col // head_size) & (spread_row < 3 * heads)
    spread = jnp.where(wanted, 1.0, 0.0).astype(jnp.bfloat16)
    skip_row = dot(side_by_side(params[...], heads), spread)[2:3, :]

    @pl.when(index == 0)
    def _():
        refs.x_rim[...] = jnp.zeros_like(refs.x_rim)
        refs.bc_rim[...] = jnp.zeros_like(refs.bc_rim)

    @pl.when(index > 0)
    def _():
        for copy in rims():
            copy.wait_recv()

    wide = 8
    for source, rim, target in ((refs.bc, refs.bc_rim, refs.bc_wide), (refs.x, refs.x_rim, refs.x_wide)):
        target[0:wide, :] = rim[...].astype(jnp.float32)[edge - wide :, :]
        target[wide:, :] = source[...].astype(jnp.float32)

    carried = jnp.zeros((nstate, channels), jnp.float32)
    carried_decay = jnp.ones((1, channels), jnp.float32)
    for block in range(blocks):
        span = pl.ds(block * QB, QB)
        step_dt = jax.nn.softplus(dt[span, :] + params[0:1, :])
        log_decay = jnp.where(lane < heads, -step_dt * params[1:2, :], 0.0)
        sums = dot(lower, side_by_side(log_decay, heads))
        cum = sums + pltpu.roll(sums, LANES - heads, 1) + pltpu.roll(sums, LANES - 2 * heads, 1)
        cum = jnp.where(lane < heads, cum, 0.0)
        refs.cum[span, :] = cum
        refs.cum_t[:, span] = cum.T[0:heads, :]
        refs.dt_t[:, span] = step_dt.T[0:heads, :]
        last = cum[QB - 1 : QB, :]
        to_end = jnp.where(lane < heads, jnp.exp(last - cum) * step_dt, 0.0)
        from_start = jnp.where(lane < heads, jnp.exp(cum), 0.0)
        to_end = dot(side_by_side(to_end, heads), spread)
        from_start = dot(side_by_side(from_start, heads), spread)
        refs.from_start[span, :] = from_start
        for source, weights, target in (
            (refs.bc_wide, refs.conv_bc, refs.bc_conv),
            (refs.x_wide, refs.conv_x, refs.x_conv),
        ):
            total = jnp.zeros((QB, source.shape[1]), jnp.float32)
            for tap in range(taps):
                shifted = source[pl.ds(block * QB + wide - taps + 1 + tap, QB), :]
                total = total + weights[tap : tap + 1, :] * shifted
            target[span, :] = silu(total).astype(jnp.bfloat16)
        x_blk = refs.x_conv[span, :]
        weighted = (x_blk.astype(jnp.float32) * to_end).astype(jnp.bfloat16)
        added = dot_tn(refs.bc_conv[span, 0:nstate], weighted)
        refs.entering[block] = carried
        refs.prior[block] = jnp.broadcast_to(carried_decay, refs.prior.shape[1:])
        decay = from_start[QB - 1 : QB, :]
        carried = carried * decay + added
        carried_decay = carried_decay * decay
    refs.own_state[...] = carried
    refs.own_decay[...] = jnp.broadcast_to(carried_decay, refs.own_decay.shape)
    copies, reach = start_states(sizes, refs, None, 0, carried, carried_decay)

    half = 2 * head_size
    pair_lane = lax.broadcasted_iota(jnp.int32, (QB, half), 1)
    causal = tri_row >= tri_col

    @pl.loop(0, blocks)
    def _(block):
        begin = pl.multiple_of(block * QB, QB)
        span = pl.ds(begin, QB)
        scores = dot_nt(refs.bc_conv[span, nstate:], refs.bc_conv[span, 0:nstate])
        for pair in range(heads // 2):
            lanes = pl.ds(pair * half, half)
            x_pair = refs.x_conv[span, lanes]
            total = jnp.zeros((QB, half), jnp.float32)
            for which in range(2):
                head = 2 * pair + which
                gap = refs.cum[span, head : head + 1] - refs.cum_t[head : head + 1, span]
                factor = jnp.exp(jnp.where(causal, gap, -jnp.inf))
                mixing = (scores * factor * refs.dt_t[head : head + 1, span]).astype(jnp.bfloat16)
                mine = (pair_lane >= head_size) if which else (pair_lane < head_size)
                total = total + dot(mixing, jnp.where(mine, x_pair, jnp.zeros_like(x_pair)))
            refs.y[span, lanes] = total + skip_row[:, pair * half : (pair + 1) * half] * x_pair.astype(
                jnp.float32
            )

    incoming = refs.incoming
    incoming[...] = jnp.zeros_like(incoming)
    refs.incoming_decay[...] = jnp.ones_like(refs.incoming_decay)
    for step, reach in enumerate(reaches):
        if step > 0:
            copies, reach = start_states(
                sizes, refs, None, step, refs.own_state[...], refs.own_decay[0:1, :]
            )

        @pl.when(index >= reach)
        def _(step=step, copies=copies):
            for copy in copies():
                copy.wait_recv()
            state = refs.state_in[step].astype(jnp.float32)
            decay = refs.decay_in[step]
            incoming[...] = incoming[...] + refs.incoming_decay[0:1, :] * state
            refs.incoming_decay[...] = refs.incoming_decay[...] * decay
            if step + 1 < len(reaches):
                refs.own_state[...] = refs.own_state[...] + refs.own_decay[0:1, :] * state
                refs.own_decay[...] = refs.own_decay[...] * decay

        @pl.when(index + reach < seq_count)
        def _(copies=copies):
            for copy in copies():
                copy.wait_send()

    @pl.when(index + 1 < seq_count)
    def _():
        for copy in rims():
            copy.wait_send()

    refs.collect_z()
    ones = jnp.ones((8, LANES), jnp.bfloat16)

    @pl.loop(0, blocks)
    def _(block):
        begin = pl.multiple_of(block * QB, QB)
        span = pl.ds(begin, QB)
        state = refs.entering[block] + incoming[...] * refs.prior[block][0:1, :]
        high, middle, low = three_parts(state)
        c_blk = refs.bc_conv[span, nstate:]
        outside = dot(c_blk, high.astype(jnp.bfloat16)) + dot(c_blk, middle.astype(jnp.bfloat16))
        outside = outside + dot(c_blk, low.astype(jnp.bfloat16))
        value = refs.y[span, :] + refs.from_start[span, :] * outside
        value = value * silu(rounded(refs.z_of(span)))
        refs.y[span, :] = value
        squares = value * value
        folded = squares[:, 0:LANES]
        for part in range(1, channels // LANES):
            folded = folded + squares[:, part * LANES : (part + 1) * LANES]
        first, second, third = three_parts(folded)
        total = dot_nt(ones, first.astype(jnp.bfloat16)) + dot_nt(ones, second.astype(jnp.bfloat16))
        refs.square[:, span] = total + dot_nt(ones, third.astype(jnp.bfloat16))

    def shares():
        return [
            pltpu.make_async_remote_copy(
                refs.square,
                refs.square_in.at[step - 1],
                refs.norm_send.at[step - 1],
                refs.norm_recv.at[step - 1],
                device_id=(index, lax.rem(column + step, head_count)),
                device_id_type=MESH,
            )
            for step in range(1, head_count)
        ]

    for copy in shares():
        copy.start()
    for copy in shares():
        copy.wait_recv()
    total = refs.square[...]
    for step in range(1, head_count):
        total = total + refs.square_in[step - 1]
    scale = lax.rsqrt(total / (head_count * channels) + EPSILON)
    first_row = lax.broadcasted_iota(jnp.int32, (8, channels), 0) == 0
    gains = jnp.where(first_row, 1.0, 0.0).astype(jnp.bfloat16)
    for block in range(blocks):
        span = pl.ds(block * QB, QB)
        wide_scale = jnp.zeros((QB, channels), jnp.float32)
        for part in three_parts(scale[:, block * QB : (block + 1) * QB]):
            wide_scale = wide_scale + dot_tn(part.astype(jnp.bfloat16), gains)
        refs.out[span, :] = (refs.y[span, :] * wide_scale * refs.norm_gain[...]).astype(jnp.bfloat16)
    for copy in shares():
        copy.wait_send()
    refs.settle()


def pick(options, which):
    value = options[0]
    for place in range(1, len(options)):
        value = jnp.where(which == place, options[place], value)
    return value


def padded(lines, length):
    return [list(line) + [0] * (length - len(line)) for line in lines]


def remote(source, target, send, recv, device):
    return pltpu.make_async_remote_copy(
        source, target, send, recv, device_id=device, device_id_type=MESH
    )


def project_kernel(sizes, names, *all_refs):
    refs = types.SimpleNamespace(**dict(zip(names, all_refs)))
    index, column = lax.axis_index("seq"), lax.axis_index("head")
    barrier = pltpu.get_barrier_semaphore()
    for step in range(1, sizes.seq_count):
        other = lax.rem(index + step, sizes.seq_count)
        pl.semaphore_signal(barrier, inc=1, device_id=(other, column), device_id_type=MESH)
    for step in range(1, sizes.head_count):
        other = lax.rem(column + step, sizes.head_count)
        pl.semaphore_signal(barrier, inc=1, device_id=(index, other), device_id_type=MESH)
    project_body(sizes, refs, barrier)
    finish_body(sizes, refs)


def project_body(sizes, refs, barrier):
    index, column = lax.axis_index("seq"), lax.axis_index("head")
    seq_count, head_count = sizes.seq_count, sizes.head_count
    cap, direct, shared, lines = sizes.cap, sizes.direct, sizes.shared, sizes.lines
    places, slot_count = sizes.places, sizes.slots
    rows, channels = refs.x.shape
    width = refs.tok.shape[1]
    blocks = rows // QB
    core, line = lax.rem(column, 2), column // 2
    half = width // 2
    foreign, chosen, slot_of, served, _ = serving_plan(seq_count)
    foreign_count = pick([len(line_) for line_ in foreign], index)
    served_count = pick([len(line_) for line_ in served], index)
    server_of, landing = [], []
    for place in range(places):
        server_of.append(pick([chosen.get((home, place), 0) for home in range(seq_count)], index))
        landing.append(pick([slot_of.get((home, place), 0) for home in range(seq_count)], index))
    homes, home_places = [], []
    for slot in range(slot_count):
        homes.append(pick([line_[slot][0] if slot < len(line_) else 0 for line_ in served], index))
        home_places.append(pick([line_[slot][1] if slot < len(line_) else 0 for line_ in served], index))

    def direct_lanes(which):
        return pl.ds(pl.multiple_of(which * half, LANES), direct)

    def shared_lanes(which, from_line):
        return pl.ds(pl.multiple_of(which * half + direct + from_line * shared, LANES), shared)

    own_copies = [
        pltpu.make_async_copy(
            refs.tokens.at[:, direct_lanes(core)], refs.own_tok.at[:, pl.ds(0, direct)], refs.local.at[0]
        ),
        pltpu.make_async_copy(
            refs.tokens.at[:, shared_lanes(core, line)],
            refs.own_tok.at[:, pl.ds(direct, shared)],
            refs.local.at[1],
        ),
    ]
    weight_copy = pltpu.make_async_copy(refs.w_in.at[0], refs.weight, refs.local.at[2])
    token_copy = pltpu.make_async_copy(refs.tokens, refs.tok, refs.local.at[3])
    side_copy = pltpu.make_async_copy(refs.w_bc, refs.side, refs.local.at[4])
    for copy in own_copies + [weight_copy, token_copy, side_copy]:
        copy.start()

    slots = refs.owner_slot[...]
    place_row = jnp.full(slots.shape, -1, jnp.int32)
    place = 0
    for owner in range(seq_count):
        away = lax.rem(owner + MODS * seq_count - index, MODS) != 0
        shift = jnp.where(away, (place - owner) * cap, 0)
        within = (slots >= owner * cap) & (slots < (owner + 1) * cap)
        moved = jnp.where(away, slots + shift, -1)
        place_row = jnp.where(within, moved, place_row)
        place = place + jnp.where(away, 1, 0)

    for place in range(min(len(line_) for line_ in foreign), places):

        @pl.when(place >= foreign_count)
        def _(place=place):
            span = pl.ds(place * cap, cap)
            refs.x_back[span, :] = jnp.zeros((cap, channels), jnp.bfloat16)
            refs.z_back[span, :] = jnp.zeros((cap, channels), jnp.bfloat16)

    def sends(place):
        server = (server_of[place], column)
        slot = landing[place]
        return [
            remote(
                refs.packed.at[place, :, pl.ds(0, direct)],
                refs.inbox.at[slot, :, direct_lanes(core)],
                refs.pack_send.at[place, 0],
                refs.pack_recv.at[slot, 0],
                server,
            ),
            remote(
                refs.packed.at[place, :, pl.ds(direct, shared)],
                refs.inbox.at[slot, :, shared_lanes(core, line)],
                refs.pack_send.at[place, 1],
                refs.pack_recv.at[slot, 1],
                server,
            ),
        ]

    for copy in own_copies:
        copy.wait()
    sublane = lax.broadcasted_iota(jnp.int32, (cap, rows), 0)
    for place in range(places):

        @pl.when(place < foreign_count)
        def _(place=place):
            chosen_rows = jnp.where(place_row == sublane + place * cap, 1.0, 0.0).astype(jnp.bfloat16)
            refs.packed[place] = dot(chosen_rows, refs.own_tok[...]).astype(jnp.bfloat16)
            if place == 0:
                pl.semaphore_wait(barrier, seq_count + head_count - 2)
            for copy in sends(place):
                copy.start()

    pair = 4 * sizes.head_size
    source = lax.broadcasted_iota(jnp.int32, (pair, pair), 0)
    target = lax.broadcasted_iota(jnp.int32, (pair, pair), 1)
    size = sizes.head_size
    from_z = target // (2 * size)
    wanted = (target % (2 * size)) // size * (2 * size) + from_z * size + target % size
    chooser = jnp.where(source == wanted, 1.0, 0.0).astype(jnp.bfloat16)
    weight_copy.wait()

    @pl.loop(0, width // QB)
    def _(part):
        span = pl.ds(pl.multiple_of(part * QB, QB), QB)
        for couple in range(sizes.heads // 2):
            split = dot(refs.weight[span, couple * pair : (couple + 1) * pair], chooser).astype(jnp.bfloat16)
            lanes = pl.ds(couple * pair // 2, pair // 2)
            refs.weight_x[span, lanes] = split[:, : pair // 2]
            refs.weight_z[span, lanes] = split[:, pair // 2 :]

    place_col = jnp.broadcast_to(place_row.astype(jnp.float32), (LANES, rows)).T
    refs.place_col[...] = place_col
    token_copy.wait()
    side_copy.wait()

    def received(slot):
        from_home = [
            remote(
                refs.inbox.at[slot, :, direct_lanes(core)],
                refs.inbox.at[slot, :, direct_lanes(core)],
                refs.pack_send.at[0, 0],
                refs.pack_recv.at[slot, 0],
                (index, column),
            ),
            remote(
                refs.inbox.at[slot, :, shared_lanes(core, line)],
                refs.inbox.at[slot, :, shared_lanes(core, line)],
                refs.pack_send.at[0, 1],
                refs.pack_recv.at[slot, 1],
                (index, column),
            ),
        ]
        return from_home

    def across_lines(slot, arriving):
        copies = []
        for step in range(1, lines):
            from_line = lax.rem(line + lines - step, lines) if arriving else line
            lanes = shared_lanes(core, from_line)
            copies.append(
                remote(
                    refs.inbox.at[slot, :, lanes],
                    refs.inbox.at[slot, :, lanes],
                    refs.line_send.at[slot, step - 1],
                    refs.line_recv.at[slot, step - 1],
                    (index, lax.rem(line + step, lines) * 2 + core),
                )
            )
        return copies

    def across_cores(slot, arriving):
        from_core = 1 - core if arriving else core
        lanes = pl.ds(pl.multiple_of(from_core * half, LANES), half)
        return remote(
            refs.inbox.at[slot, :, lanes],
            refs.inbox.at[slot, :, lanes],
            refs.core_send.at[slot],
            refs.core_recv.at[slot],
            (index, line * 2 + 1 - core),
        )

    def answer(slot, source, target, send, recv):
        home, place = pick(homes, slot), pick(home_places, slot)
        return remote(
            source.at[slot],
            target.at[pl.ds(pl.multiple_of(place * cap, cap), cap)],
            send.at[slot],
            recv.at[place],
            (home, column),
        )

    def answer_x(slot):
        return answer(slot, refs.x_served, refs.x_back, refs.x_send, refs.x_recv)

    def answer_z(slot):
        return answer(slot, refs.z_served, refs.z_back, refs.z_send, refs.z_recv)

    @pl.loop(0, max(slot_count + 2, blocks))
    def _(turn):
        @pl.when(turn < served_count)
        def _():
            for copy in received(turn):
                copy.wait_recv()
            for copy in across_lines(turn, False):
                copy.start()

        @pl.when(turn < blocks)
        def _():
            span = pl.ds(pl.multiple_of(turn * QB, QB), QB)
            tok = refs.tok[span, :]
            place = refs.place_col[span, :]
            mine = jnp.concatenate([place] * (channels // LANES), axis=1) < 0
            for target, weight in ((refs.x, refs.weight_x), (refs.z, refs.weight_z)):
                product = dot(tok, weight[...])
                target[span, :] = jnp.where(mine, product, 0.0).astype(jnp.bfloat16)
            refs.bc[span, :] = dot(tok, refs.side[...]).astype(jnp.bfloat16)
            refs.dt_raw[span, 0 : sizes.heads] = dot(tok, refs.w_dt[...])
            lane = lax.broadcasted_iota(jnp.int32, (QB, LANES), 1).astype(jnp.float32)
            for part in range(places * cap // LANES):
                hit = jnp.where(place == lane + part * LANES, 1.0, 0.0)
                refs.unpack[span, part * LANES : (part + 1) * LANES] = hit.astype(jnp.bfloat16)

        @pl.when((turn >= 1) & (turn - 1 < served_count))
        def _():
            slot = turn - 1
            for copy in across_lines(slot, True):
                copy.wait_recv()
            across_cores(slot, False).start()

        @pl.when((turn >= 2) & (turn - 2 < served_count))
        def _():
            slot = turn - 2
            across_cores(slot, True).wait_recv()
            refs.x_served[slot] = dot(refs.inbox[slot], refs.weight_x[...]).astype(jnp.bfloat16)
            answer_x(slot).start()

    @pl.loop(0, slot_count)
    def _(slot):
        @pl.when(slot < served_count)
        def _():
            refs.z_served[slot] = dot(refs.inbox[slot], refs.weight_z[...]).astype(jnp.bfloat16)
            answer_z(slot).start()

    def back(place, buffer, recv):
        span = pl.ds(pl.multiple_of(place * cap, cap), cap)
        return remote(
            buffer.at[span], buffer.at[span], refs.x_send.at[0], recv.at[place], (index, column)
        )

    def arrived(buffer, recv):
        @pl.loop(0, places)
        def _(place):
            @pl.when(place < foreign_count)
            def _():
                back(place, buffer, recv).wait_recv()

    def combined(span, own, buffer):
        return own[span, :].astype(jnp.float32) + dot(refs.unpack[span, :], buffer[...])

    def collect_x():
        arrived(refs.x_back, refs.x_recv)

        @pl.loop(0, blocks)
        def _(block):
            span = pl.ds(pl.multiple_of(block * QB, QB), QB)
            refs.x[span, :] = combined(span, refs.x, refs.x_back).astype(jnp.bfloat16)

    def collect_z():
        arrived(refs.z_back, refs.z_recv)

    def settle():
        for place in range(places):

            @pl.when(place < foreign_count)
            def _(place=place):
                for copy in sends(place):
                    copy.wait_send()

        @pl.loop(0, slot_count)
        def _(slot):
            @pl.when(slot < served_count)
            def _():
                for copy in across_lines(slot, False):
                    copy.wait_send()
                across_cores(slot, False).wait_send()
                answer_x(slot).wait_send()
                answer_z(slot).wait_send()

    refs.collect_z = collect_z
    refs.z_of = lambda span: combined(span, refs.z, refs.z_back)
    refs.settle = settle
    collect_x()


def per_device(
    tokens, owner_slot, w_in, w_bc, w_dt, conv_x, conv_bc, dt_bias, decay_rate, d_skip, norm_gain
):
    rows, width = tokens.shape
    both = w_bc.shape[1]
    heads = dt_bias.shape[0]
    channels = w_in.shape[2] // 2
    nstate = both // 2
    blocks = rows // QB
    head_count = lax.axis_size("head")
    seq_count = lax.axis_size("seq")
    lines = head_count // 2
    cap = 2 * rows // seq_count
    foreign, _, _, served, _ = serving_plan(seq_count)
    places = max(len(line) for line in foreign)
    slots = max(len(line) for line in served)
    direct = next(
        part
        for part in (width // 8, width // 4, 0)
        if (width // 2 - part) % (LANES * lines) == 0 and part % LANES == 0
    )
    shared = (width // 2 - direct) // lines
    sizes = types.SimpleNamespace(
        seq_count=seq_count,
        head_count=head_count,
        heads=heads,
        head_size=channels // heads,
        nstate=nstate,
        cap=cap,
        lines=lines,
        places=places,
        slots=slots,
        direct=direct,
        shared=shared,
    )
    steps = len(distances(seq_count))
    in_hbm = dict(tokens=tokens, w_in=w_in, w_bc=w_bc)
    in_vmem = dict(
        owner_slot=owner_slot[None],
        w_dt=w_dt,
        conv_x=conv_x,
        conv_bc=conv_bc,
        dt_bias=dt_bias[None],
        decay_rate=decay_rate[None],
        d_skip=d_skip[None],
        norm_gain=norm_gain[None],
    )
    inputs = in_hbm | in_vmem
    f32, bf16 = jnp.float32, jnp.bfloat16
    dma = pltpu.SemaphoreType.DMA
    scratch = dict(
        tok=pltpu.VMEM((rows, width), bf16),
        own_tok=pltpu.VMEM((rows, direct + shared), bf16),
        weight=pltpu.VMEM((width, 2 * channels), bf16),
        weight_x=pltpu.VMEM((width, channels), bf16),
        weight_z=pltpu.VMEM((width, channels), bf16),
        side=pltpu.VMEM((width, both), bf16),
        packed=pltpu.VMEM((places, cap, direct + shared), bf16),
        inbox=pltpu.VMEM((slots, cap, width), bf16),
        x_served=pltpu.VMEM((slots, cap, channels), bf16),
        z_served=pltpu.VMEM((slots, cap, channels), bf16),
        x_back=pltpu.VMEM((places * cap, channels), bf16),
        z_back=pltpu.VMEM((places * cap, channels), bf16),
        unpack=pltpu.VMEM((rows, places * cap), bf16),
        place_col=pltpu.VMEM((rows, LANES), f32),
        x=pltpu.VMEM((rows, channels), bf16),
        z=pltpu.VMEM((rows, channels), bf16),
        bc=pltpu.VMEM((rows, both), bf16),
        dt_raw=pltpu.VMEM((rows, LANES), f32),
        x_rim=pltpu.VMEM((16, channels), bf16),
        bc_rim=pltpu.VMEM((16, both), bf16),
        x_wide=pltpu.VMEM((rows + 8, channels), f32),
        bc_wide=pltpu.VMEM((rows + 8, both), f32),
        x_conv=pltpu.VMEM((rows, channels), bf16),
        bc_conv=pltpu.VMEM((rows, both), bf16),
        params=pltpu.VMEM((8, LANES), f32),
        cum=pltpu.VMEM((rows, LANES), f32),
        cum_t=pltpu.VMEM((heads, rows), f32),
        dt_t=pltpu.VMEM((heads, rows), f32),
        from_start=pltpu.VMEM((rows, channels), f32),
        y=pltpu.VMEM((rows, channels), f32),
        entering=pltpu.VMEM((blocks, nstate, channels), f32),
        prior=pltpu.VMEM((blocks, 8, channels), f32),
        own_state=pltpu.VMEM((nstate, channels), f32),
        own_decay=pltpu.VMEM((8, channels), f32),
        incoming=pltpu.VMEM((nstate, channels), f32),
        incoming_decay=pltpu.VMEM((8, channels), f32),
        state_out=pltpu.VMEM((steps, nstate, channels), bf16),
        state_in=pltpu.VMEM((steps, nstate, channels), bf16),
        decay_out=pltpu.VMEM((steps, 8, channels), f32),
        decay_in=pltpu.VMEM((steps, 8, channels), f32),
        square=pltpu.VMEM((8, rows), f32),
        square_in=pltpu.VMEM((head_count - 1, 8, rows), f32),
        local=dma((5,)),
        pack_send=dma((places, 2)),
        pack_recv=dma((slots, 2)),
        line_send=dma((slots, lines - 1)),
        line_recv=dma((slots, lines - 1)),
        core_send=dma((slots,)),
        core_recv=dma((slots,)),
        x_send=dma((slots,)),
        x_recv=dma((places,)),
        z_send=dma((slots,)),
        z_recv=dma((places,)),
        rim_send=dma((2,)),
        rim_recv=dma((2,)),
        scan_send=dma((steps, 2)),
        scan_recv=dma((steps, 2)),
        norm_send=dma((head_count - 1,)),
        norm_recv=dma((head_count - 1,)),
    )
    names = tuple(inputs) + ("out",) + tuple(scratch)
    any_spec = pl.BlockSpec(memory_space=pl.ANY)
    vmem_spec = pl.BlockSpec(memory_space=pltpu.VMEM)
    return pl.pallas_call(
        functools.partial(project_kernel, sizes, names),
        out_shape=jax.ShapeDtypeStruct((rows, channels), bf16),
        in_specs=[any_spec] * len(in_hbm) + [vmem_spec] * len(in_vmem),
        out_specs=vmem_spec,
        scratch_shapes=list(scratch.values()),
        compiler_params=pltpu.CompilerParams(
            collective_id=0, has_side_effects=True, vmem_limit_bytes=62 << 20
        ),
    )(*inputs.values())


def solution(mesh):
    return jax.shard_map(
        per_device,
        mesh=mesh,
        in_specs=(
            P("seq", None),
            P("seq"),
            P("seq", None, "head"),
            P(),
            P(None, "head"),
            P(None, "head"),
            P(),
            P("head"),
            P("head"),
            P("head"),
            P("head"),
        ),
        out_specs=P("seq", "head"),
        check_vma=False,
    )
```

```python
import functools
import types

import jax
import jax.numpy as jnp
from jax import lax
from jax.experimental import pallas as pl
from jax.experimental.pallas import tpu as pltpu
from jax.sharding import PartitionSpec as P

KCONV = 4
QB = 256
MODS = 3
EPSILON = 1e-05
LANES = 128
MESH = pl.DeviceIdType.MESH
Z_PARTS = 6
Z_POINTS = (0, 2, 4, 6)
DIRECT = 2
SCAN_PARTS = 4
STATE_LOAD = 0.27
BUSY_PRICE = 0.3
WIDE = 8


def plane_width(count):
    return max(side for side in range(1, count) if count % side == 0 and side * side <= count)


def route(start, end, width):
    (plane, side), (last_plane, last_side) = divmod(start, width), divmod(end, width)
    links = []
    while (plane, side) != (last_plane, last_side):
        before = plane * width + side
        if plane != last_plane:
            plane += 1 if last_plane > plane else -1
        else:
            side += 1 if last_side > side else -1
        links.append((before, plane * width + side))
    return links


def serving_plan(count, pieces, outward):
    width = plane_width(count)
    foreign = [
        [owner * pieces + piece for piece in range(pieces) for owner in range(count) if (owner - home) % MODS]
        for home in range(count)
    ]
    groups = [(home, place) for home in range(count) for place in range(len(foreign[home]))]
    loads, busy, chosen = {}, [0] * count, {}
    for start in range(count):
        for end in (start + 1, start - 1, start + width):
            if 0 <= end < count and (end == start + width or end // width == start // width):
                loads[start, end] = STATE_LOAD * pieces

    def trips(home, server):
        return [(outward, link) for link in route(home, server, width)] + [
            (1.0, link) for link in route(server, home, width)
        ]

    def add(home, server, sign):
        busy[server] += sign
        for weight, link in trips(home, server):
            loads[link] = loads.get(link, 0.0) + sign * weight

    def price(home, server):
        total = BUSY_PRICE * ((busy[server] + 1) ** 4 - busy[server] ** 4)
        for weight, link in trips(home, server):
            before = loads.get(link, 0.0)
            total += (before + weight) ** 4 - before**4
        return total

    for _ in range(12):
        for home, place in groups:
            if (home, place) in chosen:
                add(home, chosen[home, place], -1)
            owner = foreign[home][place] // pieces
            options = [server for server in range(count) if (server - owner) % MODS == 0]
            best = min(options, key=lambda server: (round(price(home, server), 6), server))
            chosen[home, place] = best
            add(home, best, 1)
    order = [[] for _ in range(count)]
    for home, place in groups:
        first = route(home, chosen[home, place], width)[0]
        earlier = sum(route(home, chosen[home, other], width)[0] == first for other in range(place))
        order[chosen[home, place]].append((earlier, place, home))
    served = [[(home, place) for _, place, home in sorted(line)] for line in order]
    slots = {group: slot for line in served for slot, group in enumerate(line)}
    return foreign, chosen, slots, served, loads


def dot(a, b):
    return jnp.dot(a, b, preferred_element_type=jnp.float32)


def dot_nt(a, b):
    return lax.dot_general(a, b, (((1,), (1,)), ((), ())), preferred_element_type=jnp.float32)


def dot_tn(a, b):
    return lax.dot_general(a, b, (((0,), (0,)), ((), ())), preferred_element_type=jnp.float32)


def rounded(value):
    return value.astype(jnp.bfloat16).astype(jnp.float32)


def three_parts(value):
    high = rounded(value)
    middle = rounded(value - high)
    return high, middle, value - high - middle


def side_by_side(value, count):
    high, middle, low = three_parts(value)
    packed = high + pltpu.roll(middle, count, 1) + pltpu.roll(low, 2 * count, 1)
    return packed.astype(jnp.bfloat16)


def silu(value):
    return value * jax.nn.sigmoid(value)


def remote(source, target, send, recv, device):
    return pltpu.make_async_remote_copy(
        source, target, send, recv, device_id=device, device_id_type=MESH
    )


def plane_copies(sizes, refs, part):
    index, side = lax.axis_index("seq"), lax.rem(lax.axis_index("seq"), sizes.side_count)
    copies = []
    for step in range(1, sizes.side_count):
        target = (index - side + lax.rem(side + step, sizes.side_count), lax.axis_index("head"))
        for place, buffer in enumerate((refs.plane_state, refs.plane_decay)):
            copies.append(
                remote(
                    buffer.at[part, 0],
                    buffer.at[part, step],
                    refs.plane_send.at[part, step - 1, place],
                    refs.plane_recv.at[part, step - 1, place],
                    target,
                )
            )
    return copies


def chain_copy(sizes, refs, part):
    return remote(
        refs.chain_out.at[part],
        refs.chain_in.at[part],
        refs.chain_send.at[part],
        refs.chain_recv.at[part],
        (lax.axis_index("seq") + sizes.side_count, lax.axis_index("head")),
    )


def join_plane(sizes, refs, part):
    side = lax.rem(lax.axis_index("seq"), sizes.side_count)
    for copy in plane_copies(sizes, refs, part):
        copy.wait_recv()
    total = jnp.zeros(refs.ahead.shape[1:], jnp.float32)
    decay = jnp.ones(refs.ahead_decay.shape[1:], jnp.float32)
    before, before_decay = total, decay
    for place in range(sizes.side_count):
        before = jnp.where(side == place, total, before)
        before_decay = jnp.where(side == place, decay, before_decay)
        slot = lax.rem(side + sizes.side_count - place, sizes.side_count)
        factor = refs.plane_decay[part, slot]
        total = total * factor[0:1, :] + refs.plane_state[part, slot].astype(jnp.float32)
        decay = decay * factor
    refs.before[part] = before
    refs.before_decay[part] = before_decay
    refs.ahead[part] = total
    refs.ahead_decay[part] = decay


def join_chain(sizes, refs, part):
    index = lax.axis_index("seq")
    share = refs.incoming.shape[1] // SCAN_PARTS
    lanes = pl.ds(part * share, share)

    @pl.when(index < sizes.side_count)
    def _():
        refs.chain_in[part] = jnp.zeros(refs.chain_in.shape[1:], jnp.bfloat16)

    @pl.when(index >= sizes.side_count)
    def _():
        chain_copy(sizes, refs, part).wait_recv()

    @pl.when(index + sizes.side_count < sizes.seq_count)
    def _():
        entering = refs.chain_in[part].astype(jnp.float32)
        leaving = refs.ahead[part] + refs.ahead_decay[part][0:1, :] * entering
        refs.chain_out[part] = leaving.astype(jnp.bfloat16)
        chain_copy(sizes, refs, part).start()

    entering = refs.chain_in[part].astype(jnp.float32)
    refs.incoming[:, lanes] = refs.before[part] + refs.before_decay[part][0:1, :] * entering


def rim_copy(refs, which):
    source, landing = ((refs.bc, refs.bc_rim), (refs.x, refs.x_rim))[which]
    edge = landing.shape[0]
    return remote(
        source.at[pl.ds(source.shape[0] - edge, edge)],
        landing,
        refs.rim_send.at[which],
        refs.rim_recv.at[which],
        (lax.axis_index("seq") + 1, lax.axis_index("head")),
    )


def send_rim(sizes, refs, which):
    @pl.when(lax.axis_index("seq") + 1 < sizes.seq_count)
    def _():
        rim_copy(refs, which).start()


def take_rim(sizes, refs, which):
    landing, target = ((refs.bc_rim, refs.bc_wide), (refs.x_rim, refs.x_wide))[which]
    edge = landing.shape[0]
    index = lax.axis_index("seq")

    @pl.when(index > 0)
    def _():
        rim_copy(refs, which).wait_recv()
        target[0:WIDE, :] = landing[...].astype(jnp.float32)[edge - WIDE :, :]

    @pl.when(index == 0)
    def _():
        target[0:WIDE, :] = jnp.zeros((WIDE, target.shape[1]), jnp.float32)


def convolved(source, weights, block):
    taps = weights.shape[0]
    total = jnp.zeros((QB, source.shape[1]), jnp.float32)
    for tap in range(taps):
        shifted = source[pl.ds(block * QB + WIDE - taps + 1 + tap, QB), :]
        total = total + weights[tap : tap + 1, :] * shifted
    return silu(total).astype(jnp.bfloat16)


def spreader(sizes, channels):
    row = lax.broadcasted_iota(jnp.int32, (LANES, channels), 0)
    col = lax.broadcasted_iota(jnp.int32, (LANES, channels), 1)
    wanted = (row % sizes.heads == col // sizes.head_size) & (row < 3 * sizes.heads)
    return jnp.where(wanted, 1.0, 0.0).astype(jnp.bfloat16)


def prepare_params(sizes, refs):
    heads = sizes.heads
    refs.params[...] = jnp.zeros_like(refs.params)
    refs.params[0:1, 0:heads] = refs.dt_bias[...]
    refs.params[1:2, 0:heads] = refs.decay_rate[...]
    refs.params[2:3, 0:heads] = refs.d_skip[...]
    refs.spread[...] = spreader(sizes, refs.x.shape[1])
    refs.skip_row[...] = dot(side_by_side(refs.params[...], heads), refs.spread[...])


def side_block(sizes, refs, block):
    heads = sizes.heads
    span = pl.ds(block * QB, QB)
    lane = lax.broadcasted_iota(jnp.int32, (1, LANES), 1)
    row = lax.broadcasted_iota(jnp.int32, (QB, QB), 0)
    col = lax.broadcasted_iota(jnp.int32, (QB, QB), 1)
    lower = jnp.where(row >= col, 1.0, 0.0).astype(jnp.bfloat16)
    step_dt = jax.nn.softplus(refs.dt_raw[span, :] + refs.params[0:1, :])
    log_decay = jnp.where(lane < heads, -step_dt * refs.params[1:2, :], 0.0)
    sums = dot(lower, side_by_side(log_decay, heads))
    cum = sums + pltpu.roll(sums, LANES - heads, 1) + pltpu.roll(sums, LANES - 2 * heads, 1)
    cum = jnp.where(lane < heads, cum, 0.0)
    refs.cum[span, :] = cum
    refs.cum_t[:, span] = cum.T[0:heads, :]
    refs.dt_t[:, span] = step_dt.T[0:heads, :]
    last = cum[QB - 1 : QB, :]
    to_end = jnp.where(lane < heads, jnp.exp(last - cum) * step_dt, 0.0)
    from_start = jnp.where(lane < heads, jnp.exp(cum), 0.0)
    refs.to_end[span, :] = dot(side_by_side(to_end, heads), refs.spread[...])
    refs.from_start[span, :] = dot(side_by_side(from_start, heads), refs.spread[...])
    if block > 0:
        side_conv(sizes, refs, block)


def side_conv(sizes, refs, block):
    if block == 0:
        take_rim(sizes, refs, 0)
    refs.bc_conv[pl.ds(block * QB, QB), :] = convolved(refs.bc_wide, refs.conv_bc, block)


def finish_body(sizes, refs):
    index, column = lax.axis_index("seq"), lax.axis_index("head")
    seq_count, head_count = sizes.seq_count, sizes.head_count
    heads, head_size, nstate = sizes.heads, sizes.head_size, sizes.nstate
    rows, channels = refs.x.shape
    blocks = rows // QB
    share = channels // SCAN_PARTS

    refs.collect_x()
    for block in [*range(1, blocks), 0]:
        span = pl.ds(block * QB, QB)
        if block == 0:
            side_conv(sizes, refs, 0)
            take_rim(sizes, refs, 1)
        x_blk = convolved(refs.x_wide, refs.conv_x, block)
        refs.x_conv[span, :] = x_blk
        weighted = (x_blk.astype(jnp.float32) * refs.to_end[span, :]).astype(jnp.bfloat16)
        refs.entering[block] = dot_tn(refs.bc_conv[span, 0:nstate], weighted)
    carried = jnp.zeros((nstate, channels), jnp.float32)
    carried_decay = jnp.ones((1, channels), jnp.float32)
    for block in range(blocks):
        added = refs.entering[block]
        refs.entering[block] = carried
        refs.prior[block] = jnp.broadcast_to(carried_decay, refs.prior.shape[1:])
        decay = refs.from_start[pl.ds((block + 1) * QB - 1, 1), :]
        carried = carried * decay + added
        carried_decay = carried_decay * decay
    for part in range(SCAN_PARTS):
        lanes = slice(part * share, (part + 1) * share)
        refs.plane_state[part, 0] = carried[:, lanes].astype(jnp.bfloat16)
        refs.plane_decay[part, 0] = jnp.broadcast_to(carried_decay[:, lanes], (8, share))
        for copy in plane_copies(sizes, refs, part):
            copy.start()
    refs.send_z(2)

    half = 2 * head_size
    pair_lane = lax.broadcasted_iota(jnp.int32, (QB, half), 1)
    row = lax.broadcasted_iota(jnp.int32, (QB, QB), 0)
    col = lax.broadcasted_iota(jnp.int32, (QB, QB), 1)
    causal = row >= col

    @pl.loop(0, blocks)
    def _(block):
        begin = pl.multiple_of(block * QB, QB)
        span = pl.ds(begin, QB)
        scores = dot_nt(refs.bc_conv[span, nstate:], refs.bc_conv[span, 0:nstate])
        for pair in range(heads // 2):
            lanes = pl.ds(pair * half, half)
            x_pair = refs.x_conv[span, lanes]
            total = jnp.zeros((QB, half), jnp.float32)
            for which in range(2):
                head = 2 * pair + which
                gap = refs.cum[span, head : head + 1] - refs.cum_t[head : head + 1, span]
                factor = jnp.exp(jnp.where(causal, gap, -jnp.inf))
                mixing = (scores * factor * refs.dt_t[head : head + 1, span]).astype(jnp.bfloat16)
                mine = (pair_lane >= head_size) if which else (pair_lane < head_size)
                total = total + dot(mixing, jnp.where(mine, x_pair, jnp.zeros_like(x_pair)))
            refs.y[span, lanes] = total + refs.skip_row[2:3, lanes] * x_pair.astype(jnp.float32)

    def gates():
        refs.collect_z()

        @pl.loop(0, blocks)
        def _(block):
            span = pl.ds(pl.multiple_of(block * QB, QB), QB)
            refs.x_wide[span, :] = silu(refs.z_of(span))

    for part in range(SCAN_PARTS):
        join_plane(sizes, refs, part)

    @pl.when(index + sizes.side_count >= seq_count)
    def _():
        refs.send_z(3)
        gates()

    for part in range(SCAN_PARTS):
        join_chain(sizes, refs, part)

    @pl.when(index + sizes.side_count < seq_count)
    def _():
        refs.send_z(3)
        gates()

    ones = jnp.ones((8, LANES), jnp.bfloat16)

    @pl.loop(0, blocks)
    def _(block):
        begin = pl.multiple_of(block * QB, QB)
        span = pl.ds(begin, QB)
        state = refs.entering[block] + refs.incoming[...] * refs.prior[block][0:1, :]
        high, middle, low = three_parts(state)
        c_blk = refs.bc_conv[span, nstate:]
        outside = dot(c_blk, high.astype(jnp.bfloat16)) + dot(c_blk, middle.astype(jnp.bfloat16))
        outside = outside + dot(c_blk, low.astype(jnp.bfloat16))
        value = (refs.y[span, :] + refs.from_start[span, :] * outside) * refs.x_wide[span, :]
        refs.y[span, :] = value
        squares = value * value
        folded = squares[:, 0:LANES]
        for part in range(1, channels // LANES):
            folded = folded + squares[:, part * LANES : (part + 1) * LANES]
        first, second, third = three_parts(folded)
        total = dot_nt(ones, first.astype(jnp.bfloat16)) + dot_nt(ones, second.astype(jnp.bfloat16))
        total = total + dot_nt(ones, third.astype(jnp.bfloat16))
        for part in range(QB // LANES):
            line = total[0:1, part * LANES : (part + 1) * LANES]
            refs.square[pl.ds(block * (QB // LANES) + part, 1), :] = line

    def shares():
        return [
            remote(
                refs.square,
                refs.square_in.at[step - 1],
                refs.norm_send.at[step - 1],
                refs.norm_recv.at[step - 1],
                (index, lax.rem(column + step, head_count)),
            )
            for step in range(1, head_count)
        ]

    for copy in shares():
        copy.start()
    for copy in shares():
        copy.wait_recv()
    total = refs.square[...]
    for step in range(1, head_count):
        total = total + refs.square_in[step - 1]
    scale = lax.rsqrt(total / (head_count * channels) + EPSILON)
    lines = rows // LANES
    line_of = lax.broadcasted_iota(jnp.int32, (lines, channels), 0)
    scales = [part.astype(jnp.bfloat16) for part in three_parts(scale)]
    for line in range(lines):
        span = pl.ds(line * LANES, LANES)
        chosen = jnp.where(line_of == line, 1.0, 0.0).astype(jnp.bfloat16)
        wide_scale = dot_tn(scales[0], chosen) + dot_tn(scales[1], chosen) + dot_tn(scales[2], chosen)
        refs.out[span, :] = (refs.y[span, :] * wide_scale * refs.norm_gain[...]).astype(jnp.bfloat16)

    for copy in shares():
        copy.wait_send()

    @pl.when(index + 1 < seq_count)
    def _():
        for which in range(2):
            rim_copy(refs, which).wait_send()

    for part in range(SCAN_PARTS):
        for copy in plane_copies(sizes, refs, part):
            copy.wait_send()

        @pl.when(index + sizes.side_count < seq_count)
        def _(part=part):
            chain_copy(sizes, refs, part).wait_send()

    refs.settle()


def pick(options, which):
    value = options[0]
    for place in range(1, len(options)):
        value = jnp.where(which == place, options[place], value)
    return value


def padded(lines, length):
    return [list(line) + [0] * (length - len(line)) for line in lines]


def project_kernel(sizes, names, *all_refs):
    refs = types.SimpleNamespace(**dict(zip(names, all_refs)))
    index, column = lax.axis_index("seq"), lax.axis_index("head")
    barrier = pltpu.get_barrier_semaphore()
    for step in range(1, sizes.seq_count):
        other = lax.rem(index + step, sizes.seq_count)
        pl.semaphore_signal(barrier, inc=1, device_id=(other, column), device_id_type=MESH)
    for step in range(1, sizes.head_count):
        other = lax.rem(column + step, sizes.head_count)
        pl.semaphore_signal(barrier, inc=1, device_id=(index, other), device_id_type=MESH)
    project_body(sizes, refs, barrier)
    finish_body(sizes, refs)


def project_body(sizes, refs, barrier):
    index, column = lax.axis_index("seq"), lax.axis_index("head")
    seq_count, head_count = sizes.seq_count, sizes.head_count
    cap, direct, shared, lines = sizes.cap, sizes.direct, sizes.shared, sizes.lines
    places, slot_count = sizes.places, sizes.slots
    rows, channels = refs.x.shape
    width = refs.tok.shape[1]
    blocks = rows // QB
    core, line = lax.rem(column, 2), column // 2
    half = width // 2
    foreign, chosen, slot_of, served, _ = serving_plan(seq_count, sizes.pieces, sizes.outward)
    foreign_count = pick([len(line_) for line_ in foreign], index)
    served_count = pick([len(line_) for line_ in served], index)
    server_of, landing = [], []
    for place in range(places):
        server_of.append(pick([chosen.get((home, place), 0) for home in range(seq_count)], index))
        landing.append(pick([slot_of.get((home, place), 0) for home in range(seq_count)], index))
    homes, home_places = [], []
    for slot in range(slot_count):
        homes.append(pick([line_[slot][0] if slot < len(line_) else 0 for line_ in served], index))
        home_places.append(pick([line_[slot][1] if slot < len(line_) else 0 for line_ in served], index))

    def direct_lanes(which):
        return pl.ds(pl.multiple_of(which * half, LANES), direct)

    def shared_lanes(which, from_line):
        return pl.ds(pl.multiple_of(which * half + direct + from_line * shared, LANES), shared)

    own_copies = [
        pltpu.make_async_copy(
            refs.tokens.at[:, shared_lanes(core, line)],
            refs.own_tok.at[:, pl.ds(direct, shared)],
            refs.local.at[1],
        )
    ]
    if direct:
        own_copies.append(
            pltpu.make_async_copy(
                refs.tokens.at[:, direct_lanes(core)], refs.own_tok.at[:, pl.ds(0, direct)], refs.local.at[0]
            )
        )
    weight_copy = pltpu.make_async_copy(refs.w_in.at[0], refs.weight, refs.local.at[2])
    token_copy = pltpu.make_async_copy(refs.tokens, refs.tok, refs.local.at[3])
    side_copy = pltpu.make_async_copy(refs.w_bc, refs.side, refs.local.at[4])
    for copy in own_copies + [weight_copy, token_copy, side_copy]:
        copy.start()

    slots = refs.owner_slot[...]
    place_row = jnp.full(slots.shape, -1, jnp.int32)
    for group in range(seq_count * sizes.pieces):
        place = pick([line_.index(group) if group in line_ else -1 for line_ in foreign], index)
        within = (slots >= group * cap) & (slots < (group + 1) * cap)
        moved = jnp.where(place >= 0, slots + (place - group) * cap, -1)
        place_row = jnp.where(within, moved, place_row)

    for place in range(min(len(line_) for line_ in foreign), places):

        @pl.when(place >= foreign_count)
        def _(place=place):
            span = pl.ds(place * cap, cap)
            refs.x_back[span, :] = jnp.zeros((cap, channels), jnp.bfloat16)
            refs.z_back[span, :] = jnp.zeros((cap, channels), jnp.bfloat16)

    def sends(place):
        server = (server_of[place], column)
        slot = landing[place]
        kinds = [(1, pl.ds(direct, shared), shared_lanes(core, line))]
        if direct:
            kinds.append((0, pl.ds(0, direct), direct_lanes(core)))
        return [
            remote(
                refs.packed.at[place, :, source],
                refs.inbox.at[slot, :, target],
                refs.pack_send.at[place, kind],
                refs.pack_recv.at[slot, kind],
                server,
            )
            for kind, source, target in kinds
        ]

    for copy in own_copies:
        copy.wait()
    sublane = lax.broadcasted_iota(jnp.int32, (cap, rows), 0)
    for place in range(places):

        @pl.when(place < foreign_count)
        def _(place=place):
            chosen_rows = jnp.where(place_row == sublane + place * cap, 1.0, 0.0).astype(jnp.bfloat16)
            refs.packed[place] = dot(chosen_rows, refs.own_tok[...]).astype(jnp.bfloat16)
            if place == 0:
                pl.semaphore_wait(barrier, seq_count + head_count - 2)
            for copy in sends(place):
                copy.start()

    prepare_params(sizes, refs)

    pair = 4 * sizes.head_size
    source = lax.broadcasted_iota(jnp.int32, (pair, pair), 0)
    target = lax.broadcasted_iota(jnp.int32, (pair, pair), 1)
    size = sizes.head_size
    from_z = target // (2 * size)
    wanted = (target % (2 * size)) // size * (2 * size) + from_z * size + target % size
    chooser = jnp.where(source == wanted, 1.0, 0.0).astype(jnp.bfloat16)
    weight_copy.wait()

    @pl.loop(0, width // QB)
    def _(part):
        span = pl.ds(pl.multiple_of(part * QB, QB), QB)
        for couple in range(sizes.heads // 2):
            split = dot(refs.weight[span, couple * pair : (couple + 1) * pair], chooser).astype(jnp.bfloat16)
            lanes = pl.ds(couple * pair // 2, pair // 2)
            refs.weight_x[span, lanes] = split[:, : pair // 2]
            refs.weight_z[span, lanes] = split[:, pair // 2 :]

    place_col = jnp.broadcast_to(place_row.astype(jnp.float32), (LANES, rows)).T
    refs.place_col[...] = place_col
    token_copy.wait()
    side_copy.wait()

    def received(slot):
        kinds = [(1, shared_lanes(core, line))] + ([(0, direct_lanes(core))] if direct else [])
        return [
            remote(
                refs.inbox.at[slot, :, lanes],
                refs.inbox.at[slot, :, lanes],
                refs.pack_send.at[0, kind],
                refs.pack_recv.at[slot, kind],
                (index, column),
            )
            for kind, lanes in kinds
        ]

    def across_lines(slot, arriving):
        copies = []
        for step in range(1, lines):
            from_line = lax.rem(line + lines - step, lines) if arriving else line
            lanes = shared_lanes(core, from_line)
            copies.append(
                remote(
                    refs.inbox.at[slot, :, lanes],
                    refs.inbox.at[slot, :, lanes],
                    refs.line_send.at[slot, step - 1],
                    refs.line_recv.at[slot, step - 1],
                    (index, lax.rem(line + step, lines) * 2 + core),
                )
            )
        return copies

    def across_cores(slot, arriving):
        from_core = 1 - core if arriving else core
        lanes = pl.ds(pl.multiple_of(from_core * half, LANES), half)
        return remote(
            refs.inbox.at[slot, :, lanes],
            refs.inbox.at[slot, :, lanes],
            refs.core_send.at[slot],
            refs.core_recv.at[slot],
            (index, line * 2 + 1 - core),
        )

    def answer(slot, source, target, send, recv):
        home, place = pick(homes, slot), pick(home_places, slot)
        return remote(
            source.at[slot],
            target.at[pl.ds(pl.multiple_of(place * cap, cap), cap)],
            send.at[slot],
            recv.at[place],
            (home, column),
        )

    def answer_x(slot):
        return answer(slot, refs.x_served, refs.x_back, refs.x_send, refs.x_recv)

    def answer_z(slot):
        return answer(slot, refs.z_served, refs.z_back, refs.z_send, refs.z_recv)

    @pl.loop(0, max(slot_count + 2, 2 * blocks))
    def _(turn):
        @pl.when(turn < served_count)
        def _():
            for copy in received(turn):
                copy.wait_recv()
            for copy in across_lines(turn, False):
                copy.start()

        @pl.when(turn < blocks)
        def _():
            span = pl.ds(pl.multiple_of(turn * QB, QB), QB)
            tok = refs.tok[span, :]
            place = refs.place_col[span, :]
            mine = jnp.concatenate([place] * (channels // LANES), axis=1) < 0
            product = dot(tok, refs.weight_x[...])
            refs.x[span, :] = jnp.where(mine, product, 0.0).astype(jnp.bfloat16)
            side = dot(tok, refs.side[...]).astype(jnp.bfloat16)
            refs.bc[span, :] = side
            wide = pl.ds(pl.multiple_of(turn * QB + WIDE, WIDE), QB)
            refs.bc_wide[wide, :] = side.astype(jnp.float32)
            refs.dt_raw[span, 0 : sizes.heads] = dot_nt(tok, refs.w_dt_t[...])
            lane = lax.broadcasted_iota(jnp.int32, (QB, LANES), 1).astype(jnp.float32)
            for part in range(places * cap // LANES):
                hit = jnp.where(place == lane + part * LANES, 1.0, 0.0)
                refs.unpack[span, part * LANES : (part + 1) * LANES] = hit.astype(jnp.bfloat16)

        for block in range(blocks):

            @pl.when(turn == blocks + (block + blocks - 1) % blocks)
            def _(block=block):
                if block == min(1, blocks - 1):
                    send_rim(sizes, refs, 0)
                side_block(sizes, refs, block)

        @pl.when((turn >= 1) & (turn - 1 < served_count))
        def _():
            slot = turn - 1
            for copy in across_lines(slot, True):
                copy.wait_recv()
            across_cores(slot, False).start()

        @pl.when((turn >= 2) & (turn - 2 < served_count))
        def _():
            slot = turn - 2
            across_cores(slot, True).wait_recv()
            refs.x_served[slot] = dot(refs.inbox[slot], refs.weight_x[...]).astype(jnp.bfloat16)
            answer_x(slot).start()

    @pl.loop(0, slot_count)
    def _(slot):
        @pl.when(slot < served_count)
        def _():
            refs.z_served[slot] = dot(refs.inbox[slot], refs.weight_z[...]).astype(jnp.bfloat16)

    def send_z(point):
        start, stop = (
            slot_count * Z_POINTS[min(edge, len(Z_POINTS) - 1)] // Z_PARTS for edge in (point, point + 1)
        )

        @pl.loop(start, stop)
        def _(slot):
            @pl.when(slot < served_count)
            def _():
                answer_z(slot).start()

    refs.send_z = send_z
    send_z(0)

    def back(place, buffer, recv):
        span = pl.ds(pl.multiple_of(place * cap, cap), cap)
        return remote(
            buffer.at[span], buffer.at[span], refs.x_send.at[0], recv.at[place], (index, column)
        )

    def arrived(buffer, recv):
        @pl.loop(0, places)
        def _(place):
            @pl.when(place < foreign_count)
            def _():
                back(place, buffer, recv).wait_recv()

    def combined(span, own, buffer):
        return own + dot(refs.unpack[span, :], buffer[...])

    def z_of(span):
        place = refs.place_col[span, :]
        mine = jnp.concatenate([place] * (channels // LANES), axis=1) < 0
        own = jnp.where(mine, dot(refs.tok[span, :], refs.weight_z[...]), 0.0)
        return rounded(combined(span, own, refs.z_back))

    def collect_x():
        arrived(refs.x_back, refs.x_recv)

        for block in [blocks - 1, *range(blocks - 1)]:
            span = pl.ds(block * QB, QB)
            merged = combined(span, refs.x[span, :].astype(jnp.float32), refs.x_back).astype(jnp.bfloat16)
            refs.x_wide[pl.ds(block * QB + WIDE, QB), :] = merged.astype(jnp.float32)
            if block == blocks - 1:
                refs.x[span, :] = merged
                send_rim(sizes, refs, 1)
                send_z(1)

    def collect_z():
        arrived(refs.z_back, refs.z_recv)

    def settle():
        for place in range(places):

            @pl.when(place < foreign_count)
            def _(place=place):
                for copy in sends(place):
                    copy.wait_send()

        @pl.loop(0, slot_count)
        def _(slot):
            @pl.when(slot < served_count)
            def _():
                for copy in across_lines(slot, False):
                    copy.wait_send()
                across_cores(slot, False).wait_send()
                answer_x(slot).wait_send()
                answer_z(slot).wait_send()

    refs.collect_z = collect_z
    refs.z_of = z_of
    refs.settle = settle
    refs.collect_x = collect_x


def per_device(
    tokens, owner_slot, w_in, w_bc, w_dt, conv_x, conv_bc, dt_bias, decay_rate, d_skip, norm_gain
):
    rows, width = tokens.shape
    both = w_bc.shape[1]
    heads = dt_bias.shape[0]
    channels = w_in.shape[2] // 2
    nstate = both // 2
    blocks = rows // QB
    head_count = lax.axis_size("head")
    seq_count = lax.axis_size("seq")
    lines = head_count // 2
    cap = min(2 * rows // seq_count, LANES)
    pieces = 2 * rows // seq_count // cap
    direct = next(
        part
        for part in (DIRECT * LANES, width // 4)
        if (width // 2 - part) % (LANES * lines) == 0 and part % LANES == 0
    )
    shared = (width // 2 - direct) // lines
    outward = 2 * (direct + shared) / (4 * channels)
    foreign, _, _, served, _ = serving_plan(seq_count, pieces, outward)
    places = max(len(line) for line in foreign)
    slots = max(len(line) for line in served)
    sizes = types.SimpleNamespace(
        seq_count=seq_count,
        head_count=head_count,
        heads=heads,
        head_size=channels // heads,
        nstate=nstate,
        cap=cap,
        pieces=pieces,
        outward=outward,
        side_count=plane_width(seq_count),
        lines=lines,
        places=places,
        slots=slots,
        direct=direct,
        shared=shared,
    )
    side_count = plane_width(seq_count)
    share = channels // SCAN_PARTS
    in_hbm = dict(tokens=tokens, w_in=w_in, w_bc=w_bc)
    in_vmem = dict(
        owner_slot=owner_slot[None],
        w_dt_t=w_dt.T,
        conv_x=conv_x,
        conv_bc=conv_bc,
        dt_bias=dt_bias[None],
        decay_rate=decay_rate[None],
        d_skip=d_skip[None],
        norm_gain=norm_gain[None],
    )
    inputs = in_hbm | in_vmem
    f32, bf16 = jnp.float32, jnp.bfloat16
    dma = pltpu.SemaphoreType.DMA
    scratch = dict(
        tok=pltpu.VMEM((rows, width), bf16),
        own_tok=pltpu.VMEM((rows, direct + shared), bf16),
        weight=pltpu.VMEM((width, 2 * channels), bf16),
        weight_x=pltpu.VMEM((width, channels), bf16),
        weight_z=pltpu.VMEM((width, channels), bf16),
        side=pltpu.VMEM((width, both), bf16),
        packed=pltpu.VMEM((places, cap, direct + shared), bf16),
        inbox=pltpu.VMEM((slots, cap, width), bf16),
        x_served=pltpu.VMEM((slots, cap, channels), bf16),
        z_served=pltpu.VMEM((slots, cap, channels), bf16),
        x_back=pltpu.VMEM((places * cap, channels), bf16),
        z_back=pltpu.VMEM((places * cap, channels), bf16),
        unpack=pltpu.VMEM((rows, places * cap), bf16),
        place_col=pltpu.VMEM((rows, LANES), f32),
        x=pltpu.VMEM((rows, channels), bf16),
        bc=pltpu.VMEM((rows, both), bf16),
        dt_raw=pltpu.VMEM((rows, LANES), f32),
        x_rim=pltpu.VMEM((16, channels), bf16),
        bc_rim=pltpu.VMEM((16, both), bf16),
        x_wide=pltpu.VMEM((rows + WIDE, channels), f32),
        bc_wide=pltpu.VMEM((rows + WIDE, both), f32),
        x_conv=pltpu.VMEM((rows, channels), bf16),
        bc_conv=pltpu.VMEM((rows, both), bf16),
        params=pltpu.VMEM((8, LANES), f32),
        spread=pltpu.VMEM((LANES, channels), bf16),
        skip_row=pltpu.VMEM((8, channels), f32),
        to_end=pltpu.VMEM((rows, channels), f32),
        cum=pltpu.VMEM((rows, LANES), f32),
        cum_t=pltpu.VMEM((heads, rows), f32),
        dt_t=pltpu.VMEM((heads, rows), f32),
        from_start=pltpu.VMEM((rows, channels), f32),
        y=pltpu.VMEM((rows, channels), f32),
        entering=pltpu.VMEM((blocks, nstate, channels), f32),
        prior=pltpu.VMEM((blocks, 8, channels), f32),
        incoming=pltpu.VMEM((nstate, channels), f32),
        before=pltpu.VMEM((SCAN_PARTS, nstate, share), f32),
        before_decay=pltpu.VMEM((SCAN_PARTS, 8, share), f32),
        ahead=pltpu.VMEM((SCAN_PARTS, nstate, share), f32),
        ahead_decay=pltpu.VMEM((SCAN_PARTS, 8, share), f32),
        plane_state=pltpu.VMEM((SCAN_PARTS, side_count, nstate, share), bf16),
        plane_decay=pltpu.VMEM((SCAN_PARTS, side_count, 8, share), f32),
        chain_in=pltpu.VMEM((SCAN_PARTS, nstate, share), bf16),
        chain_out=pltpu.VMEM((SCAN_PARTS, nstate, share), bf16),
        square=pltpu.VMEM((rows // LANES, LANES), f32),
        square_in=pltpu.VMEM((head_count - 1, rows // LANES, LANES), f32),
        local=dma((5,)),
        pack_send=dma((places, 2)),
        pack_recv=dma((slots, 2)),
        line_send=dma((slots, lines - 1)),
        line_recv=dma((slots, lines - 1)),
        core_send=dma((slots,)),
        core_recv=dma((slots,)),
        x_send=dma((slots,)),
        x_recv=dma((places,)),
        z_send=dma((slots,)),
        z_recv=dma((places,)),
        rim_send=dma((2,)),
        rim_recv=dma((2,)),
        plane_send=dma((SCAN_PARTS, side_count - 1, 2)),
        plane_recv=dma((SCAN_PARTS, side_count - 1, 2)),
        chain_send=dma((SCAN_PARTS,)),
        chain_recv=dma((SCAN_PARTS,)),
        norm_send=dma((head_count - 1,)),
        norm_recv=dma((head_count - 1,)),
    )
    names = tuple(inputs) + ("out",) + tuple(scratch)
    any_spec = pl.BlockSpec(memory_space=pl.ANY)
    vmem_spec = pl.BlockSpec(memory_space=pltpu.VMEM)
    return pl.pallas_call(
        functools.partial(project_kernel, sizes, names),
        out_shape=jax.ShapeDtypeStruct((rows, channels), bf16),
        in_specs=[any_spec] * len(in_hbm) + [vmem_spec] * len(in_vmem),
        out_specs=vmem_spec,
        scratch_shapes=list(scratch.values()),
        compiler_params=pltpu.CompilerParams(
            collective_id=0, has_side_effects=True, vmem_limit_bytes=62 << 20
        ),
    )(*inputs.values())


def solution(mesh):
    return jax.shard_map(
        per_device,
        mesh=mesh,
        in_specs=(
            P("seq", None),
            P("seq"),
            P("seq", None, "head"),
            P(),
            P(None, "head"),
            P(None, "head"),
            P(),
            P("head"),
            P("head"),
            P("head"),
            P("head"),
        ),
        out_specs=P("seq", "head"),
        check_vma=False,
    )
```

```python
import functools
import types

import jax
import jax.numpy as jnp
from jax import lax
from jax.experimental import pallas as pl
from jax.experimental.pallas import tpu as pltpu
from jax.sharding import PartitionSpec as P

KCONV = 4
QB = 256
MODS = 3
EPSILON = 1e-05
LANES = 128
MESH = pl.DeviceIdType.MESH
Z_PARTS = 12
Z_POINTS = (4, 6, 6, 10)
BATCHES = 2
Z_EACH = 2
DIRECT = 2
SCAN_PARTS = 4
STATE_LOAD = 0.27
BUSY_PRICE = 0.3
WIDE = 8


def plane_width(count):
    return max(side for side in range(1, count) if count % side == 0 and side * side <= count)


def route(start, end, width):
    (plane, side), (last_plane, last_side) = divmod(start, width), divmod(end, width)
    links = []
    while (plane, side) != (last_plane, last_side):
        before = plane * width + side
        if plane != last_plane:
            plane += 1 if last_plane > plane else -1
        else:
            side += 1 if last_side > side else -1
        links.append((before, plane * width + side))
    return links


def serving_plan(count, pieces, outward):
    width = plane_width(count)
    foreign = [
        [owner * pieces + piece for piece in range(pieces) for owner in range(count) if (owner - home) % MODS]
        for home in range(count)
    ]
    groups = [(home, place) for home in range(count) for place in range(len(foreign[home]))]
    loads, busy, chosen = {}, [0] * count, {}
    for start in range(count):
        for end in (start + 1, start - 1, start + width):
            if 0 <= end < count and (end == start + width or end // width == start // width):
                loads[start, end] = STATE_LOAD * pieces

    def trips(home, server):
        return [(outward, link) for link in route(home, server, width)] + [
            (1.0, link) for link in route(server, home, width)
        ]

    def add(home, server, sign):
        busy[server] += sign
        for weight, link in trips(home, server):
            loads[link] = loads.get(link, 0.0) + sign * weight

    def price(home, server):
        total = BUSY_PRICE * ((busy[server] + 1) ** 4 - busy[server] ** 4)
        for weight, link in trips(home, server):
            before = loads.get(link, 0.0)
            total += (before + weight) ** 4 - before**4
        return total

    for _ in range(12):
        for home, place in groups:
            if (home, place) in chosen:
                add(home, chosen[home, place], -1)
            owner = foreign[home][place] // pieces
            options = [server for server in range(count) if (server - owner) % MODS == 0]
            best = min(options, key=lambda server: (round(price(home, server), 6), server))
            chosen[home, place] = best
            add(home, best, 1)
    order = [[] for _ in range(count)]
    for home, place in groups:
        first = route(home, chosen[home, place], width)[0]
        earlier = sum(route(home, chosen[home, other], width)[0] == first for other in range(place))
        order[chosen[home, place]].append((earlier, place, home))
    served = [[(home, place) for _, place, home in sorted(line)] for line in order]
    slots = {group: slot for line in served for slot, group in enumerate(line)}
    return foreign, chosen, slots, served, loads


def dot(a, b):
    return jnp.dot(a, b, preferred_element_type=jnp.float32)


def dot_nt(a, b):
    return lax.dot_general(a, b, (((1,), (1,)), ((), ())), preferred_element_type=jnp.float32)


def dot_tn(a, b):
    return lax.dot_general(a, b, (((0,), (0,)), ((), ())), preferred_element_type=jnp.float32)


def rounded(value):
    return value.astype(jnp.bfloat16).astype(jnp.float32)


def three_parts(value):
    high = rounded(value)
    middle = rounded(value - high)
    return high, middle, value - high - middle


def side_by_side(value, count):
    high, middle, low = three_parts(value)
    packed = high + pltpu.roll(middle, count, 1) + pltpu.roll(low, 2 * count, 1)
    return packed.astype(jnp.bfloat16)


def silu(value):
    return value * jax.nn.sigmoid(value)


def remote(source, target, send, recv, device):
    return pltpu.make_async_remote_copy(
        source, target, send, recv, device_id=device, device_id_type=MESH
    )


def plane_copies(sizes, refs, part):
    index, side = lax.axis_index("seq"), lax.rem(lax.axis_index("seq"), sizes.side_count)
    copies = []
    for step in range(1, sizes.side_count):
        target = (index - side + lax.rem(side + step, sizes.side_count), lax.axis_index("head"))
        for place, buffer in enumerate((refs.plane_state, refs.plane_decay)):
            copies.append(
                remote(
                    buffer.at[part, 0],
                    buffer.at[part, step],
                    refs.plane_send.at[part, step - 1, place],
                    refs.plane_recv.at[part, step - 1, place],
                    target,
                )
            )
    return copies


def chain_copy(sizes, refs, part):
    return remote(
        refs.chain_out.at[part],
        refs.chain_in.at[part],
        refs.chain_send.at[part],
        refs.chain_recv.at[part],
        (lax.axis_index("seq") + sizes.side_count, lax.axis_index("head")),
    )


def join_plane(sizes, refs, part):
    side = lax.rem(lax.axis_index("seq"), sizes.side_count)
    for copy in plane_copies(sizes, refs, part):
        copy.wait_recv()
    total = jnp.zeros(refs.ahead.shape[1:], jnp.float32)
    decay = jnp.ones(refs.ahead_decay.shape[1:], jnp.float32)
    before, before_decay = total, decay
    for place in range(sizes.side_count):
        before = jnp.where(side == place, total, before)
        before_decay = jnp.where(side == place, decay, before_decay)
        slot = lax.rem(side + sizes.side_count - place, sizes.side_count)
        factor = refs.plane_decay[part, slot]
        total = total * factor[0:1, :] + refs.plane_state[part, slot].astype(jnp.float32)
        decay = decay * factor
    refs.before[part] = before
    refs.before_decay[part] = before_decay
    refs.ahead[part] = total
    refs.ahead_decay[part] = decay


def join_chain(sizes, refs, part):
    index = lax.axis_index("seq")
    share = refs.incoming.shape[1] // SCAN_PARTS
    lanes = pl.ds(part * share, share)

    @pl.when(index < sizes.side_count)
    def _():
        refs.chain_in[part] = jnp.zeros(refs.chain_in.shape[1:], jnp.bfloat16)

    @pl.when(index >= sizes.side_count)
    def _():
        chain_copy(sizes, refs, part).wait_recv()

    @pl.when(index + sizes.side_count < sizes.seq_count)
    def _():
        entering = refs.chain_in[part].astype(jnp.float32)
        leaving = refs.ahead[part] + refs.ahead_decay[part][0:1, :] * entering
        refs.chain_out[part] = leaving.astype(jnp.bfloat16)
        chain_copy(sizes, refs, part).start()

    entering = refs.chain_in[part].astype(jnp.float32)
    refs.incoming[:, lanes] = refs.before[part] + refs.before_decay[part][0:1, :] * entering


def rim_copy(refs, which):
    source, landing = ((refs.bc, refs.bc_rim), (refs.x, refs.x_rim))[which]
    edge = landing.shape[0]
    return remote(
        source.at[pl.ds(source.shape[0] - edge, edge)],
        landing,
        refs.rim_send.at[which],
        refs.rim_recv.at[which],
        (lax.axis_index("seq") + 1, lax.axis_index("head")),
    )


def send_rim(sizes, refs, which):
    @pl.when(lax.axis_index("seq") + 1 < sizes.seq_count)
    def _():
        rim_copy(refs, which).start()


def take_rim(sizes, refs, which):
    landing, target = ((refs.bc_rim, refs.bc_wide), (refs.x_rim, refs.x_wide))[which]
    edge = landing.shape[0]
    index = lax.axis_index("seq")

    @pl.when(index > 0)
    def _():
        rim_copy(refs, which).wait_recv()
        target[0:WIDE, :] = landing[...].astype(jnp.float32)[edge - WIDE :, :]

    @pl.when(index == 0)
    def _():
        target[0:WIDE, :] = jnp.zeros((WIDE, target.shape[1]), jnp.float32)


def convolved(source, weights, block):
    taps = weights.shape[0]
    total = jnp.zeros((QB, source.shape[1]), jnp.float32)
    for tap in range(taps):
        shifted = source[pl.ds(block * QB + WIDE - taps + 1 + tap, QB), :]
        total = total + weights[tap : tap + 1, :] * shifted
    return silu(total).astype(jnp.bfloat16)


def spreader(sizes, channels):
    row = lax.broadcasted_iota(jnp.int32, (LANES, channels), 0)
    col = lax.broadcasted_iota(jnp.int32, (LANES, channels), 1)
    wanted = (row % sizes.heads == col // sizes.head_size) & (row < 3 * sizes.heads)
    return jnp.where(wanted, 1.0, 0.0).astype(jnp.bfloat16)


def prepare_params(sizes, refs):
    heads = sizes.heads
    refs.params[...] = jnp.zeros_like(refs.params)
    refs.params[0:1, 0:heads] = refs.dt_bias[...]
    refs.params[1:2, 0:heads] = refs.decay_rate[...]
    refs.params[2:3, 0:heads] = refs.d_skip[...]
    refs.spread[...] = spreader(sizes, refs.y.shape[1])
    refs.skip_row[...] = dot(side_by_side(refs.params[...], heads), refs.spread[...])


def side_block(sizes, refs, block):
    heads = sizes.heads
    span = pl.ds(block * QB, QB)
    lane = lax.broadcasted_iota(jnp.int32, (1, LANES), 1)
    row = lax.broadcasted_iota(jnp.int32, (QB, QB), 0)
    col = lax.broadcasted_iota(jnp.int32, (QB, QB), 1)
    lower = jnp.where(row >= col, 1.0, 0.0).astype(jnp.bfloat16)
    step_dt = jax.nn.softplus(refs.dt_raw[span, :] + refs.params[0:1, :])
    log_decay = jnp.where(lane < heads, -step_dt * refs.params[1:2, :], 0.0)
    sums = dot(lower, side_by_side(log_decay, heads))
    cum = sums + pltpu.roll(sums, LANES - heads, 1) + pltpu.roll(sums, LANES - 2 * heads, 1)
    cum = jnp.where(lane < heads, cum, 0.0)
    refs.cum[span, :] = cum
    refs.cum_t[:, span] = cum.T[0:heads, :]
    refs.dt_t[:, span] = step_dt.T[0:heads, :]
    last = cum[QB - 1 : QB, :]
    to_end = jnp.where(lane < heads, jnp.exp(last - cum) * step_dt, 0.0)
    from_start = jnp.where(lane < heads, jnp.exp(cum), 0.0)
    refs.to_end[span, :] = dot(side_by_side(to_end, heads), refs.spread[...])
    refs.from_start[span, :] = dot(side_by_side(from_start, heads), refs.spread[...])
    if block > 0:
        side_conv(sizes, refs, block)


def side_conv(sizes, refs, block):
    if block == 0:
        take_rim(sizes, refs, 0)
    refs.bc_conv[pl.ds(block * QB, QB), :] = convolved(refs.bc_wide, refs.conv_bc, block)


def finish_body(sizes, refs):
    index, column = lax.axis_index("seq"), lax.axis_index("head")
    seq_count, head_count = sizes.seq_count, sizes.head_count
    heads, head_size, nstate = sizes.heads, sizes.head_size, sizes.nstate
    rows, channels = refs.y.shape
    blocks = rows // QB
    share = channels // SCAN_PARTS

    refs.collect_x()
    for block in [*range(1, blocks), 0]:
        span = pl.ds(block * QB, QB)
        if block == 0:
            side_conv(sizes, refs, 0)
            take_rim(sizes, refs, 1)
        x_blk = convolved(refs.x_wide, refs.conv_x, block)
        refs.x_conv[span, :] = x_blk
        weighted = (x_blk.astype(jnp.float32) * refs.to_end[span, :]).astype(jnp.bfloat16)
        refs.entering[block] = dot_tn(refs.bc_conv[span, 0:nstate], weighted)
    carried = jnp.zeros((nstate, channels), jnp.float32)
    carried_decay = jnp.ones((1, channels), jnp.float32)
    for block in range(blocks):
        added = refs.entering[block]
        refs.entering[block] = carried
        refs.prior[block] = jnp.broadcast_to(carried_decay, refs.prior.shape[1:])
        decay = refs.from_start[pl.ds((block + 1) * QB - 1, 1), :]
        carried = carried * decay + added
        carried_decay = carried_decay * decay
    for part in range(SCAN_PARTS):
        lanes = slice(part * share, (part + 1) * share)
        refs.plane_state[part, 0] = carried[:, lanes].astype(jnp.bfloat16)
        refs.plane_decay[part, 0] = jnp.broadcast_to(carried_decay[:, lanes], (8, share))
        for copy in plane_copies(sizes, refs, part):
            copy.start()
    refs.send_z(refs.share_of(Z_POINTS[1]), refs.share_of(Z_POINTS[2]))

    half = 2 * head_size
    pair_lane = lax.broadcasted_iota(jnp.int32, (QB, half), 1)
    row = lax.broadcasted_iota(jnp.int32, (QB, QB), 0)
    col = lax.broadcasted_iota(jnp.int32, (QB, QB), 1)
    causal = row >= col

    @pl.loop(0, blocks)
    def _(block):
        begin = pl.multiple_of(block * QB, QB)
        span = pl.ds(begin, QB)
        start = refs.share_of(Z_POINTS[2])
        stop = refs.share_of(Z_POINTS[3])
        refs.send_z(start + (stop - start) * block // blocks, start + (stop - start) * (block + 1) // blocks)
        scores = dot_nt(refs.bc_conv[span, nstate:], refs.bc_conv[span, 0:nstate])
        for pair in range(heads // 2):
            lanes = pl.ds(pair * half, half)
            x_pair = refs.x_conv[span, lanes]
            total = jnp.zeros((QB, half), jnp.float32)
            for which in range(2):
                head = 2 * pair + which
                gap = refs.cum[span, head : head + 1] - refs.cum_t[head : head + 1, span]
                factor = jnp.exp(jnp.where(causal, gap, -jnp.inf))
                mixing = (scores * factor * refs.dt_t[head : head + 1, span]).astype(jnp.bfloat16)
                mine = (pair_lane >= head_size) if which else (pair_lane < head_size)
                total = total + dot(mixing, jnp.where(mine, x_pair, jnp.zeros_like(x_pair)))
            refs.y[span, lanes] = total + refs.skip_row[2:3, lanes] * x_pair.astype(jnp.float32)

    for part in range(SCAN_PARTS):
        join_plane(sizes, refs, part)
        start = refs.share_of(Z_POINTS[3])
        stop = refs.share_of(Z_PARTS)
        refs.send_z(
            start + (stop - start) * part // SCAN_PARTS, start + (stop - start) * (part + 1) // SCAN_PARTS
        )

    for early in range(1, BATCHES + 1):
        first_plane, last_plane = index < sizes.side_count, index + sizes.side_count >= seq_count
        wanted = last_plane if early == BATCHES else ~first_plane

        @pl.when(wanted)
        def _(early=early):
            refs.gates(early - 1, early)

    for part in range(SCAN_PARTS):
        join_chain(sizes, refs, part)

    @pl.when(index < sizes.side_count)
    def _():
        refs.gates(0, BATCHES - 1)

    @pl.when(index + sizes.side_count < seq_count)
    def _():
        refs.gates(BATCHES - 1, BATCHES)

    ones = jnp.ones((8, LANES), jnp.bfloat16)

    @pl.loop(0, blocks)
    def _(block):
        begin = pl.multiple_of(block * QB, QB)
        span = pl.ds(begin, QB)
        state = refs.entering[block] + refs.incoming[...] * refs.prior[block][0:1, :]
        high, middle, _ = three_parts(state)
        c_blk = refs.bc_conv[span, nstate:]
        outside = dot(c_blk, high.astype(jnp.bfloat16)) + dot(c_blk, middle.astype(jnp.bfloat16))
        value = (refs.y[span, :] + refs.from_start[span, :] * outside) * refs.z[span, :]
        refs.y[span, :] = value
        squares = value * value
        folded = squares[:, 0:LANES]
        for part in range(1, channels // LANES):
            folded = folded + squares[:, part * LANES : (part + 1) * LANES]
        first, second, third = three_parts(folded)
        total = dot_nt(ones, first.astype(jnp.bfloat16)) + dot_nt(ones, second.astype(jnp.bfloat16))
        total = total + dot_nt(ones, third.astype(jnp.bfloat16))
        for part in range(QB // LANES):
            line = total[0:1, part * LANES : (part + 1) * LANES]
            refs.square[pl.ds(block * (QB // LANES) + part, 1), :] = line

    def shares():
        return [
            remote(
                refs.square,
                refs.square_in.at[step - 1],
                refs.norm_send.at[step - 1],
                refs.norm_recv.at[step - 1],
                (index, lax.rem(column + step, head_count)),
            )
            for step in range(1, head_count)
        ]

    for copy in shares():
        copy.start()
    for copy in shares():
        copy.wait_recv()
    total = refs.square[...]
    for step in range(1, head_count):
        total = total + refs.square_in[step - 1]
    scale = lax.rsqrt(total / (head_count * channels) + EPSILON)
    lines = rows // LANES
    line_of = lax.broadcasted_iota(jnp.int32, (lines, channels), 0)
    scales = [part.astype(jnp.bfloat16) for part in three_parts(scale)]
    for line in range(lines):
        span = pl.ds(line * LANES, LANES)
        chosen = jnp.where(line_of == line, 1.0, 0.0).astype(jnp.bfloat16)
        wide_scale = dot_tn(scales[0], chosen) + dot_tn(scales[1], chosen) + dot_tn(scales[2], chosen)
        refs.out[span, :] = (refs.y[span, :] * wide_scale * refs.norm_gain[...]).astype(jnp.bfloat16)

    for copy in shares():
        copy.wait_send()

    @pl.when(index + 1 < seq_count)
    def _():
        for which in range(2):
            rim_copy(refs, which).wait_send()

    for part in range(SCAN_PARTS):
        for copy in plane_copies(sizes, refs, part):
            copy.wait_send()

        @pl.when(index + sizes.side_count < seq_count)
        def _(part=part):
            chain_copy(sizes, refs, part).wait_send()

    refs.settle()


def pick(options, which):
    value = options[0]
    for place in range(1, len(options)):
        value = jnp.where(which == place, options[place], value)
    return value


def padded(lines, length):
    return [list(line) + [0] * (length - len(line)) for line in lines]


def project_kernel(sizes, names, *all_refs):
    refs = types.SimpleNamespace(**dict(zip(names, all_refs)))
    index, column = lax.axis_index("seq"), lax.axis_index("head")
    barrier = pltpu.get_barrier_semaphore()
    for step in range(1, sizes.seq_count):
        other = lax.rem(index + step, sizes.seq_count)
        pl.semaphore_signal(barrier, inc=1, device_id=(other, column), device_id_type=MESH)
    for step in range(1, sizes.head_count):
        other = lax.rem(column + step, sizes.head_count)
        pl.semaphore_signal(barrier, inc=1, device_id=(index, other), device_id_type=MESH)
    project_body(sizes, refs, barrier)
    finish_body(sizes, refs)


def project_body(sizes, refs, barrier):
    index, column = lax.axis_index("seq"), lax.axis_index("head")
    seq_count, head_count = sizes.seq_count, sizes.head_count
    cap, direct, shared, lines = sizes.cap, sizes.direct, sizes.shared, sizes.lines
    places, slot_count = sizes.places, sizes.slots
    rows, channels = refs.y.shape
    width = refs.tok.shape[1]
    blocks = rows // QB
    core, line = lax.rem(column, 2), column // 2
    half = width // 2
    foreign, chosen, slot_of, served, _ = serving_plan(seq_count, sizes.pieces, sizes.outward)
    foreign_count = pick([len(line_) for line_ in foreign], index)
    served_count = pick([len(line_) for line_ in served], index)
    server_of, landing = [], []
    for place in range(places):
        server_of.append(pick([chosen.get((home, place), 0) for home in range(seq_count)], index))
        landing.append(pick([slot_of.get((home, place), 0) for home in range(seq_count)], index))
    homes, home_places = [], []
    for slot in range(slot_count):
        homes.append(pick([line_[slot][0] if slot < len(line_) else 0 for line_ in served], index))
        home_places.append(pick([line_[slot][1] if slot < len(line_) else 0 for line_ in served], index))

    def direct_lanes(which):
        return pl.ds(pl.multiple_of(which * half, LANES), direct)

    def shared_lanes(which, from_line):
        return pl.ds(pl.multiple_of(which * half + direct + from_line * shared, LANES), shared)

    own_copies = [
        pltpu.make_async_copy(
            refs.tokens.at[:, shared_lanes(core, line)],
            refs.own_tok.at[:, pl.ds(direct, shared)],
            refs.local.at[1],
        )
    ]
    if direct:
        own_copies.append(
            pltpu.make_async_copy(
                refs.tokens.at[:, direct_lanes(core)], refs.own_tok.at[:, pl.ds(0, direct)], refs.local.at[0]
            )
        )
    weight_copy = pltpu.make_async_copy(refs.w_in.at[0], refs.weight, refs.local.at[2])
    token_copy = pltpu.make_async_copy(refs.tokens, refs.tok, refs.local.at[3])
    side_copy = pltpu.make_async_copy(refs.w_bc, refs.side, refs.local.at[4])
    for copy in own_copies + [weight_copy, token_copy, side_copy]:
        copy.start()

    slots = refs.owner_slot[...]
    place_row = jnp.full(slots.shape, -1, jnp.int32)
    for group in range(seq_count * sizes.pieces):
        place = pick([line_.index(group) if group in line_ else -1 for line_ in foreign], index)
        within = (slots >= group * cap) & (slots < (group + 1) * cap)
        moved = jnp.where(place >= 0, slots + (place - group) * cap, -1)
        place_row = jnp.where(within, moved, place_row)

    for place in range(min(len(line_) for line_ in foreign), places):

        @pl.when(place >= foreign_count)
        def _(place=place):
            span = pl.ds(place * cap, cap)
            refs.x_back[span, :] = jnp.zeros((cap, channels), jnp.bfloat16)
            refs.z_back[span, :] = jnp.zeros((cap, channels), jnp.bfloat16)

    def sends(place):
        server = (server_of[place], column)
        slot = landing[place]
        kinds = [(1, pl.ds(direct, shared), shared_lanes(core, line))]
        if direct:
            kinds.append((0, pl.ds(0, direct), direct_lanes(core)))
        return [
            remote(
                refs.packed.at[place, :, source],
                refs.inbox.at[slot, :, target],
                refs.pack_send.at[place, kind],
                refs.pack_recv.at[slot, kind],
                server,
            )
            for kind, source, target in kinds
        ]

    for copy in own_copies:
        copy.wait()
    sublane = lax.broadcasted_iota(jnp.int32, (cap, rows), 0)
    for place in range(places):

        @pl.when(place < foreign_count)
        def _(place=place):
            chosen_rows = jnp.where(place_row == sublane + place * cap, 1.0, 0.0).astype(jnp.bfloat16)
            refs.packed[place] = dot(chosen_rows, refs.own_tok[...]).astype(jnp.bfloat16)
            if place == 0:
                pl.semaphore_wait(barrier, seq_count + head_count - 2)
            for copy in sends(place):
                copy.start()

    prepare_params(sizes, refs)

    pair = 4 * sizes.head_size
    source = lax.broadcasted_iota(jnp.int32, (pair, pair), 0)
    target = lax.broadcasted_iota(jnp.int32, (pair, pair), 1)
    size = sizes.head_size
    from_z = target // (2 * size)
    wanted = (target % (2 * size)) // size * (2 * size) + from_z * size + target % size
    chooser = jnp.where(source == wanted, 1.0, 0.0).astype(jnp.bfloat16)
    weight_copy.wait()

    @pl.loop(0, width // QB)
    def _(part):
        span = pl.ds(pl.multiple_of(part * QB, QB), QB)
        for couple in range(sizes.heads // 2):
            split = dot(refs.weight[span, couple * pair : (couple + 1) * pair], chooser).astype(jnp.bfloat16)
            lanes = pl.ds(couple * pair // 2, pair // 2)
            refs.weight_x[span, lanes] = split[:, : pair // 2]
            refs.weight_z[span, lanes] = split[:, pair // 2 :]

    place_col = jnp.broadcast_to(place_row.astype(jnp.float32), (LANES, rows)).T
    refs.place_col[...] = place_col
    token_copy.wait()
    side_copy.wait()

    def received(slot):
        kinds = [(1, shared_lanes(core, line))] + ([(0, direct_lanes(core))] if direct else [])
        return [
            remote(
                refs.inbox.at[slot, :, lanes],
                refs.inbox.at[slot, :, lanes],
                refs.pack_send.at[0, kind],
                refs.pack_recv.at[slot, kind],
                (index, column),
            )
            for kind, lanes in kinds
        ]

    def across_lines(slot, arriving):
        copies = []
        for step in range(1, lines):
            from_line = lax.rem(line + lines - step, lines) if arriving else line
            lanes = shared_lanes(core, from_line)
            copies.append(
                remote(
                    refs.inbox.at[slot, :, lanes],
                    refs.inbox.at[slot, :, lanes],
                    refs.line_send.at[slot, step - 1],
                    refs.line_recv.at[slot, step - 1],
                    (index, lax.rem(line + step, lines) * 2 + core),
                )
            )
        return copies

    def across_cores(slot, arriving):
        from_core = 1 - core if arriving else core
        lanes = pl.ds(pl.multiple_of(from_core * half, LANES), half)
        return remote(
            refs.inbox.at[slot, :, lanes],
            refs.inbox.at[slot, :, lanes],
            refs.core_send.at[slot],
            refs.core_recv.at[slot],
            (index, line * 2 + 1 - core),
        )

    def answer(slot, source, target, send, recv):
        home, place = pick(homes, slot), pick(home_places, slot)
        return remote(
            source.at[slot],
            target.at[pl.ds(pl.multiple_of(place * cap, cap), cap)],
            send.at[slot],
            recv.at[place],
            (home, column),
        )

    def answer_x(slot):
        return answer(slot, refs.x_served, refs.x_back, refs.x_send, refs.x_recv)

    def answer_z(slot):
        return answer(slot, refs.z_served, refs.z_back, refs.z_send, refs.z_recv)

    quiet = 2 * blocks
    last_turn = max(slot_count + 2, 3 * blocks, quiet + -(-slot_count // Z_EACH))

    @pl.loop(0, last_turn)
    def _(turn):
        @pl.when(turn < served_count)
        def _():
            for copy in received(turn):
                copy.wait_recv()
            for copy in across_lines(turn, False):
                copy.start()

        @pl.when(turn < blocks)
        def _():
            span = pl.ds(pl.multiple_of(turn * QB, QB), QB)
            tok = refs.tok[span, :]
            place = refs.place_col[span, :]
            mine = jnp.concatenate([place] * (channels // LANES), axis=1) < 0
            product = dot(tok, refs.weight_x[...])
            wide = pl.ds(pl.multiple_of(turn * QB + WIDE, WIDE), QB)
            refs.x_wide[wide, :] = rounded(jnp.where(mine, product, 0.0))
            side = dot(tok, refs.side[...]).astype(jnp.bfloat16)
            refs.bc[span, :] = side
            refs.bc_wide[wide, :] = side.astype(jnp.float32)
            refs.dt_raw[span, 0 : sizes.heads] = dot_nt(tok, refs.w_dt_t[...])
            lane = lax.broadcasted_iota(jnp.int32, (QB, LANES), 1).astype(jnp.float32)
            for part in range(places * cap // LANES):
                hit = jnp.where(place == lane + part * LANES, 1.0, 0.0)
                refs.unpack[span, part * LANES : (part + 1) * LANES] = hit.astype(jnp.bfloat16)

        for block in range(blocks):

            @pl.when(turn == blocks + (block + blocks - 1) % blocks)
            def _(block=block):
                if block == min(1, blocks - 1):
                    send_rim(sizes, refs, 0)
                side_block(sizes, refs, block)

        @pl.when((turn >= quiet) & (turn < quiet + blocks))
        def _():
            span = pl.ds(pl.multiple_of((turn - quiet) * QB, QB), QB)
            place = refs.place_col[span, :]
            mine = jnp.concatenate([place] * (channels // LANES), axis=1) < 0
            product = dot(refs.tok[span, :], refs.weight_z[...])
            refs.z[span, :] = rounded(jnp.where(mine, product, 0.0))

        @pl.when((turn >= 1) & (turn - 1 < served_count))
        def _():
            slot = turn - 1
            for copy in across_lines(slot, True):
                copy.wait_recv()
            across_cores(slot, False).start()

        @pl.when((turn >= 2) & (turn - 2 < served_count))
        def _():
            slot = turn - 2
            across_cores(slot, True).wait_recv()
            refs.x_served[slot] = dot(refs.inbox[slot], refs.weight_x[...]).astype(jnp.bfloat16)
            answer_x(slot).start()

        for extra in range(Z_EACH):
            slot = (turn - quiet) * Z_EACH + extra

            @pl.when((turn >= quiet) & (slot < served_count))
            def _(slot=slot):
                refs.z_served[slot] = dot(refs.inbox[slot], refs.weight_z[...]).astype(jnp.bfloat16)

    def send_z(start, stop):
        @pl.loop(start, stop)
        def _(slot):
            @pl.when(slot < served_count)
            def _():
                answer_z(slot).start()

    def share_of(part):
        return slot_count * part // Z_PARTS

    refs.send_z, refs.share_of = send_z, share_of
    send_z(0, share_of(Z_POINTS[0]))

    def back(place, buffer, recv):
        span = pl.ds(pl.multiple_of(place * cap, cap), cap)
        return remote(
            buffer.at[span], buffer.at[span], refs.x_send.at[0], recv.at[place], (index, column)
        )

    batch = -(-places // BATCHES)

    def arrived(group, buffer, recv):
        @pl.loop(group * batch, min((group + 1) * batch, places))
        def _(place):
            @pl.when(place < foreign_count)
            def _():
                back(place, buffer, recv).wait_recv()

    def unpacked(group, span, buffer):
        lines_ = slice(group * batch * cap, min((group + 1) * batch, places) * cap)
        return dot(refs.unpack[span, lines_], buffer[lines_, :])

    def collect_x():
        for group in range(BATCHES - 1):
            arrived(group, refs.x_back, refs.x_recv)

            @pl.loop(0, blocks)
            def _(block, group=group):
                span = pl.ds(pl.multiple_of(block * QB, QB), QB)
                wide = pl.ds(pl.multiple_of(block * QB + WIDE, WIDE), QB)
                refs.x_wide[wide, :] = refs.x_wide[wide, :] + unpacked(group, span, refs.x_back)

        arrived(BATCHES - 1, refs.x_back, refs.x_recv)
        for block in [blocks - 1, *range(blocks - 1)]:
            span, wide = pl.ds(block * QB, QB), pl.ds(block * QB + WIDE, QB)
            merged = refs.x_wide[wide, :] + unpacked(BATCHES - 1, span, refs.x_back)
            refs.x_wide[wide, :] = merged
            if block == blocks - 1:
                edge = refs.x.shape[0]
                refs.x[...] = merged[QB - edge :, :].astype(jnp.bfloat16)
                send_rim(sizes, refs, 1)
                send_z(share_of(Z_POINTS[0]), share_of(Z_POINTS[1]))

    def gates(first, last):
        for group in range(first, last):
            arrived(group, refs.z_back, refs.z_recv)

            @pl.loop(0, blocks)
            def _(block, group=group):
                span = pl.ds(pl.multiple_of(block * QB, QB), QB)
                total = refs.z[span, :] + unpacked(group, span, refs.z_back)
                refs.z[span, :] = silu(total) if group == BATCHES - 1 else total

    def settle():
        for place in range(places):

            @pl.when(place < foreign_count)
            def _(place=place):
                for copy in sends(place):
                    copy.wait_send()

        @pl.loop(0, slot_count)
        def _(slot):
            @pl.when(slot < served_count)
            def _():
                for copy in across_lines(slot, False):
                    copy.wait_send()
                across_cores(slot, False).wait_send()
                answer_x(slot).wait_send()
                answer_z(slot).wait_send()

    refs.gates = gates
    refs.settle = settle
    refs.collect_x = collect_x


def per_device(
    tokens, owner_slot, w_in, w_bc, w_dt, conv_x, conv_bc, dt_bias, decay_rate, d_skip, norm_gain
):
    rows, width = tokens.shape
    both = w_bc.shape[1]
    heads = dt_bias.shape[0]
    channels = w_in.shape[2] // 2
    nstate = both // 2
    blocks = rows // QB
    head_count = lax.axis_size("head")
    seq_count = lax.axis_size("seq")
    lines = head_count // 2
    cap = min(2 * rows // seq_count, LANES)
    pieces = 2 * rows // seq_count // cap
    direct = next(
        part
        for part in (DIRECT * LANES, width // 4)
        if (width // 2 - part) % (LANES * lines) == 0 and part % LANES == 0
    )
    shared = (width // 2 - direct) // lines
    outward = 2 * (direct + shared) / (4 * channels)
    foreign, _, _, served, _ = serving_plan(seq_count, pieces, outward)
    places = max(len(line) for line in foreign)
    slots = max(len(line) for line in served)
    sizes = types.SimpleNamespace(
        seq_count=seq_count,
        head_count=head_count,
        heads=heads,
        head_size=channels // heads,
        nstate=nstate,
        cap=cap,
        pieces=pieces,
        outward=outward,
        side_count=plane_width(seq_count),
        lines=lines,
        places=places,
        slots=slots,
        direct=direct,
        shared=shared,
    )
    side_count = plane_width(seq_count)
    share = channels // SCAN_PARTS
    in_hbm = dict(tokens=tokens, w_in=w_in, w_bc=w_bc)
    in_vmem = dict(
        owner_slot=owner_slot[None],
        w_dt_t=w_dt.T,
        conv_x=conv_x,
        conv_bc=conv_bc,
        dt_bias=dt_bias[None],
        decay_rate=decay_rate[None],
        d_skip=d_skip[None],
        norm_gain=norm_gain[None],
    )
    inputs = in_hbm | in_vmem
    f32, bf16 = jnp.float32, jnp.bfloat16
    dma = pltpu.SemaphoreType.DMA
    scratch = dict(
        tok=pltpu.VMEM((rows, width), bf16),
        own_tok=pltpu.VMEM((rows, direct + shared), bf16),
        weight=pltpu.VMEM((width, 2 * channels), bf16),
        weight_x=pltpu.VMEM((width, channels), bf16),
        weight_z=pltpu.VMEM((width, channels), bf16),
        side=pltpu.VMEM((width, both), bf16),
        packed=pltpu.VMEM((places, cap, direct + shared), bf16),
        inbox=pltpu.VMEM((slots, cap, width), bf16),
        x_served=pltpu.VMEM((slots, cap, channels), bf16),
        z_served=pltpu.VMEM((slots, cap, channels), bf16),
        x_back=pltpu.VMEM((places * cap, channels), bf16),
        z_back=pltpu.VMEM((places * cap, channels), bf16),
        unpack=pltpu.VMEM((rows, places * cap), bf16),
        place_col=pltpu.VMEM((rows, LANES), f32),
        x=pltpu.VMEM((16, channels), bf16),
        z=pltpu.VMEM((rows, channels), f32),
        bc=pltpu.VMEM((rows, both), bf16),
        dt_raw=pltpu.VMEM((rows, LANES), f32),
        x_rim=pltpu.VMEM((16, channels), bf16),
        bc_rim=pltpu.VMEM((16, both), bf16),
        x_wide=pltpu.VMEM((rows + WIDE, channels), f32),
        bc_wide=pltpu.VMEM((rows + WIDE, both), f32),
        x_conv=pltpu.VMEM((rows, channels), bf16),
        bc_conv=pltpu.VMEM((rows, both), bf16),
        params=pltpu.VMEM((8, LANES), f32),
        spread=pltpu.VMEM((LANES, channels), bf16),
        skip_row=pltpu.VMEM((8, channels), f32),
        to_end=pltpu.VMEM((rows, channels), f32),
        cum=pltpu.VMEM((rows, LANES), f32),
        cum_t=pltpu.VMEM((heads, rows), f32),
        dt_t=pltpu.VMEM((heads, rows), f32),
        from_start=pltpu.VMEM((rows, channels), f32),
        y=pltpu.VMEM((rows, channels), f32),
        entering=pltpu.VMEM((blocks, nstate, channels), f32),
        prior=pltpu.VMEM((blocks, 8, channels), f32),
        incoming=pltpu.VMEM((nstate, channels), f32),
        before=pltpu.VMEM((SCAN_PARTS, nstate, share), f32),
        before_decay=pltpu.VMEM((SCAN_PARTS, 8, share), f32),
        ahead=pltpu.VMEM((SCAN_PARTS, nstate, share), f32),
        ahead_decay=pltpu.VMEM((SCAN_PARTS, 8, share), f32),
        plane_state=pltpu.VMEM((SCAN_PARTS, side_count, nstate, share), bf16),
        plane_decay=pltpu.VMEM((SCAN_PARTS, side_count, 8, share), f32),
        chain_in=pltpu.VMEM((SCAN_PARTS, nstate, share), bf16),
        chain_out=pltpu.VMEM((SCAN_PARTS, nstate, share), bf16),
        square=pltpu.VMEM((rows // LANES, LANES), f32),
        square_in=pltpu.VMEM((head_count - 1, rows // LANES, LANES), f32),
        local=dma((5,)),
        pack_send=dma((places, 2)),
        pack_recv=dma((slots, 2)),
        line_send=dma((slots, lines - 1)),
        line_recv=dma((slots, lines - 1)),
        core_send=dma((slots,)),
        core_recv=dma((slots,)),
        x_send=dma((slots,)),
        x_recv=dma((places,)),
        z_send=dma((slots,)),
        z_recv=dma((places,)),
        rim_send=dma((2,)),
        rim_recv=dma((2,)),
        plane_send=dma((SCAN_PARTS, side_count - 1, 2)),
        plane_recv=dma((SCAN_PARTS, side_count - 1, 2)),
        chain_send=dma((SCAN_PARTS,)),
        chain_recv=dma((SCAN_PARTS,)),
        norm_send=dma((head_count - 1,)),
        norm_recv=dma((head_count - 1,)),
    )
    names = tuple(inputs) + ("out",) + tuple(scratch)
    any_spec = pl.BlockSpec(memory_space=pl.ANY)
    vmem_spec = pl.BlockSpec(memory_space=pltpu.VMEM)
    return pl.pallas_call(
        functools.partial(project_kernel, sizes, names),
        out_shape=jax.ShapeDtypeStruct((rows, channels), bf16),
        in_specs=[any_spec] * len(in_hbm) + [vmem_spec] * len(in_vmem),
        out_specs=vmem_spec,
        scratch_shapes=list(scratch.values()),
        compiler_params=pltpu.CompilerParams(
            collective_id=0, has_side_effects=True, vmem_limit_bytes=62 << 20
        ),
    )(*inputs.values())


def solution(mesh):
    return jax.shard_map(
        per_device,
        mesh=mesh,
        in_specs=(
            P("seq", None),
            P("seq"),
            P("seq", None, "head"),
            P(),
            P(None, "head"),
            P(None, "head"),
            P(),
            P("head"),
            P("head"),
            P("head"),
            P("head"),
        ),
        out_specs=P("seq", "head"),
        check_vma=False,
    )
```

```python
import functools
import types

import jax
import jax.numpy as jnp
from jax import lax
from jax.experimental import pallas as pl
from jax.experimental.pallas import tpu as pltpu
from jax.sharding import PartitionSpec as P

KCONV = 4
QB = 256
MODS = 3
EPSILON = 1e-05
LANES = 128
MESH = pl.DeviceIdType.MESH
Z_PARTS = 12
Z_POINTS = (4, 6, 6, 10)
BATCHES = 2
Z_EACH = 2
DIRECT = 2
SCAN_PARTS = 4
STATE_LOAD = 0.27
BUSY_PRICE = 0.3
WIDE = 8


def plane_width(count):
    return max(side for side in range(1, count) if count % side == 0 and side * side <= count)


def route(start, end, width):
    (plane, side), (last_plane, last_side) = divmod(start, width), divmod(end, width)
    links = []
    while (plane, side) != (last_plane, last_side):
        before = plane * width + side
        if plane != last_plane:
            plane += 1 if last_plane > plane else -1
        else:
            side += 1 if last_side > side else -1
        links.append((before, plane * width + side))
    return links


def serving_plan(count, pieces, outward):
    width = plane_width(count)
    foreign = [
        [owner * pieces + piece for piece in range(pieces) for owner in range(count) if (owner - home) % MODS]
        for home in range(count)
    ]
    groups = [(home, place) for home in range(count) for place in range(len(foreign[home]))]
    loads, busy, chosen = {}, [0] * count, {}
    for start in range(count):
        for end in (start + 1, start - 1, start + width):
            if 0 <= end < count and (end == start + width or end // width == start // width):
                loads[start, end] = STATE_LOAD * pieces

    def trips(home, server):
        return [(outward, link) for link in route(home, server, width)] + [
            (1.0, link) for link in route(server, home, width)
        ]

    def add(home, server, sign):
        busy[server] += sign
        for weight, link in trips(home, server):
            loads[link] = loads.get(link, 0.0) + sign * weight

    def price(home, server):
        total = BUSY_PRICE * ((busy[server] + 1) ** 4 - busy[server] ** 4)
        for weight, link in trips(home, server):
            before = loads.get(link, 0.0)
            total += (before + weight) ** 4 - before**4
        return total

    for _ in range(12):
        for home, place in groups:
            if (home, place) in chosen:
                add(home, chosen[home, place], -1)
            owner = foreign[home][place] // pieces
            options = [server for server in range(count) if (server - owner) % MODS == 0]
            best = min(options, key=lambda server: (round(price(home, server), 6), server))
            chosen[home, place] = best
            add(home, best, 1)
    order = [[] for _ in range(count)]
    for home, place in groups:
        first = route(home, chosen[home, place], width)[0]
        earlier = sum(route(home, chosen[home, other], width)[0] == first for other in range(place))
        order[chosen[home, place]].append((earlier, place, home))
    served = [[(home, place) for _, place, home in sorted(line)] for line in order]
    slots = {group: slot for line in served for slot, group in enumerate(line)}
    return foreign, chosen, slots, served, loads


def dot(a, b):
    return jnp.dot(a, b, preferred_element_type=jnp.float32)


def dot_nt(a, b):
    return lax.dot_general(a, b, (((1,), (1,)), ((), ())), preferred_element_type=jnp.float32)


def dot_tn(a, b):
    return lax.dot_general(a, b, (((0,), (0,)), ((), ())), preferred_element_type=jnp.float32)


def rounded(value):
    return value.astype(jnp.bfloat16).astype(jnp.float32)


def three_parts(value):
    high = rounded(value)
    middle = rounded(value - high)
    return high, middle, value - high - middle


def side_by_side(value, count):
    high, middle, low = three_parts(value)
    packed = high + pltpu.roll(middle, count, 1) + pltpu.roll(low, 2 * count, 1)
    return packed.astype(jnp.bfloat16)


def silu(value):
    return value * jax.nn.sigmoid(value)


def remote(source, target, send, recv, device):
    return pltpu.make_async_remote_copy(
        source, target, send, recv, device_id=device, device_id_type=MESH
    )


def plane_copies(sizes, refs, part):
    index, side = lax.axis_index("seq"), lax.rem(lax.axis_index("seq"), sizes.side_count)
    copies = []
    for step in range(1, sizes.side_count):
        target = (index - side + lax.rem(side + step, sizes.side_count), lax.axis_index("head"))
        for place, buffer in enumerate((refs.plane_state, refs.plane_decay)):
            copies.append(
                remote(
                    buffer.at[part, 0],
                    buffer.at[part, step],
                    refs.plane_send.at[part, step - 1, place],
                    refs.plane_recv.at[part, step - 1, place],
                    target,
                )
            )
    return copies


def chain_copy(sizes, refs, part):
    return remote(
        refs.chain_out.at[part],
        refs.chain_in.at[part],
        refs.chain_send.at[part],
        refs.chain_recv.at[part],
        (lax.axis_index("seq") + sizes.side_count, lax.axis_index("head")),
    )


def join_plane(sizes, refs, part):
    side = lax.rem(lax.axis_index("seq"), sizes.side_count)
    for copy in plane_copies(sizes, refs, part):
        copy.wait_recv()
    total = jnp.zeros(refs.ahead.shape[1:], jnp.float32)
    decay = jnp.ones(refs.ahead_decay.shape[1:], jnp.float32)
    before, before_decay = total, decay
    for place in range(sizes.side_count):
        before = jnp.where(side == place, total, before)
        before_decay = jnp.where(side == place, decay, before_decay)
        slot = lax.rem(side + sizes.side_count - place, sizes.side_count)
        factor = refs.plane_decay[part, slot]
        total = total * factor[0:1, :] + refs.plane_state[part, slot].astype(jnp.float32)
        decay = decay * factor
    refs.before[part] = before
    refs.before_decay[part] = before_decay
    refs.ahead[part] = total
    refs.ahead_decay[part] = decay


def join_chain(sizes, refs, part):
    index = lax.axis_index("seq")
    share = refs.incoming.shape[1] // SCAN_PARTS
    lanes = pl.ds(part * share, share)

    @pl.when(index < sizes.side_count)
    def _():
        refs.chain_in[part] = jnp.zeros(refs.chain_in.shape[1:], jnp.bfloat16)

    @pl.when(index >= sizes.side_count)
    def _():
        chain_copy(sizes, refs, part).wait_recv()

    @pl.when(index + sizes.side_count < sizes.seq_count)
    def _():
        entering = refs.chain_in[part].astype(jnp.float32)
        leaving = refs.ahead[part] + refs.ahead_decay[part][0:1, :] * entering
        refs.chain_out[part] = leaving.astype(jnp.bfloat16)
        chain_copy(sizes, refs, part).start()

    entering = refs.chain_in[part].astype(jnp.float32)
    refs.incoming[:, lanes] = refs.before[part] + refs.before_decay[part][0:1, :] * entering


def rim_copy(refs, which):
    source, landing = ((refs.bc, refs.bc_rim), (refs.x, refs.x_rim))[which]
    edge = landing.shape[0]
    return remote(
        source.at[pl.ds(source.shape[0] - edge, edge)],
        landing,
        refs.rim_send.at[which],
        refs.rim_recv.at[which],
        (lax.axis_index("seq") + 1, lax.axis_index("head")),
    )


def send_rim(sizes, refs, which):
    @pl.when(lax.axis_index("seq") + 1 < sizes.seq_count)
    def _():
        rim_copy(refs, which).start()


def take_rim(sizes, refs, which):
    landing, target = ((refs.bc_rim, refs.bc_wide), (refs.x_rim, refs.x_wide))[which]
    edge = landing.shape[0]
    index = lax.axis_index("seq")

    @pl.when(index > 0)
    def _():
        rim_copy(refs, which).wait_recv()
        target[0:WIDE, :] = landing[...].astype(jnp.float32)[edge - WIDE :, :]

    @pl.when(index == 0)
    def _():
        target[0:WIDE, :] = jnp.zeros((WIDE, target.shape[1]), jnp.float32)


def convolved(source, weights, block):
    taps = weights.shape[0]
    total = jnp.zeros((QB, source.shape[1]), jnp.float32)
    for tap in range(taps):
        shifted = source[pl.ds(block * QB + WIDE - taps + 1 + tap, QB), :]
        total = total + weights[tap : tap + 1, :] * shifted
    return silu(total).astype(jnp.bfloat16)


def spreader(sizes, channels):
    row = lax.broadcasted_iota(jnp.int32, (LANES, channels), 0)
    col = lax.broadcasted_iota(jnp.int32, (LANES, channels), 1)
    wanted = (row % sizes.heads == col // sizes.head_size) & (row < 3 * sizes.heads)
    return jnp.where(wanted, 1.0, 0.0).astype(jnp.bfloat16)


def prepare_params(sizes, refs):
    heads = sizes.heads
    refs.params[...] = jnp.zeros_like(refs.params)
    refs.params[0:1, 0:heads] = refs.dt_bias[...]
    refs.params[1:2, 0:heads] = refs.decay_rate[...]
    refs.params[2:3, 0:heads] = refs.d_skip[...]
    refs.spread[...] = spreader(sizes, refs.y.shape[1])
    refs.skip_row[...] = dot(side_by_side(refs.params[...], heads), refs.spread[...])


def side_block(sizes, refs, block):
    heads = sizes.heads
    span = pl.ds(block * QB, QB)
    lane = lax.broadcasted_iota(jnp.int32, (1, LANES), 1)
    row = lax.broadcasted_iota(jnp.int32, (QB, QB), 0)
    col = lax.broadcasted_iota(jnp.int32, (QB, QB), 1)
    lower = jnp.where(row >= col, 1.0, 0.0).astype(jnp.bfloat16)
    step_dt = jax.nn.softplus(refs.dt_raw[span, :] + refs.params[0:1, :])
    log_decay = jnp.where(lane < heads, -step_dt * refs.params[1:2, :], 0.0)
    sums = dot(lower, side_by_side(log_decay, heads))
    cum = sums + pltpu.roll(sums, LANES - heads, 1) + pltpu.roll(sums, LANES - 2 * heads, 1)
    cum = jnp.where(lane < heads, cum, 0.0)
    refs.cum[span, :] = cum
    refs.cum_t[:, span] = cum.T[0:heads, :]
    refs.dt_t[:, span] = step_dt.T[0:heads, :]
    last = cum[QB - 1 : QB, :]
    to_end = jnp.where(lane < heads, jnp.exp(last - cum) * step_dt, 0.0)
    from_start = jnp.where(lane < heads, jnp.exp(cum), 0.0)
    refs.to_end[span, :] = dot(side_by_side(to_end, heads), refs.spread[...])
    refs.from_start[span, :] = dot(side_by_side(from_start, heads), refs.spread[...])
    if block > 0:
        side_conv(sizes, refs, block)


def side_conv(sizes, refs, block):
    if block == 0:
        take_rim(sizes, refs, 0)
    refs.bc_conv[pl.ds(block * QB, QB), :] = convolved(refs.bc_wide, refs.conv_bc, block)


def finish_body(sizes, refs):
    index, column = lax.axis_index("seq"), lax.axis_index("head")
    seq_count, head_count = sizes.seq_count, sizes.head_count
    heads, head_size, nstate = sizes.heads, sizes.head_size, sizes.nstate
    rows, channels = refs.y.shape
    blocks = rows // QB
    share = channels // SCAN_PARTS

    refs.collect_x()
    for block in [*range(1, blocks), 0]:
        span = pl.ds(block * QB, QB)
        if block == 0:
            side_conv(sizes, refs, 0)
            take_rim(sizes, refs, 1)
        x_blk = convolved(refs.x_wide, refs.conv_x, block)
        refs.x_conv[span, :] = x_blk
        weighted = (x_blk.astype(jnp.float32) * refs.to_end[span, :]).astype(jnp.bfloat16)
        refs.entering[block] = dot_tn(refs.bc_conv[span, 0:nstate], weighted)
    carried = jnp.zeros((nstate, channels), jnp.float32)
    carried_decay = jnp.ones((1, channels), jnp.float32)
    for block in range(blocks):
        added = refs.entering[block]
        refs.entering[block] = carried
        refs.prior[block] = jnp.broadcast_to(carried_decay, refs.prior.shape[1:])
        decay = refs.from_start[pl.ds((block + 1) * QB - 1, 1), :]
        carried = carried * decay + added
        carried_decay = carried_decay * decay
    for part in range(SCAN_PARTS):
        lanes = slice(part * share, (part + 1) * share)
        refs.plane_state[part, 0] = carried[:, lanes].astype(jnp.bfloat16)
        refs.plane_decay[part, 0] = jnp.broadcast_to(carried_decay[:, lanes], (8, share))
        for copy in plane_copies(sizes, refs, part):
            copy.start()
    refs.send_z(refs.share_of(Z_POINTS[1]), refs.share_of(Z_POINTS[2]))

    half = 2 * head_size
    pair_lane = lax.broadcasted_iota(jnp.int32, (QB, half), 1)
    row = lax.broadcasted_iota(jnp.int32, (QB, QB), 0)
    col = lax.broadcasted_iota(jnp.int32, (QB, QB), 1)
    causal = row >= col

    @pl.loop(0, blocks)
    def _(block):
        begin = pl.multiple_of(block * QB, QB)
        span = pl.ds(begin, QB)
        start = refs.share_of(Z_POINTS[2])
        stop = refs.share_of(Z_POINTS[3])
        refs.send_z(start + (stop - start) * block // blocks, start + (stop - start) * (block + 1) // blocks)
        scores = dot_nt(refs.bc_conv[span, nstate:], refs.bc_conv[span, 0:nstate])
        for pair in range(heads // 2):
            lanes = pl.ds(pair * half, half)
            x_pair = refs.x_conv[span, lanes]
            total = jnp.zeros((QB, half), jnp.float32)
            for which in range(2):
                head = 2 * pair + which
                gap = refs.cum[span, head : head + 1] - refs.cum_t[head : head + 1, span]
                factor = jnp.exp(jnp.where(causal, gap, -jnp.inf))
                mixing = (scores * factor * refs.dt_t[head : head + 1, span]).astype(jnp.bfloat16)
                mine = (pair_lane >= head_size) if which else (pair_lane < head_size)
                total = total + dot(mixing, jnp.where(mine, x_pair, jnp.zeros_like(x_pair)))
            refs.y[span, lanes] = total + refs.skip_row[2:3, lanes] * x_pair.astype(jnp.float32)

    for part in range(SCAN_PARTS):
        join_plane(sizes, refs, part)
        start = refs.share_of(Z_POINTS[3])
        stop = refs.share_of(Z_PARTS)
        refs.send_z(
            start + (stop - start) * part // SCAN_PARTS, start + (stop - start) * (part + 1) // SCAN_PARTS
        )

    for early in range(1, BATCHES + 1):
        first_plane, last_plane = index < sizes.side_count, index + sizes.side_count >= seq_count
        wanted = last_plane if early == BATCHES else ~first_plane

        @pl.when(wanted)
        def _(early=early):
            refs.gates(early - 1, early)

    for part in range(SCAN_PARTS):
        join_chain(sizes, refs, part)

    @pl.when(index < sizes.side_count)
    def _():
        refs.gates(0, BATCHES - 1)

    @pl.when(index + sizes.side_count < seq_count)
    def _():
        refs.gates(BATCHES - 1, BATCHES)

    ones = jnp.ones((8, LANES), jnp.bfloat16)

    @pl.loop(0, blocks)
    def _(block):
        begin = pl.multiple_of(block * QB, QB)
        span = pl.ds(begin, QB)
        state = refs.entering[block] + refs.incoming[...] * refs.prior[block][0:1, :]
        high, middle, _ = three_parts(state)
        c_blk = refs.bc_conv[span, nstate:]
        outside = dot(c_blk, high.astype(jnp.bfloat16)) + dot(c_blk, middle.astype(jnp.bfloat16))
        value = (refs.y[span, :] + refs.from_start[span, :] * outside) * refs.z[span, :]
        refs.y[span, :] = value
        squares = value * value
        folded = squares[:, 0:LANES]
        for part in range(1, channels // LANES):
            folded = folded + squares[:, part * LANES : (part + 1) * LANES]
        first, second, third = three_parts(folded)
        total = dot_nt(ones, first.astype(jnp.bfloat16)) + dot_nt(ones, second.astype(jnp.bfloat16))
        total = total + dot_nt(ones, third.astype(jnp.bfloat16))
        for part in range(QB // LANES):
            line = total[0:1, part * LANES : (part + 1) * LANES]
            refs.square[pl.ds(block * (QB // LANES) + part, 1), :] = line

    def shares():
        return [
            remote(
                refs.square,
                refs.square_in.at[step - 1],
                refs.norm_send.at[step - 1],
                refs.norm_recv.at[step - 1],
                (index, lax.rem(column + step, head_count)),
            )
            for step in range(1, head_count)
        ]

    for copy in shares():
        copy.start()
    for copy in shares():
        copy.wait_recv()
    total = refs.square[...]
    for step in range(1, head_count):
        total = total + refs.square_in[step - 1]
    scale = lax.rsqrt(total / (head_count * channels) + EPSILON)
    lines = rows // LANES
    line_of = lax.broadcasted_iota(jnp.int32, (lines, channels), 0)
    scales = [part.astype(jnp.bfloat16) for part in three_parts(scale)]
    for line in range(lines):
        span = pl.ds(line * LANES, LANES)
        chosen = jnp.where(line_of == line, 1.0, 0.0).astype(jnp.bfloat16)
        wide_scale = dot_tn(scales[0], chosen) + dot_tn(scales[1], chosen) + dot_tn(scales[2], chosen)
        refs.out[span, :] = (refs.y[span, :] * wide_scale * refs.norm_gain[...]).astype(jnp.bfloat16)

    for copy in shares():
        copy.wait_send()

    @pl.when(index + 1 < seq_count)
    def _():
        for which in range(2):
            rim_copy(refs, which).wait_send()

    for part in range(SCAN_PARTS):
        for copy in plane_copies(sizes, refs, part):
            copy.wait_send()

        @pl.when(index + sizes.side_count < seq_count)
        def _(part=part):
            chain_copy(sizes, refs, part).wait_send()

    refs.settle()


def pick(options, which):
    value = options[0]
    for place in range(1, len(options)):
        value = jnp.where(which == place, options[place], value)
    return value


def padded(lines, length):
    return [list(line) + [0] * (length - len(line)) for line in lines]


def project_kernel(sizes, names, *all_refs):
    refs = types.SimpleNamespace(**dict(zip(names, all_refs)))
    index, column = lax.axis_index("seq"), lax.axis_index("head")
    barrier = pltpu.get_barrier_semaphore()

    def greet():
        for step in range(1, sizes.seq_count):
            other = lax.rem(index + step, sizes.seq_count)
            pl.semaphore_signal(barrier, inc=1, device_id=(other, column), device_id_type=MESH)
        for step in range(1, sizes.head_count):
            other = lax.rem(column + step, sizes.head_count)
            pl.semaphore_signal(barrier, inc=1, device_id=(index, other), device_id_type=MESH)

    project_body(sizes, refs, barrier, greet)
    finish_body(sizes, refs)


def project_body(sizes, refs, barrier, greet):
    index, column = lax.axis_index("seq"), lax.axis_index("head")
    seq_count, head_count = sizes.seq_count, sizes.head_count
    cap, direct, shared, lines = sizes.cap, sizes.direct, sizes.shared, sizes.lines
    places, slot_count = sizes.places, sizes.slots
    rows, channels = refs.y.shape
    width = refs.tok.shape[1]
    blocks = rows // QB
    core, line = lax.rem(column, 2), column // 2
    half = width // 2
    def direct_lanes(which):
        return pl.ds(pl.multiple_of(which * half, LANES), direct)

    def shared_lanes(which, from_line):
        return pl.ds(pl.multiple_of(which * half + direct + from_line * shared, LANES), shared)

    own_copies = [
        pltpu.make_async_copy(
            refs.tokens.at[:, shared_lanes(core, line)],
            refs.own_tok.at[:, pl.ds(direct, shared)],
            refs.local.at[1],
        )
    ]
    if direct:
        own_copies.append(
            pltpu.make_async_copy(
                refs.tokens.at[:, direct_lanes(core)], refs.own_tok.at[:, pl.ds(0, direct)], refs.local.at[0]
            )
        )
    weight_copy = pltpu.make_async_copy(refs.w_in.at[0], refs.weight, refs.local.at[2])
    token_copy = pltpu.make_async_copy(refs.tokens, refs.tok, refs.local.at[3])
    side_copy = pltpu.make_async_copy(refs.w_bc, refs.side, refs.local.at[4])
    for copy in own_copies + [weight_copy, token_copy, side_copy]:
        copy.start()
    greet()
    foreign, chosen, slot_of, served, _ = serving_plan(seq_count, sizes.pieces, sizes.outward)
    foreign_count = pick([len(line_) for line_ in foreign], index)
    served_count = pick([len(line_) for line_ in served], index)
    server_of, landing = [], []
    for place in range(places):
        server_of.append(pick([chosen.get((home, place), 0) for home in range(seq_count)], index))
        landing.append(pick([slot_of.get((home, place), 0) for home in range(seq_count)], index))
    homes, home_places = [], []
    for slot in range(slot_count):
        homes.append(pick([line_[slot][0] if slot < len(line_) else 0 for line_ in served], index))
        home_places.append(pick([line_[slot][1] if slot < len(line_) else 0 for line_ in served], index))

    slots = refs.owner_slot[...]
    place_row = jnp.full(slots.shape, -1, jnp.int32)
    for group in range(seq_count * sizes.pieces):
        place = pick([line_.index(group) if group in line_ else -1 for line_ in foreign], index)
        within = (slots >= group * cap) & (slots < (group + 1) * cap)
        moved = jnp.where(place >= 0, slots + (place - group) * cap, -1)
        place_row = jnp.where(within, moved, place_row)

    for place in range(min(len(line_) for line_ in foreign), places):

        @pl.when(place >= foreign_count)
        def _(place=place):
            span = pl.ds(place * cap, cap)
            refs.x_back[span, :] = jnp.zeros((cap, channels), jnp.bfloat16)
            refs.z_back[span, :] = jnp.zeros((cap, channels), jnp.bfloat16)

    def sends(place):
        server = (server_of[place], column)
        slot = landing[place]
        kinds = [(1, pl.ds(direct, shared), shared_lanes(core, line))]
        if direct:
            kinds.append((0, pl.ds(0, direct), direct_lanes(core)))
        return [
            remote(
                refs.packed.at[place, :, source],
                refs.inbox.at[slot, :, target],
                refs.pack_send.at[place, kind],
                refs.pack_recv.at[slot, kind],
                server,
            )
            for kind, source, target in kinds
        ]

    for copy in own_copies:
        copy.wait()
    sublane = lax.broadcasted_iota(jnp.int32, (cap, rows), 0)
    for place in range(places):

        @pl.when(place < foreign_count)
        def _(place=place):
            chosen_rows = jnp.where(place_row == sublane + place * cap, 1.0, 0.0).astype(jnp.bfloat16)
            refs.packed[place] = dot(chosen_rows, refs.own_tok[...]).astype(jnp.bfloat16)
            if place == 0:
                pl.semaphore_wait(barrier, seq_count + head_count - 2)
            for copy in sends(place):
                copy.start()

    prepare_params(sizes, refs)

    pair = 4 * sizes.head_size
    source = lax.broadcasted_iota(jnp.int32, (pair, pair), 0)
    target = lax.broadcasted_iota(jnp.int32, (pair, pair), 1)
    size = sizes.head_size
    from_z = target // (2 * size)
    wanted = (target % (2 * size)) // size * (2 * size) + from_z * size + target % size
    chooser = jnp.where(source == wanted, 1.0, 0.0).astype(jnp.bfloat16)
    weight_copy.wait()

    place_col = jnp.broadcast_to(place_row.astype(jnp.float32), (LANES, rows)).T
    refs.place_col[...] = place_col

    def received(slot):
        kinds = [(1, shared_lanes(core, line))] + ([(0, direct_lanes(core))] if direct else [])
        return [
            remote(
                refs.inbox.at[slot, :, lanes],
                refs.inbox.at[slot, :, lanes],
                refs.pack_send.at[0, kind],
                refs.pack_recv.at[slot, kind],
                (index, column),
            )
            for kind, lanes in kinds
        ]

    def across_lines(slot, arriving):
        copies = []
        for step in range(1, lines):
            from_line = lax.rem(line + lines - step, lines) if arriving else line
            lanes = shared_lanes(core, from_line)
            copies.append(
                remote(
                    refs.inbox.at[slot, :, lanes],
                    refs.inbox.at[slot, :, lanes],
                    refs.line_send.at[slot, step - 1],
                    refs.line_recv.at[slot, step - 1],
                    (index, lax.rem(line + step, lines) * 2 + core),
                )
            )
        return copies

    def across_cores(slot, arriving):
        from_core = 1 - core if arriving else core
        lanes = pl.ds(pl.multiple_of(from_core * half, LANES), half)
        return remote(
            refs.inbox.at[slot, :, lanes],
            refs.inbox.at[slot, :, lanes],
            refs.core_send.at[slot],
            refs.core_recv.at[slot],
            (index, line * 2 + 1 - core),
        )

    def take(slot):
        for copy in received(slot):
            copy.wait_recv()
        for copy in across_lines(slot, False):
            copy.start()

    def separate(part):
        span = pl.ds(pl.multiple_of(part * QB, QB), QB)
        for couple in range(sizes.heads // 2):
            split = dot(refs.weight[span, couple * pair : (couple + 1) * pair], chooser).astype(jnp.bfloat16)
            lanes = pl.ds(couple * pair // 2, pair // 2)
            refs.weight_x[span, lanes] = split[:, : pair // 2]
            refs.weight_z[span, lanes] = split[:, pair // 2 :]

    parts = width // QB
    pl.loop(0, parts // 2)(separate)

    for slot in range(2):

        @pl.when(slot < served_count)
        def _(slot=slot):
            take(slot)

    pl.loop(parts // 2, parts)(separate)
    token_copy.wait()
    side_copy.wait()

    def answer(slot, source, target, send, recv):
        home, place = pick(homes, slot), pick(home_places, slot)
        return remote(
            source.at[slot],
            target.at[pl.ds(pl.multiple_of(place * cap, cap), cap)],
            send.at[slot],
            recv.at[place],
            (home, column),
        )

    def answer_x(slot):
        return answer(slot, refs.x_served, refs.x_back, refs.x_send, refs.x_recv)

    def answer_z(slot):
        return answer(slot, refs.z_served, refs.z_back, refs.z_send, refs.z_recv)

    z_turns = -(-slot_count // Z_EACH)
    quiet = max(2 * blocks, z_turns * (Z_EACH - 1) + 2)
    last_turn = max(slot_count + 2, quiet + blocks, quiet + z_turns)

    @pl.loop(0, last_turn)
    def _(turn):
        @pl.when((turn >= 2) & (turn < served_count))
        def _():
            take(turn)

        @pl.when(turn < blocks)
        def _():
            span = pl.ds(pl.multiple_of(turn * QB, QB), QB)
            tok = refs.tok[span, :]
            place = refs.place_col[span, :]
            mine = jnp.concatenate([place] * (channels // LANES), axis=1) < 0
            product = dot(tok, refs.weight_x[...])
            wide = pl.ds(pl.multiple_of(turn * QB + WIDE, WIDE), QB)
            refs.x_wide[wide, :] = rounded(jnp.where(mine, product, 0.0))
            side = dot(tok, refs.side[...]).astype(jnp.bfloat16)
            refs.bc[span, :] = side
            refs.bc_wide[wide, :] = side.astype(jnp.float32)
            refs.dt_raw[span, 0 : sizes.heads] = dot_nt(tok, refs.w_dt_t[...])
            lane = lax.broadcasted_iota(jnp.int32, (QB, LANES), 1).astype(jnp.float32)
            for part in range(places * cap // LANES):
                hit = jnp.where(place == lane + part * LANES, 1.0, 0.0)
                refs.unpack[span, part * LANES : (part + 1) * LANES] = hit.astype(jnp.bfloat16)

        for block in range(blocks):

            @pl.when(turn == blocks + (block + blocks - 1) % blocks)
            def _(block=block):
                if block == min(1, blocks - 1):
                    send_rim(sizes, refs, 0)
                side_block(sizes, refs, block)

        @pl.when((turn >= quiet) & (turn < quiet + blocks))
        def _():
            span = pl.ds(pl.multiple_of((turn - quiet) * QB, QB), QB)
            place = refs.place_col[span, :]
            mine = jnp.concatenate([place] * (channels // LANES), axis=1) < 0
            product = dot(refs.tok[span, :], refs.weight_z[...])
            refs.z[span, :] = rounded(jnp.where(mine, product, 0.0))

        @pl.when((turn >= 1) & (turn - 1 < served_count))
        def _():
            slot = turn - 1
            for copy in across_lines(slot, True):
                copy.wait_recv()
            across_cores(slot, False).start()

        @pl.when((turn >= 2) & (turn - 2 < served_count))
        def _():
            slot = turn - 2
            across_cores(slot, True).wait_recv()
            refs.x_served[slot] = dot(refs.inbox[slot], refs.weight_x[...]).astype(jnp.bfloat16)
            answer_x(slot).start()

        for extra in range(Z_EACH):
            slot = (turn - quiet) * Z_EACH + extra

            @pl.when((turn >= quiet) & (slot < served_count))
            def _(slot=slot):
                refs.z_served[slot] = dot(refs.inbox[slot], refs.weight_z[...]).astype(jnp.bfloat16)

    def send_z(start, stop):
        @pl.loop(start, stop)
        def _(slot):
            @pl.when(slot < served_count)
            def _():
                answer_z(slot).start()

    def share_of(part):
        return slot_count * part // Z_PARTS

    refs.send_z, refs.share_of = send_z, share_of
    send_z(0, share_of(Z_POINTS[0]))

    def back(place, buffer, recv):
        span = pl.ds(pl.multiple_of(place * cap, cap), cap)
        return remote(
            buffer.at[span], buffer.at[span], refs.x_send.at[0], recv.at[place], (index, column)
        )

    batch = -(-places // BATCHES)

    def arrived(group, buffer, recv):
        @pl.loop(group * batch, min((group + 1) * batch, places))
        def _(place):
            @pl.when(place < foreign_count)
            def _():
                back(place, buffer, recv).wait_recv()

    def unpacked(group, span, buffer):
        lines_ = slice(group * batch * cap, min((group + 1) * batch, places) * cap)
        return dot(refs.unpack[span, lines_], buffer[lines_, :])

    def collect_x():
        for group in range(BATCHES - 1):
            arrived(group, refs.x_back, refs.x_recv)

            @pl.loop(0, blocks)
            def _(block, group=group):
                span = pl.ds(pl.multiple_of(block * QB, QB), QB)
                wide = pl.ds(pl.multiple_of(block * QB + WIDE, WIDE), QB)
                refs.x_wide[wide, :] = refs.x_wide[wide, :] + unpacked(group, span, refs.x_back)

        arrived(BATCHES - 1, refs.x_back, refs.x_recv)
        for block in [blocks - 1, *range(blocks - 1)]:
            span, wide = pl.ds(block * QB, QB), pl.ds(block * QB + WIDE, QB)
            merged = refs.x_wide[wide, :] + unpacked(BATCHES - 1, span, refs.x_back)
            refs.x_wide[wide, :] = merged
            if block == blocks - 1:
                edge = refs.x.shape[0]
                refs.x[...] = merged[QB - edge :, :].astype(jnp.bfloat16)
                send_rim(sizes, refs, 1)
                send_z(share_of(Z_POINTS[0]), share_of(Z_POINTS[1]))

    def gates(first, last):
        for group in range(first, last):
            arrived(group, refs.z_back, refs.z_recv)

            @pl.loop(0, blocks)
            def _(block, group=group):
                span = pl.ds(pl.multiple_of(block * QB, QB), QB)
                total = refs.z[span, :] + unpacked(group, span, refs.z_back)
                refs.z[span, :] = silu(total) if group == BATCHES - 1 else total

    def settle():
        for place in range(places):

            @pl.when(place < foreign_count)
            def _(place=place):
                for copy in sends(place):
                    copy.wait_send()

        @pl.loop(0, slot_count)
        def _(slot):
            @pl.when(slot < served_count)
            def _():
                for copy in across_lines(slot, False):
                    copy.wait_send()
                across_cores(slot, False).wait_send()
                answer_x(slot).wait_send()
                answer_z(slot).wait_send()

    refs.gates = gates
    refs.settle = settle
    refs.collect_x = collect_x


def per_device(
    tokens, owner_slot, w_in, w_bc, w_dt, conv_x, conv_bc, dt_bias, decay_rate, d_skip, norm_gain
):
    rows, width = tokens.shape
    both = w_bc.shape[1]
    heads = dt_bias.shape[0]
    channels = w_in.shape[2] // 2
    nstate = both // 2
    blocks = rows // QB
    head_count = lax.axis_size("head")
    seq_count = lax.axis_size("seq")
    lines = head_count // 2
    cap = min(2 * rows // seq_count, LANES)
    pieces = 2 * rows // seq_count // cap
    direct = next(
        part
        for part in (DIRECT * LANES, width // 4)
        if (width // 2 - part) % (LANES * lines) == 0 and part % LANES == 0
    )
    shared = (width // 2 - direct) // lines
    outward = 2 * (direct + shared) / (4 * channels)
    foreign, _, _, served, _ = serving_plan(seq_count, pieces, outward)
    places = max(len(line) for line in foreign)
    slots = max(len(line) for line in served)
    sizes = types.SimpleNamespace(
        seq_count=seq_count,
        head_count=head_count,
        heads=heads,
        head_size=channels // heads,
        nstate=nstate,
        cap=cap,
        pieces=pieces,
        outward=outward,
        side_count=plane_width(seq_count),
        lines=lines,
        places=places,
        slots=slots,
        direct=direct,
        shared=shared,
    )
    side_count = plane_width(seq_count)
    share = channels // SCAN_PARTS
    in_hbm = dict(tokens=tokens, w_in=w_in, w_bc=w_bc)
    in_vmem = dict(
        owner_slot=owner_slot[None],
        w_dt_t=w_dt.T,
        conv_x=conv_x,
        conv_bc=conv_bc,
        dt_bias=dt_bias[None],
        decay_rate=decay_rate[None],
        d_skip=d_skip[None],
        norm_gain=norm_gain[None],
    )
    inputs = in_hbm | in_vmem
    f32, bf16 = jnp.float32, jnp.bfloat16
    dma = pltpu.SemaphoreType.DMA
    scratch = dict(
        tok=pltpu.VMEM((rows, width), bf16),
        own_tok=pltpu.VMEM((rows, direct + shared), bf16),
        weight=pltpu.VMEM((width, 2 * channels), bf16),
        weight_x=pltpu.VMEM((width, channels), bf16),
        weight_z=pltpu.VMEM((width, channels), bf16),
        side=pltpu.VMEM((width, both), bf16),
        packed=pltpu.VMEM((places, cap, direct + shared), bf16),
        inbox=pltpu.VMEM((slots, cap, width), bf16),
        x_served=pltpu.VMEM((slots, cap, channels), bf16),
        z_served=pltpu.VMEM((slots, cap, channels), bf16),
        x_back=pltpu.VMEM((places * cap, channels), bf16),
        z_back=pltpu.VMEM((places * cap, channels), bf16),
        unpack=pltpu.VMEM((rows, places * cap), bf16),
        place_col=pltpu.VMEM((rows, LANES), f32),
        x=pltpu.VMEM((16, channels), bf16),
        z=pltpu.VMEM((rows, channels), f32),
        bc=pltpu.VMEM((rows, both), bf16),
        dt_raw=pltpu.VMEM((rows, LANES), f32),
        x_rim=pltpu.VMEM((16, channels), bf16),
        bc_rim=pltpu.VMEM((16, both), bf16),
        x_wide=pltpu.VMEM((rows + WIDE, channels), f32),
        bc_wide=pltpu.VMEM((rows + WIDE, both), f32),
        x_conv=pltpu.VMEM((rows, channels), bf16),
        bc_conv=pltpu.VMEM((rows, both), bf16),
        params=pltpu.VMEM((8, LANES), f32),
        spread=pltpu.VMEM((LANES, channels), bf16),
        skip_row=pltpu.VMEM((8, channels), f32),
        to_end=pltpu.VMEM((rows, channels), f32),
        cum=pltpu.VMEM((rows, LANES), f32),
        cum_t=pltpu.VMEM((heads, rows), f32),
        dt_t=pltpu.VMEM((heads, rows), f32),
        from_start=pltpu.VMEM((rows, channels), f32),
        y=pltpu.VMEM((rows, channels), f32),
        entering=pltpu.VMEM((blocks, nstate, channels), f32),
        prior=pltpu.VMEM((blocks, 8, channels), f32),
        incoming=pltpu.VMEM((nstate, channels), f32),
        before=pltpu.VMEM((SCAN_PARTS, nstate, share), f32),
        before_decay=pltpu.VMEM((SCAN_PARTS, 8, share), f32),
        ahead=pltpu.VMEM((SCAN_PARTS, nstate, share), f32),
        ahead_decay=pltpu.VMEM((SCAN_PARTS, 8, share), f32),
        plane_state=pltpu.VMEM((SCAN_PARTS, side_count, nstate, share), bf16),
        plane_decay=pltpu.VMEM((SCAN_PARTS, side_count, 8, share), f32),
        chain_in=pltpu.VMEM((SCAN_PARTS, nstate, share), bf16),
        chain_out=pltpu.VMEM((SCAN_PARTS, nstate, share), bf16),
        square=pltpu.VMEM((rows // LANES, LANES), f32),
        square_in=pltpu.VMEM((head_count - 1, rows // LANES, LANES), f32),
        local=dma((5,)),
        pack_send=dma((places, 2)),
        pack_recv=dma((slots, 2)),
        line_send=dma((slots, lines - 1)),
        line_recv=dma((slots, lines - 1)),
        core_send=dma((slots,)),
        core_recv=dma((slots,)),
        x_send=dma((slots,)),
        x_recv=dma((places,)),
        z_send=dma((slots,)),
        z_recv=dma((places,)),
        rim_send=dma((2,)),
        rim_recv=dma((2,)),
        plane_send=dma((SCAN_PARTS, side_count - 1, 2)),
        plane_recv=dma((SCAN_PARTS, side_count - 1, 2)),
        chain_send=dma((SCAN_PARTS,)),
        chain_recv=dma((SCAN_PARTS,)),
        norm_send=dma((head_count - 1,)),
        norm_recv=dma((head_count - 1,)),
    )
    names = tuple(inputs) + ("out",) + tuple(scratch)
    any_spec = pl.BlockSpec(memory_space=pl.ANY)
    vmem_spec = pl.BlockSpec(memory_space=pltpu.VMEM)
    return pl.pallas_call(
        functools.partial(project_kernel, sizes, names),
        out_shape=jax.ShapeDtypeStruct((rows, channels), bf16),
        in_specs=[any_spec] * len(in_hbm) + [vmem_spec] * len(in_vmem),
        out_specs=vmem_spec,
        scratch_shapes=list(scratch.values()),
        compiler_params=pltpu.CompilerParams(
            collective_id=0, has_side_effects=True, vmem_limit_bytes=62 << 20
        ),
    )(*inputs.values())


def solution(mesh):
    return jax.shard_map(
        per_device,
        mesh=mesh,
        in_specs=(
            P("seq", None),
            P("seq"),
            P("seq", None, "head"),
            P(),
            P(None, "head"),
            P(None, "head"),
            P(),
            P("head"),
            P("head"),
            P("head"),
            P("head"),
        ),
        out_specs=P("seq", "head"),
        check_vma=False,
    )
```

```python
import functools
import types

import jax
import jax.numpy as jnp
from jax import lax
from jax.experimental import pallas as pl
from jax.experimental.pallas import tpu as pltpu
from jax.sharding import PartitionSpec as P

KCONV = 4
QB = 256
MODS = 3
EPSILON = 1e-05
LANES = 128
MESH = pl.DeviceIdType.MESH
Z_PARTS = 12
Z_POINTS = (4, 6, 6, 10)
BATCHES = 2
Z_EACH = 2
DIRECT = 2
SCAN_PARTS = 4
STATE_LOAD = 0.27
BUSY_PRICE = 0.3
WIDE = 8


def plane_width(count):
    return max(side for side in range(1, count) if count % side == 0 and side * side <= count)


def route(start, end, width):
    (plane, side), (last_plane, last_side) = divmod(start, width), divmod(end, width)
    links = []
    while (plane, side) != (last_plane, last_side):
        before = plane * width + side
        if plane != last_plane:
            plane += 1 if last_plane > plane else -1
        else:
            side += 1 if last_side > side else -1
        links.append((before, plane * width + side))
    return links


def serving_plan(count, pieces, outward):
    width = plane_width(count)
    foreign = [
        [owner * pieces + piece for piece in range(pieces) for owner in range(count) if (owner - home) % MODS]
        for home in range(count)
    ]
    groups = [(home, place) for home in range(count) for place in range(len(foreign[home]))]
    loads, busy, chosen = {}, [0] * count, {}
    for start in range(count):
        for end in (start + 1, start - 1, start + width):
            if 0 <= end < count and (end == start + width or end // width == start // width):
                loads[start, end] = STATE_LOAD * pieces

    def trips(home, server):
        return [(outward, link) for link in route(home, server, width)] + [
            (1.0, link) for link in route(server, home, width)
        ]

    def add(home, server, sign):
        busy[server] += sign
        for weight, link in trips(home, server):
            loads[link] = loads.get(link, 0.0) + sign * weight

    def price(home, server):
        total = BUSY_PRICE * ((busy[server] + 1) ** 4 - busy[server] ** 4)
        for weight, link in trips(home, server):
            before = loads.get(link, 0.0)
            total += (before + weight) ** 4 - before**4
        return total

    for _ in range(12):
        for home, place in groups:
            if (home, place) in chosen:
                add(home, chosen[home, place], -1)
            owner = foreign[home][place] // pieces
            options = [server for server in range(count) if (server - owner) % MODS == 0]
            best = min(options, key=lambda server: (round(price(home, server), 6), server))
            chosen[home, place] = best
            add(home, best, 1)
    order = [[] for _ in range(count)]
    for home, place in groups:
        first = route(home, chosen[home, place], width)[0]
        earlier = sum(route(home, chosen[home, other], width)[0] == first for other in range(place))
        order[chosen[home, place]].append((earlier, place, home))
    served = [[(home, place) for _, place, home in sorted(line)] for line in order]
    slots = {group: slot for line in served for slot, group in enumerate(line)}
    return foreign, chosen, slots, served, loads


def dot(a, b):
    return jnp.dot(a, b, preferred_element_type=jnp.float32)


def dot_nt(a, b):
    return lax.dot_general(a, b, (((1,), (1,)), ((), ())), preferred_element_type=jnp.float32)


def dot_tn(a, b):
    return lax.dot_general(a, b, (((0,), (0,)), ((), ())), preferred_element_type=jnp.float32)


def rounded(value):
    return value.astype(jnp.bfloat16).astype(jnp.float32)


def three_parts(value):
    high = rounded(value)
    middle = rounded(value - high)
    return high, middle, value - high - middle


def side_by_side(value, count):
    high, middle, low = three_parts(value)
    packed = high + pltpu.roll(middle, count, 1) + pltpu.roll(low, 2 * count, 1)
    return packed.astype(jnp.bfloat16)


def silu(value):
    return value * jax.nn.sigmoid(value)


def remote(source, target, send, recv, device):
    return pltpu.make_async_remote_copy(
        source, target, send, recv, device_id=device, device_id_type=MESH
    )


def plane_copies(sizes, refs, part):
    index, side = lax.axis_index("seq"), lax.rem(lax.axis_index("seq"), sizes.side_count)
    copies = []
    for step in range(1, sizes.side_count):
        target = (index - side + lax.rem(side + step, sizes.side_count), lax.axis_index("head"))
        for place, buffer in enumerate((refs.plane_state, refs.plane_decay)):
            copies.append(
                remote(
                    buffer.at[part, 0],
                    buffer.at[part, step],
                    refs.plane_send.at[part, step - 1, place],
                    refs.plane_recv.at[part, step - 1, place],
                    target,
                )
            )
    return copies


def chain_copy(sizes, refs, part):
    return remote(
        refs.chain_out.at[part],
        refs.chain_in.at[part],
        refs.chain_send.at[part],
        refs.chain_recv.at[part],
        (lax.axis_index("seq") + sizes.side_count, lax.axis_index("head")),
    )


def join_plane(sizes, refs, part):
    side = lax.rem(lax.axis_index("seq"), sizes.side_count)
    for copy in plane_copies(sizes, refs, part):
        copy.wait_recv()
    total = jnp.zeros(refs.ahead.shape[1:], jnp.float32)
    decay = jnp.ones(refs.ahead_decay.shape[1:], jnp.float32)
    before, before_decay = total, decay
    for place in range(sizes.side_count):
        before = jnp.where(side == place, total, before)
        before_decay = jnp.where(side == place, decay, before_decay)
        slot = lax.rem(side + sizes.side_count - place, sizes.side_count)
        factor = refs.plane_decay[part, slot]
        total = total * factor[0:1, :] + refs.plane_state[part, slot].astype(jnp.float32)
        decay = decay * factor
    refs.before[part] = before
    refs.before_decay[part] = before_decay
    refs.ahead[part] = total
    refs.ahead_decay[part] = decay


def join_chain(sizes, refs, part):
    index = lax.axis_index("seq")
    share = refs.incoming.shape[1] // SCAN_PARTS
    lanes = pl.ds(part * share, share)

    @pl.when(index < sizes.side_count)
    def _():
        refs.chain_in[part] = jnp.zeros(refs.chain_in.shape[1:], jnp.bfloat16)

    @pl.when(index >= sizes.side_count)
    def _():
        chain_copy(sizes, refs, part).wait_recv()

    @pl.when(index + sizes.side_count < sizes.seq_count)
    def _():
        entering = refs.chain_in[part].astype(jnp.float32)
        leaving = refs.ahead[part] + refs.ahead_decay[part][0:1, :] * entering
        refs.chain_out[part] = leaving.astype(jnp.bfloat16)
        chain_copy(sizes, refs, part).start()

    entering = refs.chain_in[part].astype(jnp.float32)
    refs.incoming[:, lanes] = refs.before[part] + refs.before_decay[part][0:1, :] * entering


def rim_copy(refs, which):
    source, landing = ((refs.bc, refs.bc_rim), (refs.x, refs.x_rim))[which]
    edge = landing.shape[0]
    return remote(
        source.at[pl.ds(source.shape[0] - edge, edge)],
        landing,
        refs.rim_send.at[which],
        refs.rim_recv.at[which],
        (lax.axis_index("seq") + 1, lax.axis_index("head")),
    )


def send_rim(sizes, refs, which):
    @pl.when(lax.axis_index("seq") + 1 < sizes.seq_count)
    def _():
        rim_copy(refs, which).start()


def take_rim(sizes, refs, which):
    landing, target = ((refs.bc_rim, refs.bc_wide), (refs.x_rim, refs.x_wide))[which]
    edge = landing.shape[0]
    index = lax.axis_index("seq")

    @pl.when(index > 0)
    def _():
        rim_copy(refs, which).wait_recv()
        target[0:WIDE, :] = landing[...].astype(jnp.float32)[edge - WIDE :, :]

    @pl.when(index == 0)
    def _():
        target[0:WIDE, :] = jnp.zeros((WIDE, target.shape[1]), jnp.float32)


def convolved(source, weights, block):
    taps = weights.shape[0]
    total = jnp.zeros((QB, source.shape[1]), jnp.float32)
    for tap in range(taps):
        shifted = source[pl.ds(block * QB + WIDE - taps + 1 + tap, QB), :]
        total = total + weights[tap : tap + 1, :] * shifted
    return silu(total).astype(jnp.bfloat16)


def spreader(sizes, channels):
    row = lax.broadcasted_iota(jnp.int32, (LANES, channels), 0)
    col = lax.broadcasted_iota(jnp.int32, (LANES, channels), 1)
    wanted = (row % sizes.heads == col // sizes.head_size) & (row < 3 * sizes.heads)
    return jnp.where(wanted, 1.0, 0.0).astype(jnp.bfloat16)


def prepare_params(sizes, refs):
    heads = sizes.heads
    refs.params[...] = jnp.zeros_like(refs.params)
    refs.params[0:1, 0:heads] = refs.dt_bias[...]
    refs.params[1:2, 0:heads] = refs.decay_rate[...]
    refs.params[2:3, 0:heads] = refs.d_skip[...]
    refs.spread[...] = spreader(sizes, refs.y.shape[1])
    refs.skip_row[...] = dot(side_by_side(refs.params[...], heads), refs.spread[...])


def side_block(sizes, refs, block):
    heads = sizes.heads
    span = pl.ds(block * QB, QB)
    lane = lax.broadcasted_iota(jnp.int32, (1, LANES), 1)
    row = lax.broadcasted_iota(jnp.int32, (QB, QB), 0)
    col = lax.broadcasted_iota(jnp.int32, (QB, QB), 1)
    lower = jnp.where(row >= col, 1.0, 0.0).astype(jnp.bfloat16)
    step_dt = jax.nn.softplus(refs.dt_raw[span, :] + refs.params[0:1, :])
    log_decay = jnp.where(lane < heads, -step_dt * refs.params[1:2, :], 0.0)
    sums = dot(lower, side_by_side(log_decay, heads))
    cum = sums + pltpu.roll(sums, LANES - heads, 1) + pltpu.roll(sums, LANES - 2 * heads, 1)
    cum = jnp.where(lane < heads, cum, 0.0)
    refs.cum[span, :] = cum
    refs.cum_t[:, span] = cum.T[0:heads, :]
    refs.dt_t[:, span] = step_dt.T[0:heads, :]
    last = cum[QB - 1 : QB, :]
    to_end = jnp.where(lane < heads, jnp.exp(last - cum) * step_dt, 0.0)
    from_start = jnp.where(lane < heads, jnp.exp(cum), 0.0)
    refs.to_end[span, :] = dot(side_by_side(to_end, heads), refs.spread[...])
    refs.from_start[span, :] = dot(side_by_side(from_start, heads), refs.spread[...])
    if block > 0:
        side_conv(sizes, refs, block)


def side_conv(sizes, refs, block):
    if block == 0:
        take_rim(sizes, refs, 0)
    refs.bc_conv[pl.ds(block * QB, QB), :] = convolved(refs.bc_wide, refs.conv_bc, block)


def finish_body(sizes, refs):
    index, column = lax.axis_index("seq"), lax.axis_index("head")
    seq_count, head_count = sizes.seq_count, sizes.head_count
    heads, head_size, nstate = sizes.heads, sizes.head_size, sizes.nstate
    rows, channels = refs.y.shape
    blocks = rows // QB
    share = channels // SCAN_PARTS

    refs.collect_x()
    for block in [*range(1, blocks), 0]:
        span = pl.ds(block * QB, QB)
        if block == 0:
            side_conv(sizes, refs, 0)
            take_rim(sizes, refs, 1)
        x_blk = convolved(refs.x_wide, refs.conv_x, block)
        refs.x_conv[span, :] = x_blk
        weighted = (x_blk.astype(jnp.float32) * refs.to_end[span, :]).astype(jnp.bfloat16)
        refs.entering[block] = dot_tn(refs.bc_conv[span, 0:nstate], weighted)
    carried = jnp.zeros((nstate, channels), jnp.float32)
    carried_decay = jnp.ones((1, channels), jnp.float32)
    for block in range(blocks):
        added = refs.entering[block]
        refs.entering[block] = carried
        refs.prior[block] = jnp.broadcast_to(carried_decay, refs.prior.shape[1:])
        decay = refs.from_start[pl.ds((block + 1) * QB - 1, 1), :]
        carried = carried * decay + added
        carried_decay = carried_decay * decay
    for part in range(SCAN_PARTS):
        lanes = slice(part * share, (part + 1) * share)
        refs.plane_state[part, 0] = carried[:, lanes].astype(jnp.bfloat16)
        refs.plane_decay[part, 0] = jnp.broadcast_to(carried_decay[:, lanes], (8, share))
        for copy in plane_copies(sizes, refs, part):
            copy.start()
    refs.send_z(refs.share_of(Z_POINTS[1]), refs.share_of(Z_POINTS[2]))

    half = 2 * head_size
    pair_lane = lax.broadcasted_iota(jnp.int32, (QB, half), 1)
    row = lax.broadcasted_iota(jnp.int32, (QB, QB), 0)
    col = lax.broadcasted_iota(jnp.int32, (QB, QB), 1)
    causal = row >= col

    @pl.loop(0, blocks)
    def _(block):
        begin = pl.multiple_of(block * QB, QB)
        span = pl.ds(begin, QB)
        start = refs.share_of(Z_POINTS[2])
        stop = refs.share_of(Z_POINTS[3])
        refs.send_z(start + (stop - start) * block // blocks, start + (stop - start) * (block + 1) // blocks)
        scores = dot_nt(refs.bc_conv[span, nstate:], refs.bc_conv[span, 0:nstate])
        for pair in range(heads // 2):
            lanes = pl.ds(pair * half, half)
            x_pair = refs.x_conv[span, lanes]
            total = jnp.zeros((QB, half), jnp.float32)
            for which in range(2):
                head = 2 * pair + which
                gap = refs.cum[span, head : head + 1] - refs.cum_t[head : head + 1, span]
                factor = jnp.exp(jnp.where(causal, gap, -jnp.inf))
                mixing = (scores * factor * refs.dt_t[head : head + 1, span]).astype(jnp.bfloat16)
                mine = (pair_lane >= head_size) if which else (pair_lane < head_size)
                total = total + dot(mixing, jnp.where(mine, x_pair, jnp.zeros_like(x_pair)))
            refs.y[span, lanes] = total + refs.skip_row[2:3, lanes] * x_pair.astype(jnp.float32)

    for part in range(SCAN_PARTS):
        join_plane(sizes, refs, part)
        start = refs.share_of(Z_POINTS[3])
        stop = refs.share_of(Z_PARTS)
        refs.send_z(
            start + (stop - start) * part // SCAN_PARTS, start + (stop - start) * (part + 1) // SCAN_PARTS
        )

    for early in range(1, BATCHES + 1):
        first_plane, last_plane = index < sizes.side_count, index + sizes.side_count >= seq_count
        wanted = last_plane if early == BATCHES else ~first_plane

        @pl.when(wanted)
        def _(early=early):
            refs.gates(early - 1, early)

    for part in range(SCAN_PARTS):
        join_chain(sizes, refs, part)

    @pl.when(index < sizes.side_count)
    def _():
        refs.gates(0, BATCHES - 1)

    @pl.when(index + sizes.side_count < seq_count)
    def _():
        refs.gates(BATCHES - 1, BATCHES)

    ones = jnp.ones((8, LANES), jnp.bfloat16)

    @pl.loop(0, blocks)
    def _(block):
        begin = pl.multiple_of(block * QB, QB)
        span = pl.ds(begin, QB)
        state = refs.entering[block] + refs.incoming[...] * refs.prior[block][0:1, :]
        high, middle, _ = three_parts(state)
        c_blk = refs.bc_conv[span, nstate:]
        outside = dot(c_blk, high.astype(jnp.bfloat16)) + dot(c_blk, middle.astype(jnp.bfloat16))
        value = (refs.y[span, :] + refs.from_start[span, :] * outside) * refs.z[span, :]
        refs.y[span, :] = value
        squares = value * value
        folded = squares[:, 0:LANES]
        for part in range(1, channels // LANES):
            folded = folded + squares[:, part * LANES : (part + 1) * LANES]
        first, second, _ = three_parts(folded)
        total = dot_nt(ones, first.astype(jnp.bfloat16)) + dot_nt(ones, second.astype(jnp.bfloat16))
        for part in range(QB // LANES):
            line = total[0:1, part * LANES : (part + 1) * LANES]
            refs.square[pl.ds(block * (QB // LANES) + part, 1), :] = line

    def shares():
        return [
            remote(
                refs.square,
                refs.square_in.at[step - 1],
                refs.norm_send.at[step - 1],
                refs.norm_recv.at[step - 1],
                (index, lax.rem(column + step, head_count)),
            )
            for step in range(1, head_count)
        ]

    for copy in shares():
        copy.start()
    for copy in shares():
        copy.wait_recv()
    total = refs.square[...]
    for step in range(1, head_count):
        total = total + refs.square_in[step - 1]
    scale = lax.rsqrt(total / (head_count * channels) + EPSILON)
    lines = rows // LANES
    line_of = lax.broadcasted_iota(jnp.int32, (lines, channels), 0)
    scales = [part.astype(jnp.bfloat16) for part in three_parts(scale)[:2]]
    for line in range(lines):
        span = pl.ds(line * LANES, LANES)
        chosen = jnp.where(line_of == line, 1.0, 0.0).astype(jnp.bfloat16)
        wide_scale = dot_tn(scales[0], chosen) + dot_tn(scales[1], chosen)
        refs.out[span, :] = (refs.y[span, :] * wide_scale * refs.norm_gain[...]).astype(jnp.bfloat16)

    for copy in shares():
        copy.wait_send()

    @pl.when(index + 1 < seq_count)
    def _():
        for which in range(2):
            rim_copy(refs, which).wait_send()

    for part in range(SCAN_PARTS):
        for copy in plane_copies(sizes, refs, part):
            copy.wait_send()

        @pl.when(index + sizes.side_count < seq_count)
        def _(part=part):
            chain_copy(sizes, refs, part).wait_send()

    refs.settle()


def pick(options, which):
    value = options[0]
    for place in range(1, len(options)):
        value = jnp.where(which == place, options[place], value)
    return value


def padded(lines, length):
    return [list(line) + [0] * (length - len(line)) for line in lines]


def project_kernel(sizes, names, *all_refs):
    refs = types.SimpleNamespace(**dict(zip(names, all_refs)))
    index, column = lax.axis_index("seq"), lax.axis_index("head")
    barrier = pltpu.get_barrier_semaphore()

    def greet():
        for step in range(1, sizes.seq_count):
            other = lax.rem(index + step, sizes.seq_count)
            pl.semaphore_signal(barrier, inc=1, device_id=(other, column), device_id_type=MESH)
        for step in range(1, sizes.head_count):
            other = lax.rem(column + step, sizes.head_count)
            pl.semaphore_signal(barrier, inc=1, device_id=(index, other), device_id_type=MESH)

    project_body(sizes, refs, barrier, greet)
    finish_body(sizes, refs)


def project_body(sizes, refs, barrier, greet):
    index, column = lax.axis_index("seq"), lax.axis_index("head")
    seq_count, head_count = sizes.seq_count, sizes.head_count
    cap, direct, shared, lines = sizes.cap, sizes.direct, sizes.shared, sizes.lines
    places, slot_count = sizes.places, sizes.slots
    rows, channels = refs.y.shape
    width = refs.tok.shape[1]
    blocks = rows // QB
    core, line = lax.rem(column, 2), column // 2
    half = width // 2
    def direct_lanes(which):
        return pl.ds(pl.multiple_of(which * half, LANES), direct)

    def shared_lanes(which, from_line):
        return pl.ds(pl.multiple_of(which * half + direct + from_line * shared, LANES), shared)

    own_copies = [
        pltpu.make_async_copy(
            refs.tokens.at[:, shared_lanes(core, line)],
            refs.own_tok.at[:, pl.ds(direct, shared)],
            refs.local.at[1],
        )
    ]
    if direct:
        own_copies.append(
            pltpu.make_async_copy(
                refs.tokens.at[:, direct_lanes(core)], refs.own_tok.at[:, pl.ds(0, direct)], refs.local.at[0]
            )
        )
    weight_copy = pltpu.make_async_copy(refs.w_in.at[0], refs.weight, refs.local.at[2])
    token_copy = pltpu.make_async_copy(refs.tokens, refs.tok, refs.local.at[3])
    side_copy = pltpu.make_async_copy(refs.w_bc, refs.side, refs.local.at[4])
    for copy in own_copies + [weight_copy, token_copy, side_copy]:
        copy.start()
    greet()
    foreign, chosen, slot_of, served, _ = serving_plan(seq_count, sizes.pieces, sizes.outward)
    foreign_count = pick([len(line_) for line_ in foreign], index)
    served_count = pick([len(line_) for line_ in served], index)
    server_of, landing = [], []
    for place in range(places):
        server_of.append(pick([chosen.get((home, place), 0) for home in range(seq_count)], index))
        landing.append(pick([slot_of.get((home, place), 0) for home in range(seq_count)], index))
    homes, home_places = [], []
    for slot in range(slot_count):
        homes.append(pick([line_[slot][0] if slot < len(line_) else 0 for line_ in served], index))
        home_places.append(pick([line_[slot][1] if slot < len(line_) else 0 for line_ in served], index))

    slots = refs.owner_slot[...]
    place_row = jnp.full(slots.shape, -1, jnp.int32)
    for group in range(seq_count * sizes.pieces):
        place = pick([line_.index(group) if group in line_ else -1 for line_ in foreign], index)
        within = (slots >= group * cap) & (slots < (group + 1) * cap)
        moved = jnp.where(place >= 0, slots + (place - group) * cap, -1)
        place_row = jnp.where(within, moved, place_row)

    for place in range(min(len(line_) for line_ in foreign), places):

        @pl.when(place >= foreign_count)
        def _(place=place):
            span = pl.ds(place * cap, cap)
            refs.x_back[span, :] = jnp.zeros((cap, channels), jnp.bfloat16)
            refs.z_back[span, :] = jnp.zeros((cap, channels), jnp.bfloat16)

    def sends(place):
        server = (server_of[place], column)
        slot = landing[place]
        kinds = [(1, pl.ds(direct, shared), shared_lanes(core, line))]
        if direct:
            kinds.append((0, pl.ds(0, direct), direct_lanes(core)))
        return [
            remote(
                refs.packed.at[place, :, source],
                refs.inbox.at[slot, :, target],
                refs.pack_send.at[place, kind],
                refs.pack_recv.at[slot, kind],
                server,
            )
            for kind, source, target in kinds
        ]

    for copy in own_copies:
        copy.wait()
    sublane = lax.broadcasted_iota(jnp.int32, (cap, rows), 0)
    for place in range(places):

        @pl.when(place < foreign_count)
        def _(place=place):
            chosen_rows = jnp.where(place_row == sublane + place * cap, 1.0, 0.0).astype(jnp.bfloat16)
            refs.packed[place] = dot(chosen_rows, refs.own_tok[...]).astype(jnp.bfloat16)
            if place == 0:
                pl.semaphore_wait(barrier, seq_count + head_count - 2)
            for copy in sends(place):
                copy.start()

    prepare_params(sizes, refs)

    pair = 4 * sizes.head_size
    source = lax.broadcasted_iota(jnp.int32, (pair, pair), 0)
    target = lax.broadcasted_iota(jnp.int32, (pair, pair), 1)
    size = sizes.head_size
    from_z = target // (2 * size)
    wanted = (target % (2 * size)) // size * (2 * size) + from_z * size + target % size
    chooser = jnp.where(source == wanted, 1.0, 0.0).astype(jnp.bfloat16)
    weight_copy.wait()

    place_col = jnp.broadcast_to(place_row.astype(jnp.float32), (LANES, rows)).T
    refs.place_col[...] = place_col

    def received(slot):
        kinds = [(1, shared_lanes(core, line))] + ([(0, direct_lanes(core))] if direct else [])
        return [
            remote(
                refs.inbox.at[slot, :, lanes],
                refs.inbox.at[slot, :, lanes],
                refs.pack_send.at[0, kind],
                refs.pack_recv.at[slot, kind],
                (index, column),
            )
            for kind, lanes in kinds
        ]

    def across_lines(slot, arriving):
        copies = []
        for step in range(1, lines):
            from_line = lax.rem(line + lines - step, lines) if arriving else line
            lanes = shared_lanes(core, from_line)
            copies.append(
                remote(
                    refs.inbox.at[slot, :, lanes],
                    refs.inbox.at[slot, :, lanes],
                    refs.line_send.at[slot, step - 1],
                    refs.line_recv.at[slot, step - 1],
                    (index, lax.rem(line + step, lines) * 2 + core),
                )
            )
        return copies

    def across_cores(slot, arriving):
        from_core = 1 - core if arriving else core
        lanes = pl.ds(pl.multiple_of(from_core * half, LANES), half)
        return remote(
            refs.inbox.at[slot, :, lanes],
            refs.inbox.at[slot, :, lanes],
            refs.core_send.at[slot],
            refs.core_recv.at[slot],
            (index, line * 2 + 1 - core),
        )

    def take(slot):
        for copy in received(slot):
            copy.wait_recv()
        for copy in across_lines(slot, False):
            copy.start()

    def separate(part):
        span = pl.ds(pl.multiple_of(part * QB, QB), QB)
        for couple in range(sizes.heads // 2):
            split = dot(refs.weight[span, couple * pair : (couple + 1) * pair], chooser).astype(jnp.bfloat16)
            lanes = pl.ds(couple * pair // 2, pair // 2)
            refs.weight_x[span, lanes] = split[:, : pair // 2]
            refs.weight_z[span, lanes] = split[:, pair // 2 :]

    parts = width // QB
    pl.loop(0, parts // 2)(separate)

    for slot in range(2):

        @pl.when(slot < served_count)
        def _(slot=slot):
            take(slot)

    pl.loop(parts // 2, parts)(separate)
    token_copy.wait()
    side_copy.wait()

    def answer(slot, source, target, send, recv):
        home, place = pick(homes, slot), pick(home_places, slot)
        return remote(
            source.at[slot],
            target.at[pl.ds(pl.multiple_of(place * cap, cap), cap)],
            send.at[slot],
            recv.at[place],
            (home, column),
        )

    def answer_x(slot):
        return answer(slot, refs.x_served, refs.x_back, refs.x_send, refs.x_recv)

    def answer_z(slot):
        return answer(slot, refs.z_served, refs.z_back, refs.z_send, refs.z_recv)

    z_turns = -(-slot_count // Z_EACH)
    quiet = max(2 * blocks, z_turns * (Z_EACH - 1) + 2)
    last_turn = max(slot_count + 2, quiet + blocks, quiet + z_turns)

    @pl.loop(0, last_turn)
    def _(turn):
        @pl.when((turn >= 2) & (turn < served_count))
        def _():
            take(turn)

        @pl.when(turn < blocks)
        def _():
            span = pl.ds(pl.multiple_of(turn * QB, QB), QB)
            tok = refs.tok[span, :]
            place = refs.place_col[span, :]
            mine = jnp.concatenate([place] * (channels // LANES), axis=1) < 0
            product = dot(tok, refs.weight_x[...])
            wide = pl.ds(pl.multiple_of(turn * QB + WIDE, WIDE), QB)
            refs.x_wide[wide, :] = rounded(jnp.where(mine, product, 0.0))
            side = dot(tok, refs.side[...]).astype(jnp.bfloat16)
            refs.bc[span, :] = side
            refs.bc_wide[wide, :] = side.astype(jnp.float32)
            refs.dt_raw[span, 0 : sizes.heads] = dot_nt(tok, refs.w_dt_t[...])
            lane = lax.broadcasted_iota(jnp.int32, (QB, LANES), 1).astype(jnp.float32)
            for part in range(places * cap // LANES):
                hit = jnp.where(place == lane + part * LANES, 1.0, 0.0)
                refs.unpack[span, part * LANES : (part + 1) * LANES] = hit.astype(jnp.bfloat16)

        for block in range(blocks):

            @pl.when(turn == blocks + (block + blocks - 1) % blocks)
            def _(block=block):
                if block == min(1, blocks - 1):
                    send_rim(sizes, refs, 0)
                side_block(sizes, refs, block)

        @pl.when((turn >= quiet) & (turn < quiet + blocks))
        def _():
            span = pl.ds(pl.multiple_of((turn - quiet) * QB, QB), QB)
            place = refs.place_col[span, :]
            mine = jnp.concatenate([place] * (channels // LANES), axis=1) < 0
            product = dot(refs.tok[span, :], refs.weight_z[...])
            refs.z[span, :] = rounded(jnp.where(mine, product, 0.0))

        @pl.when((turn >= 1) & (turn - 1 < served_count))
        def _():
            slot = turn - 1
            for copy in across_lines(slot, True):
                copy.wait_recv()
            across_cores(slot, False).start()

        @pl.when((turn >= 2) & (turn - 2 < served_count))
        def _():
            slot = turn - 2
            across_cores(slot, True).wait_recv()
            refs.x_served[slot] = dot(refs.inbox[slot], refs.weight_x[...]).astype(jnp.bfloat16)
            answer_x(slot).start()

        for extra in range(Z_EACH):
            slot = (turn - quiet) * Z_EACH + extra

            @pl.when((turn >= quiet) & (slot < served_count))
            def _(slot=slot):
                refs.z_served[slot] = dot(refs.inbox[slot], refs.weight_z[...]).astype(jnp.bfloat16)

    def send_z(start, stop):
        @pl.loop(start, stop)
        def _(slot):
            @pl.when(slot < served_count)
            def _():
                answer_z(slot).start()

    def share_of(part):
        return slot_count * part // Z_PARTS

    refs.send_z, refs.share_of = send_z, share_of
    send_z(0, share_of(Z_POINTS[0]))

    def back(place, buffer, recv):
        span = pl.ds(pl.multiple_of(place * cap, cap), cap)
        return remote(
            buffer.at[span], buffer.at[span], refs.x_send.at[0], recv.at[place], (index, column)
        )

    batch = -(-places // BATCHES)

    def arrived(group, buffer, recv):
        @pl.loop(group * batch, min((group + 1) * batch, places))
        def _(place):
            @pl.when(place < foreign_count)
            def _():
                back(place, buffer, recv).wait_recv()

    def unpacked(group, span, buffer):
        lines_ = slice(group * batch * cap, min((group + 1) * batch, places) * cap)
        return dot(refs.unpack[span, lines_], buffer[lines_, :])

    def collect_x():
        for group in range(BATCHES - 1):
            arrived(group, refs.x_back, refs.x_recv)

            @pl.loop(0, blocks)
            def _(block, group=group):
                span = pl.ds(pl.multiple_of(block * QB, QB), QB)
                wide = pl.ds(pl.multiple_of(block * QB + WIDE, WIDE), QB)
                refs.x_wide[wide, :] = refs.x_wide[wide, :] + unpacked(group, span, refs.x_back)

        arrived(BATCHES - 1, refs.x_back, refs.x_recv)
        for block in [blocks - 1, *range(blocks - 1)]:
            span, wide = pl.ds(block * QB, QB), pl.ds(block * QB + WIDE, QB)
            merged = refs.x_wide[wide, :] + unpacked(BATCHES - 1, span, refs.x_back)
            refs.x_wide[wide, :] = merged
            if block == blocks - 1:
                edge = refs.x.shape[0]
                refs.x[...] = merged[QB - edge :, :].astype(jnp.bfloat16)
                send_rim(sizes, refs, 1)
                send_z(share_of(Z_POINTS[0]), share_of(Z_POINTS[1]))

    def gates(first, last):
        for group in range(first, last):
            arrived(group, refs.z_back, refs.z_recv)

            @pl.loop(0, blocks)
            def _(block, group=group):
                span = pl.ds(pl.multiple_of(block * QB, QB), QB)
                total = refs.z[span, :] + unpacked(group, span, refs.z_back)
                refs.z[span, :] = silu(total) if group == BATCHES - 1 else total

    def settle():
        for place in range(places):

            @pl.when(place < foreign_count)
            def _(place=place):
                for copy in sends(place):
                    copy.wait_send()

        @pl.loop(0, slot_count)
        def _(slot):
            @pl.when(slot < served_count)
            def _():
                for copy in across_lines(slot, False):
                    copy.wait_send()
                across_cores(slot, False).wait_send()
                answer_x(slot).wait_send()
                answer_z(slot).wait_send()

    refs.gates = gates
    refs.settle = settle
    refs.collect_x = collect_x


def per_device(
    tokens, owner_slot, w_in, w_bc, w_dt, conv_x, conv_bc, dt_bias, decay_rate, d_skip, norm_gain
):
    rows, width = tokens.shape
    both = w_bc.shape[1]
    heads = dt_bias.shape[0]
    channels = w_in.shape[2] // 2
    nstate = both // 2
    blocks = rows // QB
    head_count = lax.axis_size("head")
    seq_count = lax.axis_size("seq")
    lines = head_count // 2
    cap = min(2 * rows // seq_count, LANES)
    pieces = 2 * rows // seq_count // cap
    direct = next(
        part
        for part in (DIRECT * LANES, width // 4)
        if (width // 2 - part) % (LANES * lines) == 0 and part % LANES == 0
    )
    shared = (width // 2 - direct) // lines
    outward = 2 * (direct + shared) / (4 * channels)
    foreign, _, _, served, _ = serving_plan(seq_count, pieces, outward)
    places = max(len(line) for line in foreign)
    slots = max(len(line) for line in served)
    sizes = types.SimpleNamespace(
        seq_count=seq_count,
        head_count=head_count,
        heads=heads,
        head_size=channels // heads,
        nstate=nstate,
        cap=cap,
        pieces=pieces,
        outward=outward,
        side_count=plane_width(seq_count),
        lines=lines,
        places=places,
        slots=slots,
        direct=direct,
        shared=shared,
    )
    side_count = plane_width(seq_count)
    share = channels // SCAN_PARTS
    in_hbm = dict(tokens=tokens, w_in=w_in, w_bc=w_bc)
    in_vmem = dict(
        owner_slot=owner_slot[None],
        w_dt_t=w_dt.T,
        conv_x=conv_x,
        conv_bc=conv_bc,
        dt_bias=dt_bias[None],
        decay_rate=decay_rate[None],
        d_skip=d_skip[None],
        norm_gain=norm_gain[None],
    )
    inputs = in_hbm | in_vmem
    f32, bf16 = jnp.float32, jnp.bfloat16
    dma = pltpu.SemaphoreType.DMA
    scratch = dict(
        tok=pltpu.VMEM((rows, width), bf16),
        own_tok=pltpu.VMEM((rows, direct + shared), bf16),
        weight=pltpu.VMEM((width, 2 * channels), bf16),
        weight_x=pltpu.VMEM((width, channels), bf16),
        weight_z=pltpu.VMEM((width, channels), bf16),
        side=pltpu.VMEM((width, both), bf16),
        packed=pltpu.VMEM((places, cap, direct + shared), bf16),
        inbox=pltpu.VMEM((slots, cap, width), bf16),
        x_served=pltpu.VMEM((slots, cap, channels), bf16),
        z_served=pltpu.VMEM((slots, cap, channels), bf16),
        x_back=pltpu.VMEM((places * cap, channels), bf16),
        z_back=pltpu.VMEM((places * cap, channels), bf16),
        unpack=pltpu.VMEM((rows, places * cap), bf16),
        place_col=pltpu.VMEM((rows, LANES), f32),
        x=pltpu.VMEM((16, channels), bf16),
        z=pltpu.VMEM((rows, channels), f32),
        bc=pltpu.VMEM((rows, both), bf16),
        dt_raw=pltpu.VMEM((rows, LANES), f32),
        x_rim=pltpu.VMEM((16, channels), bf16),
        bc_rim=pltpu.VMEM((16, both), bf16),
        x_wide=pltpu.VMEM((rows + WIDE, channels), f32),
        bc_wide=pltpu.VMEM((rows + WIDE, both), f32),
        x_conv=pltpu.VMEM((rows, channels), bf16),
        bc_conv=pltpu.VMEM((rows, both), bf16),
        params=pltpu.VMEM((8, LANES), f32),
        spread=pltpu.VMEM((LANES, channels), bf16),
        skip_row=pltpu.VMEM((8, channels), f32),
        to_end=pltpu.VMEM((rows, channels), f32),
        cum=pltpu.VMEM((rows, LANES), f32),
        cum_t=pltpu.VMEM((heads, rows), f32),
        dt_t=pltpu.VMEM((heads, rows), f32),
        from_start=pltpu.VMEM((rows, channels), f32),
        y=pltpu.VMEM((rows, channels), f32),
        entering=pltpu.VMEM((blocks, nstate, channels), f32),
        prior=pltpu.VMEM((blocks, 8, channels), f32),
        incoming=pltpu.VMEM((nstate, channels), f32),
        before=pltpu.VMEM((SCAN_PARTS, nstate, share), f32),
        before_decay=pltpu.VMEM((SCAN_PARTS, 8, share), f32),
        ahead=pltpu.VMEM((SCAN_PARTS, nstate, share), f32),
        ahead_decay=pltpu.VMEM((SCAN_PARTS, 8, share), f32),
        plane_state=pltpu.VMEM((SCAN_PARTS, side_count, nstate, share), bf16),
        plane_decay=pltpu.VMEM((SCAN_PARTS, side_count, 8, share), f32),
        chain_in=pltpu.VMEM((SCAN_PARTS, nstate, share), bf16),
        chain_out=pltpu.VMEM((SCAN_PARTS, nstate, share), bf16),
        square=pltpu.VMEM((rows // LANES, LANES), f32),
        square_in=pltpu.VMEM((head_count - 1, rows // LANES, LANES), f32),
        local=dma((5,)),
        pack_send=dma((places, 2)),
        pack_recv=dma((slots, 2)),
        line_send=dma((slots, lines - 1)),
        line_recv=dma((slots, lines - 1)),
        core_send=dma((slots,)),
        core_recv=dma((slots,)),
        x_send=dma((slots,)),
        x_recv=dma((places,)),
        z_send=dma((slots,)),
        z_recv=dma((places,)),
        rim_send=dma((2,)),
        rim_recv=dma((2,)),
        plane_send=dma((SCAN_PARTS, side_count - 1, 2)),
        plane_recv=dma((SCAN_PARTS, side_count - 1, 2)),
        chain_send=dma((SCAN_PARTS,)),
        chain_recv=dma((SCAN_PARTS,)),
        norm_send=dma((head_count - 1,)),
        norm_recv=dma((head_count - 1,)),
    )
    names = tuple(inputs) + ("out",) + tuple(scratch)
    any_spec = pl.BlockSpec(memory_space=pl.ANY)
    vmem_spec = pl.BlockSpec(memory_space=pltpu.VMEM)
    return pl.pallas_call(
        functools.partial(project_kernel, sizes, names),
        out_shape=jax.ShapeDtypeStruct((rows, channels), bf16),
        in_specs=[any_spec] * len(in_hbm) + [vmem_spec] * len(in_vmem),
        out_specs=vmem_spec,
        scratch_shapes=list(scratch.values()),
        compiler_params=pltpu.CompilerParams(
            collective_id=0, has_side_effects=True, vmem_limit_bytes=62 << 20
        ),
    )(*inputs.values())


def solution(mesh):
    return jax.shard_map(
        per_device,
        mesh=mesh,
        in_specs=(
            P("seq", None),
            P("seq"),
            P("seq", None, "head"),
            P(),
            P(None, "head"),
            P(None, "head"),
            P(),
            P("head"),
            P("head"),
            P("head"),
            P("head"),
        ),
        out_specs=P("seq", "head"),
        check_vma=False,
    )
```
